32 devices in a mesh: fsdp: 16 (over z, y, x), dp: 2 (over core).
Axes of the slice: x: 2, y: 2, z: 4, core: 2. Of those that a mesh axis runs over, the one named last changes fastest.
Arguments:
- token_ids: int32 [32, 512], P(('fsdp', 'dp')), may hold values from 0 to 30719, as said below
- labels: int32 [32, 512], P(('fsdp', 'dp')), may hold values 0 or 1
- loss_mask: int32 [32, 512], P(('fsdp', 'dp')), may hold values from 0 to 1, as said below
- batch_of: int32 [32], P(('fsdp', 'dp')), may hold values from 0 to 1, as said below
- layer_in: float32 [1, 1024, 8192], P(None, None, ('fsdp', 'dp'))
- layer_down: float32 [1, 4096, 1024], P(None, ('fsdp', 'dp')), may hold values from -0.09375 to 0.09375
- word_table: float32 [30720, 1024], P(('fsdp', 'dp')), may hold values from -0.3 to 0.3
- side_mat: float32 [1536, 1024], P(('fsdp', 'dp'))
- vectors: float32 [16384], P(('fsdp', 'dp'))
- in_rows: float32 [1, 3, 1024], replicated, may hold values from 1e-07 to 1e-05
- in_cols: float32 [1, 8192], P(None, ('fsdp', 'dp')), may hold values from 1e-07 to 1e-05
- down_rows: float32 [1, 4096], P(None, ('fsdp', 'dp')), may hold values from 1e-07 to 1e-05
- down_cols: float32 [1, 1024], replicated, may hold values from 1e-07 to 1e-05
- word_rows: float32 [30720], P(('fsdp', 'dp')), may hold values from 1e-12 to 1e-10
- word_cols: float32 [1024], replicated, may hold values from 1e-12 to 1e-10
- side_rows: float32 [1536], P(('fsdp', 'dp')), may hold values from 1e-07 to 1e-05
- side_cols: float32 [2, 1024], replicated, may hold values from 1e-07 to 1e-05
- vec_moment: float32 [16384], P(('fsdp', 'dp')), as said below
Outputs:
- loss: float32 [], replicated
- new_in: float32 [1, 1024, 8192], P(None, None, ('fsdp', 'dp'))
- new_in_rows: float32 [1, 3, 1024], replicated
- new_in_cols: float32 [1, 8192], P(None, ('fsdp', 'dp'))
- in_copy: bfloat16 [1, 1024, 8192], P(None, None, ('fsdp', 'dp'))
- new_down: float32 [1, 4096, 1024], P(None, ('fsdp', 'dp'))
- new_down_rows: float32 [1, 4096], P(None, ('fsdp', 'dp'))
- new_down_cols: float32 [1, 1024], replicated
- down_copy: bfloat16 [1, 4096, 1024], P(None, ('fsdp', 'dp'))
- new_word: float32 [30720, 1024], P(('fsdp', 'dp'))
- new_word_rows: float32 [30720], P(('fsdp', 'dp'))
- new_word_cols: float32 [1024], replicated
- word_copy: bfloat16 [30720, 1024], P(('fsdp', 'dp'))
- new_side: float32 [1536, 1024], P(('fsdp', 'dp'))
- new_side_rows: float32 [1536], P(('fsdp', 'dp'))
- new_side_cols: float32 [2, 1024], replicated
- side_copy: bfloat16 [1536, 1024], P(('fsdp', 'dp'))
- new_vectors: float32 [16384], P(('fsdp', 'dp'))
- new_moment: float32 [16384], P(('fsdp', 'dp'))
- vector_copy: bfloat16 [16384], P(('fsdp', 'dp'))
The draws below stay inside these ranges and needn't reach their ends.
Inputs may be any that keep to these rules, and one draw needn't show every extreme that they name: `token_ids`: the 512 tokens of one device (its 1 sequence along fsdp+dp) fall at most 32 times into one block of 960 consecutive vocabulary rows, and in every device some block gets exactly 32. `loss_mask`: position 0 of every sequence counts. `batch_of`: each of the 2 micro-batches holds 16 sequences. `vec_moment`: every entry is positive.
All inputs are finite; a program needn't handle non-finite values. No bound on the sum of `labels` on one device may be relied on, other than what follows from the above.
Results may differ from the reference program's by a relative error of at most 0.0055.
The reference program's roundings to bfloat16 on the way count: a program that leaves them out, or rounds other values in their place, can miss the bound.
Values may be sent and summed in bfloat16 or wider, within the bound.
A program may use at most 256 MiB of HBM per device.

```python
import math
import jax
import jax.numpy as jnp
from jax import lax

D = 1024
HEADS = 16
HEAD_DIM = 64
FF = 4096
VOCAB = 30720
SEQ_LEN = 512
LAYERS = 1
MICRO = 2
SEQS = 32
TOK_DEV = 512
CAP = 32
IN_WIDTH = 8192
SIDE = 1536
VEC = 16384
DEVICES = 32


def unit_noise(key, shape):
    return jax.random.normal(key, shape, jnp.float32)


def draw_token_ids(key, part):
    blocks = DEVICES
    slots = CAP * blocks
    block_rows = VOCAB // blocks

    def one_device(device_index):
        subkey = jax.random.fold_in(key, device_index)
        order = jax.random.permutation(jax.random.fold_in(subkey, 1), slots).astype(jnp.int32)
        chosen = jax.random.randint(jax.random.fold_in(subkey, 2), (), 0, blocks)
        owner = jnp.arange(slots, dtype=jnp.int32) % blocks
        score = order - slots * (owner == chosen).astype(jnp.int32)
        picked = jnp.argsort(score, stable=True)[:TOK_DEV].astype(jnp.int32)
        offset = jax.random.randint(jax.random.fold_in(subkey, 3), (TOK_DEV,), 0, block_rows)
        return picked % blocks * block_rows + offset
    drawn = jax.vmap(one_device)(jnp.arange(DEVICES, dtype=jnp.int32))
    return drawn.reshape(SEQS, SEQ_LEN).astype(jnp.int32)


def draw_loss_mask(key, part):
    coins = jax.random.randint(jax.random.fold_in(key, 11), (SEQS, SEQ_LEN), 0, 20)
    kept = (coins < 17).astype(jnp.int32)
    first = (jnp.arange(SEQ_LEN)[None, :] == 0).astype(jnp.int32)
    return jnp.maximum(kept, first).astype(jnp.int32)


def draw_batch_of(key, part):
    order = jax.random.permutation(jax.random.fold_in(key, 13), SEQS).astype(jnp.int32)
    return (order % MICRO).astype(jnp.int32)


def draw_layer_in(key, part):
    column = jnp.arange(IN_WIDTH)
    boost = jnp.where((column >= 3 * D) & (column < 4 * D), 8.0, 1.0)
    noise = unit_noise(jax.random.fold_in(key, 17), (LAYERS, D, IN_WIDTH))
    return noise * (boost * D ** (-0.5))[None, None, :]


def draw_side_mat(key, part):
    row = jnp.arange(SIDE)
    scale = jnp.where(row < SEQ_LEN, 0.05, D ** (-0.5))
    noise = unit_noise(jax.random.fold_in(key, 19), (SIDE, D))
    return noise * scale[:, None]


def draw_vectors(key, part):
    position = jnp.arange(VEC)
    piece_width = 8 * D + FF
    inner = position % piece_width
    in_layers = position < LAYERS * piece_width
    tail = position - LAYERS * piece_width
    layer_gain = (inner >= 3 * D) & (inner < 4 * D) | (inner >= 6 * D + FF) & (inner < 7 * D + FF)
    is_gain = jnp.where(in_layers, layer_gain, tail < D)
    is_predictor = jnp.logical_not(in_layers) & (tail >= 3 * D)
    noise = unit_noise(jax.random.fold_in(key, 23), (VEC,))
    entries = 0.1 * noise
    return jnp.where(is_gain, 1.0 + 0.1 * noise, jnp.where(is_predictor, 2.0 * D ** (-0.5) * noise, entries))


def draw_vec_moment(key, part):
    lower_end, upper_end = (1e-07, 1e-05)
    exponent = jax.random.uniform(jax.random.fold_in(key, 29), (VEC,), jnp.float32, math.log(lower_end), math.log(upper_end))
    return jnp.exp(exponent)


def plant(entries, rng, smallest, top_value):
    longest = entries.shape.index(max(entries.shape))
    spots = []
    for shift in (0, 1):
        where = [jax.random.randint(jax.random.fold_in(rng, axis), (), 0, length) for axis, length in enumerate(entries.shape)]
        where[longest] = (where[longest] + shift) % entries.shape[longest]
        spots.append(tuple(where))
    return entries.at[spots[0]].set(smallest).at[spots[1]].set(top_value)


def level_of(rng, dims, split, least, largest):
    def one(axis_at, blocks):
        draws = jax.random.uniform(jax.random.fold_in(jax.random.fold_in(rng, 6), axis_at), (blocks,), jnp.float32, least / len(split), largest / len(split))
        return jnp.repeat(jnp.exp(draws), dims[axis_at] // blocks).reshape((-1,) + (1,) * (len(dims) - axis_at - 1))

    gain = one(*split[0])
    for cut in split[1:]:
        gain = gain * one(*cut)
    return gain


def bell_draw(rng, dims, width, bound, split=(), kind=jnp.bfloat16):
    loudness = level_of(rng, dims, split, -0.22, 0.18) if split else 1.0
    values = jax.random.normal(rng, dims, jnp.float32) * width * loudness
    return jnp.minimum(jnp.maximum(values, -bound), bound).astype(kind)


def setup_inputs(seed: int = 0) -> dict:
    key_of = jax.random.split(jax.random.key(seed), 19)
    token_ids = draw_token_ids(jax.random.fold_in(key_of[18], 71), 0)
    labels = plant((jax.random.randint(key_of[1], (SEQS, SEQ_LEN), 0, 20) < 3).astype(jnp.int32), jax.random.fold_in(key_of[1], 1), 0, 1)
    loss_mask = draw_loss_mask(jax.random.fold_in(key_of[18], 71), 0)
    batch_of = draw_batch_of(jax.random.fold_in(key_of[18], 71), 0)
    layer_in = draw_layer_in(jax.random.fold_in(key_of[18], 71), 0)
    layer_down = bell_draw(key_of[5], (LAYERS, FF, D), FF ** -0.5, 0.09375, ((1, 32),), jnp.float32)
    word_table = bell_draw(key_of[6], (VOCAB, D), 0.05, 0.3, ((0, 32),), jnp.float32)
    side_mat = draw_side_mat(jax.random.fold_in(key_of[18], 71), 0)
    vectors = draw_vectors(jax.random.fold_in(key_of[18], 71), 0)
    in_rows = jnp.clip(jnp.exp(jax.random.uniform(key_of[9], (LAYERS, 3, D), jnp.float32, math.log(1.0000000116860974e-07), math.log(9.999999747378752e-06))), 1.0000000116860974e-07, 9.999999747378752e-06)
    in_cols = jnp.clip(jnp.exp(math.log(9.999999747378752e-06) - 4.6051701 * jax.random.uniform(key_of[10], (LAYERS, IN_WIDTH), jnp.float32) ** level_of(key_of[10], (LAYERS, IN_WIDTH), ((1, 32),), -0.2, 0.2)), 1.0000000116860974e-07, 9.999999747378752e-06)
    down_rows = jnp.clip(jnp.exp(math.log(9.999999747378752e-06) - 4.6051701 * jax.random.uniform(key_of[11], (LAYERS, FF), jnp.float32) ** level_of(key_of[11], (LAYERS, FF), ((1, 32),), -0.2, 0.2)), 1.0000000116860974e-07, 9.999999747378752e-06)
    down_cols = jnp.clip(jnp.exp(jax.random.uniform(key_of[12], (LAYERS, D), jnp.float32, math.log(1.0000000116860974e-07), math.log(9.999999747378752e-06))), 1.0000000116860974e-07, 9.999999747378752e-06)
    word_rows = jnp.clip(jnp.exp(math.log(1.000000013351432e-10) - 4.6051702 * jax.random.uniform(key_of[13], (VOCAB,), jnp.float32) ** level_of(key_of[13], (VOCAB,), ((0, 32),), -0.2, 0.2)), 9.999999960041972e-13, 1.000000013351432e-10)
    word_cols = jnp.clip(jnp.exp(jax.random.uniform(key_of[14], (D,), jnp.float32, math.log(9.999999960041972e-13), math.log(1.000000013351432e-10))), 9.999999960041972e-13, 1.000000013351432e-10)
    side_rows = jnp.clip(jnp.exp(math.log(9.999999747378752e-06) - 4.6051701 * jax.random.uniform(key_of[15], (SIDE,), jnp.float32) ** level_of(key_of[15], (SIDE,), ((0, 32),), -0.2, 0.2)), 1.0000000116860974e-07, 9.999999747378752e-06)
    side_cols = jnp.clip(jnp.exp(jax.random.uniform(key_of[16], (2, D), jnp.float32, math.log(1.0000000116860974e-07), math.log(9.999999747378752e-06))), 1.0000000116860974e-07, 9.999999747378752e-06)
    vec_moment = draw_vec_moment(jax.random.fold_in(key_of[18], 71), 0)
    return dict(token_ids=token_ids, labels=labels, loss_mask=loss_mask, batch_of=batch_of, layer_in=layer_in, layer_down=layer_down, word_table=word_table, side_mat=side_mat, vectors=vectors, in_rows=in_rows, in_cols=in_cols, down_rows=down_rows, down_cols=down_cols, word_rows=word_rows, word_cols=word_cols, side_rows=side_rows, side_cols=side_cols, vec_moment=vec_moment)


learn_rate = 0.02
decay_rate = 0.5
tiny_square = 1e-30
norm_epsilon = 1e-12
precise = lax.Precision.HIGHEST

@jax.custom_vjp
def low(v):
    return lax.optimization_barrier(v.astype(jnp.bfloat16)).astype(jnp.float32)

@jax.custom_vjp
def low_back(v):
    return v

def low_keep(v):
    return (low(v), None)

def low_pass(kept, grad):
    return (grad,)

def back_keep(v):
    return (v, None)

def back_low(kept, grad):
    return (low(grad),)
low.defvjp(low_keep, low_pass)
low_back.defvjp(back_keep, back_low)

def layer_norm(inputs, norm_gain, norm_shift):
    center = inputs - lax.optimization_barrier(jnp.mean(inputs, axis=-1, keepdims=True))
    spread = lax.optimization_barrier(jnp.mean(center * center, axis=-1, keepdims=True))
    return center * lax.rsqrt(spread + norm_epsilon) * norm_gain + norm_shift

def product(pattern, left_side, right_side):
    return jnp.einsum(pattern, left_side, right_side, precision=precise)

def piece_bounds():
    return [0, D, 2 * D, 3 * D, 4 * D, 5 * D, 5 * D + FF, 6 * D + FF, 7 * D + FF, 8 * D + FF]

def layer_slices(all_vectors, layer_index):
    bounds = piece_bounds()
    offset = layer_index * (8 * D + FF)
    return [all_vectors[offset + bounds[slot_index]:offset + bounds[slot_index + 1]] for slot_index in range(9)]

def global_slices(all_vectors):
    offset = LAYERS * (8 * D + FF)
    return [all_vectors[offset + slot_index * D:offset + (slot_index + 1) * D] for slot_index in range(4)]

def segment_spans():
    spans = []
    bounds = piece_bounds()
    for layer_index in range(LAYERS):
        offset = layer_index * (8 * D + FF)
        for slot_index in range(9):
            spans.append((offset + bounds[slot_index], offset + bounds[slot_index + 1]))
    offset = LAYERS * (8 * D + FF)
    for slot_index in range(4):
        spans.append((offset + slot_index * D, offset + (slot_index + 1) * D))
    return spans

def forward(word_table, side_mat, layer_in, layer_down, vectors, token_ids, labels, token_weight):
    word_low = low(word_table)
    side_low = low(side_mat)
    in_low = low(layer_in)
    down_low = low(layer_down)
    vector_low = low(vectors)
    group_size, length = token_ids.shape
    gain_emb, shift_emb, head_bias, predictor = global_slices(vector_low)
    embedded = jnp.take(word_low, token_ids, axis=0) + side_low[:length][None, :, :]
    hidden = layer_norm(embedded, gain_emb, shift_emb)
    score_scale = HEAD_DIM ** (-0.5)
    for layer_index in range(LAYERS):
        bias_q, bias_v, bias_o, gain_a, shift_a, bias_up, bias_down, gain_b, shift_b = layer_slices(vector_low, layer_index)
        weight_in = in_low[layer_index]
        joint_bias = jnp.concatenate([bias_q, jnp.zeros_like(bias_q), bias_v])
        projected = low(low_back(product('gsd,de->gse', low(hidden), weight_in[:, :3 * D]) + joint_bias))
        heads_view = projected.reshape(group_size, length, 3, HEADS, HEAD_DIM)
        scores = low_back(product('gqhe,gkhe->ghqk', heads_view[:, :, 0], heads_view[:, :, 1]) * score_scale)
        soft_probs = jax.nn.softmax(scores, axis=-1)
        mixed = product('ghqk,gkhe->gqhe', low(soft_probs), heads_view[:, :, 2])
        context = low(low_back(mixed.reshape(group_size, length, D)))
        attended = low_back(product('gsd,de->gse', context, weight_in[:, 3 * D:4 * D]) + bias_o)
        middle = layer_norm(hidden + attended, gain_a, shift_a)
        lifted = low_back(product('gsd,df->gsf', low(middle), weight_in[:, 4 * D:]) + bias_up)
        activated = low(jax.nn.gelu(lifted, approximate=False))
        lowered = low_back(product('gsf,fd->gsd', activated, down_low[layer_index]) + bias_down)
        hidden = layer_norm(middle + lowered, gain_b, shift_b)
    head_pre = low_back(product('gsd,de->gse', low(hidden), side_low[length:]) + head_bias)
    head_act = low(jax.nn.gelu(head_pre, approximate=False))
    logits = product('gsd,d->gs', head_act, predictor)
    per_token = jax.nn.softplus(logits) - labels * logits
    return jnp.sum(token_weight * per_token)

def factored(gradient, rows_old, cols_old, weight):
    square = gradient * gradient + tiny_square
    rows_new = decay_rate * rows_old + (1.0 - decay_rate) * lax.optimization_barrier(jnp.mean(square, axis=1))
    cols_new = decay_rate * cols_old + (1.0 - decay_rate) * lax.optimization_barrier(jnp.mean(square, axis=0))
    second = rows_new[:, None] * cols_new[None, :] / jnp.mean(rows_new)
    update = gradient * lax.rsqrt(second)
    clip_scale = jnp.maximum(1.0, jnp.sqrt(jnp.mean(update * update)))
    return (weight - learn_rate * update / clip_scale, rows_new, cols_new)

def unfactored(gradient, moment_old, weight):
    moment = decay_rate * moment_old + (1.0 - decay_rate) * (gradient * gradient + tiny_square)
    update = gradient * lax.rsqrt(moment)
    clip_scale = jnp.maximum(1.0, jnp.sqrt(jnp.mean(update * update)))
    return (weight - learn_rate * update / clip_scale, moment)

def reference(token_ids, labels, loss_mask, batch_of, layer_in, layer_down, word_table, side_mat, vectors, in_rows, in_cols, down_rows, down_cols, word_rows, word_cols, side_rows, side_cols, vec_moment):
    mask_float = loss_mask.astype(jnp.float32)
    member = (batch_of[:, None] == jnp.arange(MICRO)[None, :]).astype(jnp.float32)
    counts = lax.optimization_barrier(jnp.sum(member * lax.optimization_barrier(jnp.sum(mask_float, axis=1))[:, None], axis=0))
    seq_count = lax.optimization_barrier(jnp.sum(member * counts[None, :], axis=1))
    token_weight = mask_float / (seq_count * MICRO)[:, None]
    bundle = 8
    stacked = (token_ids.reshape(-1, bundle, SEQ_LEN), labels.astype(jnp.float32).reshape(-1, bundle, SEQ_LEN), token_weight.reshape(-1, bundle, SEQ_LEN))
    params = (word_table, side_mat, layer_in, layer_down, vectors)

    def group_step(carry, pieces):
        loss_sum, grads = carry
        group_ids, group_labels, group_weight = pieces

        def local_loss(word_arg, side_arg, in_arg, down_arg, vector_arg):
            return forward(word_arg, side_arg, in_arg, down_arg, vector_arg, group_ids, group_labels, group_weight)
        loss_part, pull = jax.vjp(local_loss, *params)
        parts = pull(jnp.ones((), jnp.float32))
        return ((loss_sum + loss_part, tuple((old + new for old, new in zip(grads, parts)))), None)
    zeros = tuple((jnp.zeros_like(array) for array in params))
    (loss, grads), unused = lax.scan(group_step, (jnp.zeros((), jnp.float32), zeros), stacked)
    grad_word, grad_side, grad_in, grad_down, grad_vec = grads
    cuts = [(0, 3 * D), (3 * D, 4 * D), (4 * D, 4 * D + FF)]
    in_new, in_rows_new, in_cols_new = ([], [], [])
    down_new, down_rows_new, down_cols_new = ([], [], [])
    for layer_index in range(LAYERS):
        weight_parts, row_parts, col_parts = ([], [], [])
        for part_index in range(3):
            col_from, col_to = cuts[part_index]
            new_part, rows_part, cols_part = factored(grad_in[layer_index][:, col_from:col_to], in_rows[layer_index, part_index], in_cols[layer_index, col_from:col_to], layer_in[layer_index][:, col_from:col_to])
            weight_parts.append(new_part)
            row_parts.append(rows_part)
            col_parts.append(cols_part)
        in_new.append(jnp.concatenate(weight_parts, axis=1))
        in_rows_new.append(jnp.stack(row_parts))
        in_cols_new.append(jnp.concatenate(col_parts))
        new_part, rows_part, cols_part = factored(grad_down[layer_index], down_rows[layer_index], down_cols[layer_index], layer_down[layer_index])
        down_new.append(new_part)
        down_rows_new.append(rows_part)
        down_cols_new.append(cols_part)
    new_in = jnp.stack(in_new)
    new_down = jnp.stack(down_new)
    new_word, new_word_rows, new_word_cols = factored(grad_word, word_rows, word_cols, word_table)
    pos_new, pos_rows_new, pos_cols_new = factored(grad_side[:SEQ_LEN], side_rows[:SEQ_LEN], side_cols[0], side_mat[:SEQ_LEN])
    head_new, head_rows_new, head_cols_new = factored(grad_side[SEQ_LEN:], side_rows[SEQ_LEN:], side_cols[1], side_mat[SEQ_LEN:])
    new_side = jnp.concatenate([pos_new, head_new], axis=0)
    vector_parts, moment_parts = ([], [])
    for span_from, span_to in segment_spans():
        new_part, moment_part = unfactored(grad_vec[span_from:span_to], vec_moment[span_from:span_to], vectors[span_from:span_to])
        vector_parts.append(new_part)
        moment_parts.append(moment_part)
    new_vectors = jnp.concatenate(vector_parts)
    new_moment = jnp.concatenate(moment_parts)
    return (loss, new_in, jnp.stack(in_rows_new), jnp.stack(in_cols_new), new_in.astype(jnp.bfloat16), new_down, jnp.stack(down_rows_new), jnp.stack(down_cols_new), new_down.astype(jnp.bfloat16), new_word, new_word_rows, new_word_cols, new_word.astype(jnp.bfloat16), new_side, jnp.concatenate([pos_rows_new, head_rows_new]), jnp.stack([pos_cols_new, head_cols_new]), new_side.astype(jnp.bfloat16), new_vectors, new_moment, new_vectors.astype(jnp.bfloat16))
```

```python
import functools
import math

import jax
import jax.numpy as jnp
from jax import lax
from jax.experimental import pallas as pl
from jax.experimental.pallas import tpu as pltpu
from jax.sharding import PartitionSpec as P

D = 1024
HEADS = 16
HEAD_DIM = 64
FF = 4096
VOCAB = 30720
SEQ_LEN = 512
LAYERS = 1
MICRO = 2
BOTH = ("fsdp", "dp")
LOW = jnp.bfloat16
MESH = pl.DeviceIdType.MESH
ALL = slice(None)


learn_rate = 0.02
decay_rate = 0.5
tiny_square = 1e-30
norm_epsilon = 1e-12
precise = lax.Precision.HIGHEST


def layer_norm(inputs, norm_gain, norm_shift):
    center = inputs - jnp.mean(inputs, axis=-1, keepdims=True)
    spread = jnp.mean(center * center, axis=-1, keepdims=True)
    return center * lax.rsqrt(spread + norm_epsilon) * norm_gain + norm_shift


def norm_back(inputs, norm_gain, norm_shift, cotangent):
    result, pull = jax.vjp(layer_norm, inputs, norm_gain, norm_shift)
    return pull(cotangent)


def exact_gelu(inputs):
    return jax.nn.gelu(inputs, approximate=False)


def gelu_back(inputs, cotangent):
    result, pull = jax.vjp(exact_gelu, inputs)
    return pull(cotangent)[0]


def multiply(left_side, right_side):
    return jnp.dot(left_side, right_side, preferred_element_type=jnp.float32)


def multiply_left(left_side, right_side):
    return lax.dot_general(
        left_side, right_side, (((0,), (0,)), ((), ())), preferred_element_type=jnp.float32
    )


def multiply_right(left_side, right_side):
    return lax.dot_general(
        left_side, right_side, (((1,), (1,)), ((), ())), preferred_element_type=jnp.float32
    )


def piece_bounds():
    return [0, D, 2 * D, 3 * D, 4 * D, 5 * D, 5 * D + FF, 6 * D + FF, 7 * D + FF, 8 * D + FF]


def layer_slices(all_vectors, layer_index):
    bounds = piece_bounds()
    offset = layer_index * (8 * D + FF)
    return [
        all_vectors[offset + bounds[slot_index] : offset + bounds[slot_index + 1]]
        for slot_index in range(9)
    ]


def segment_index(position):
    piece_width = 8 * D + FF
    inner = position % piece_width
    layer_of = position // piece_width
    bounds = piece_bounds()[1:-1]
    local_segment = sum(((inner >= bound).astype(jnp.int32) for bound in bounds))
    tail = 9 * LAYERS + (position - LAYERS * piece_width) // D
    return jnp.where(position < LAYERS * piece_width, 9 * layer_of + local_segment, tail)


def segment_sizes():
    sizes = []
    sizes = sizes + [D, D, D, D, D, FF, D, D, D]
    return jnp.array(sizes + [D, D, D, D], jnp.float32)


def attend(queries, key_rows, values):
    scores = jnp.einsum(
        "qhe,khe->hqk", queries, key_rows, preferred_element_type=jnp.float32
    ) * HEAD_DIM ** (-0.5)
    peak_score = jnp.max(scores, axis=-1, keepdims=True)
    exponent = jnp.exp(scores - peak_score)
    running = jnp.sum(exponent, axis=-1, keepdims=True)
    soft_probs = exponent / running
    context = jnp.einsum(
        "hqk,khe->qhe", soft_probs.astype(jnp.bfloat16), values, preferred_element_type=jnp.float32
    )
    return (context, peak_score + jnp.log(running))


def attend_back(queries, key_rows, values, log_total, d_context):
    score_scale = HEAD_DIM ** (-0.5)
    scores = (
        jnp.einsum("qhe,khe->hqk", queries, key_rows, preferred_element_type=jnp.float32)
        * score_scale
    )
    soft_probs = jnp.exp(scores - log_total)
    d_values = jnp.einsum(
        "hqk,qhe->khe",
        soft_probs.astype(jnp.bfloat16),
        d_context,
        preferred_element_type=jnp.float32,
    )
    d_probs = jnp.einsum("qhe,khe->hqk", d_context, values, preferred_element_type=jnp.float32)
    d_scores = soft_probs * (d_probs - jnp.sum(d_probs * soft_probs, axis=-1, keepdims=True))
    d_scores_low = d_scores.astype(jnp.bfloat16)
    d_queries = (
        jnp.einsum("hqk,khe->qhe", d_scores_low, key_rows, preferred_element_type=jnp.float32)
        * score_scale
    )
    d_keys = (
        jnp.einsum("hqk,qhe->khe", d_scores_low, queries, preferred_element_type=jnp.float32)
        * score_scale
    )
    return jnp.stack([d_queries, d_keys, d_values], axis=1)


def layer_forward(hidden, weight_in, weight_down, pieces, seq_dev):
    bias_q, bias_v, bias_o, gain_a, shift_a, bias_up, bias_down, gain_b, shift_b = pieces
    tokens = hidden.shape[0]
    length = tokens // seq_dev
    hidden_low = hidden.astype(jnp.bfloat16)
    joint_bias = jnp.concatenate([bias_q, jnp.zeros_like(bias_q), bias_v])
    projected = (multiply_right(hidden_low, weight_in[: 3 * D]) + joint_bias).astype(jnp.bfloat16)
    heads_view = projected.reshape(seq_dev, length, 3, HEADS, HEAD_DIM)
    context, log_total = jax.vmap(attend)(
        heads_view[:, :, 0], heads_view[:, :, 1], heads_view[:, :, 2]
    )
    context_low = context.reshape(tokens, D).astype(jnp.bfloat16)
    mid_in = hidden + (multiply_right(context_low, weight_in[3 * D : 4 * D]) + bias_o)
    middle = layer_norm(mid_in, gain_a, shift_a)
    middle_low = middle.astype(jnp.bfloat16)
    lifted = multiply_right(middle_low, weight_in[4 * D :]) + bias_up
    active_low = exact_gelu(lifted).astype(jnp.bfloat16)
    out_in = middle + (multiply(active_low, weight_down) + bias_down)
    output = layer_norm(out_in, gain_b, shift_b)
    return (
        output,
        (
            hidden_low,
            projected,
            log_total,
            context_low,
            mid_in,
            middle_low,
            lifted,
            active_low,
            out_in,
        ),
    )


def layer_backward(grad_out, weight_in, weight_down, pieces, kept, seq_dev):
    bias_q, bias_v, bias_o, gain_a, shift_a, bias_up, bias_down, gain_b, shift_b = pieces
    (
        hidden_low,
        projected,
        log_total,
        context_low,
        mid_in,
        middle_low,
        lifted,
        active_low,
        out_in,
    ) = kept
    tokens = mid_in.shape[0]
    length = tokens // seq_dev
    d_out_in, d_gain_b, d_shift_b = norm_back(out_in, gain_b, shift_b, grad_out)
    d_down_low = d_out_in.astype(jnp.bfloat16)
    grad_down = multiply_left(active_low, d_down_low)
    d_lifted_low = gelu_back(lifted, multiply_right(d_down_low, weight_down)).astype(jnp.bfloat16)
    grad_up = multiply_left(d_lifted_low, middle_low)
    d_middle = d_out_in + multiply(d_lifted_low, weight_in[4 * D :])
    d_mid_in, d_gain_a, d_shift_a = norm_back(mid_in, gain_a, shift_a, d_middle)
    d_attended_low = d_mid_in.astype(jnp.bfloat16)
    grad_out_proj = multiply_left(d_attended_low, context_low)
    d_context_low = multiply(d_attended_low, weight_in[3 * D : 4 * D]).astype(jnp.bfloat16)
    heads_view = projected.reshape(seq_dev, length, 3, HEADS, HEAD_DIM)
    d_heads = jax.vmap(attend_back)(
        heads_view[:, :, 0],
        heads_view[:, :, 1],
        heads_view[:, :, 2],
        log_total,
        d_context_low.reshape(seq_dev, length, HEADS, HEAD_DIM),
    )
    d_projected_low = d_heads.reshape(tokens, 3 * D).astype(jnp.bfloat16)
    grad_joint = multiply_left(d_projected_low, hidden_low)
    d_hidden = d_mid_in + multiply(d_projected_low, weight_in[: 3 * D])
    joint_sums = jnp.sum(d_projected_low.astype(jnp.float32), axis=0)
    grad_pieces = jnp.concatenate(
        [
            joint_sums[:D],
            joint_sums[2 * D :],
            jnp.sum(d_attended_low.astype(jnp.float32), axis=0),
            d_gain_a,
            d_shift_a,
            jnp.sum(d_lifted_low.astype(jnp.float32), axis=0),
            jnp.sum(d_down_low.astype(jnp.float32), axis=0),
            d_gain_b,
            d_shift_b,
        ]
    )
    return (
        d_hidden,
        [grad_joint, grad_out_proj, grad_up],
        grad_down,
        grad_pieces,
    )


def place():
    block = lax.axis_index("fsdp")
    return block // 4, (block // 2) % 2, block % 2, lax.axis_index("dp")


def device(z, y, x, c):
    return ((z * 2 + y) * 2 + x, c)


def my_rank():
    return lax.axis_index("fsdp") * 2 + lax.axis_index("dp")


def by_rank(index):
    return (index // 2, index % 2)


def neighbours(z, y, x, c):
    return (
        device(z, y, 1 - x, c),
        device(z, 1 - y, x, c),
        device(z, y, x, 1 - c),
        [device((z + k) % 4, y, x, c) for k in (1, 2, 3)],
    )


def enter(n):
    me = my_rank()
    barrier = pltpu.get_barrier_semaphore()

    def greet(step, carry):
        pl.semaphore_signal(
            barrier, inc=1, device_id=by_rank((me + step) % n), device_id_type=MESH
        )
        return carry

    lax.fori_loop(1, n, greet, 0)
    pl.semaphore_wait(barrier, n - 1)


class Copies:
    def __init__(self, send, recv):
        self.send, self.recv, self.begun = send, recv, []

    def start(self, src, dst, target):
        slot = len(self.begun)
        copy = pltpu.make_async_remote_copy(
            src_ref=src,
            dst_ref=dst,
            send_sem=self.send.at[slot],
            recv_sem=self.recv.at[slot],
            device_id=target,
            device_id_type=MESH,
        )
        copy.start()
        self.begun.append(copy)
        return copy

    def drain(self):
        for copy in self.begun:
            copy.wait_send()


def exchange_copy(src, dst, send, recv, step, n):
    me = my_rank()
    target = (me + step) % n
    return pltpu.make_async_remote_copy(
        src_ref=src.at[target],
        dst_ref=dst.at[me],
        send_sem=send.at[step],
        recv_sem=recv.at[step],
        device_id=by_rank(target),
        device_id_type=MESH,
    )


def exchange_start(src, dst, send, recv, n):
    def begin(step, carry):
        exchange_copy(src, dst, send, recv, step, n).start()
        return carry

    lax.fori_loop(1, n, begin, 0)


def exchange_wait(src, dst, send, recv, n):
    def finish(step, carry):
        exchange_copy(src, dst, send, recv, step, n).wait()
        return carry

    lax.fori_loop(1, n, finish, 0)


def pipeline(order, chunks):
    live = [iter(chunk) for chunk in chunks]
    for index in order:
        next(live[index], None)


def gather_order(plan):
    first = [i for i, p in enumerate(plan) if p[3]]
    rest = [i for i, p in enumerate(plan) if not p[3]]
    order = first + rest + first + first
    for step in range(len(rest) + 4):
        order += [rest[i] for i in range(min(step, len(rest) - 1), -1, -1) if 0 <= step - i < 4]
    return order + first + first


def gather_kernel(plan, count, *refs):
    local, out = refs[:count], refs[count + 1 : 2 * count + 1]
    found, rows = refs[count], refs[2 * count + 1]
    send, recv, own_sem, row_send, row_recv = refs[2 * count + 2 :]
    z, y, x, c = place()
    n = 32
    me = my_rank()
    enter(n)
    copies = Copies(send, recv)
    own = []
    for i in range(count):
        own.append(pltpu.make_async_copy(local[i], out[i].at[z, y, x, c], own_sem.at[i]))
    own.append(pltpu.make_async_copy(found.at[me], rows.at[me], own_sem.at[count]))
    for copy in own:
        copy.start()
    to_x, to_y, to_core, to_z = neighbours(z, y, x, c)

    def pass_on(ref, where, target):
        return copies.start(ref.at[where], ref.at[where], target)

    landed = set()

    def own_there(i):
        if i not in landed:
            own[i].wait()
            landed.add(i)

    def chunk(i, start, size, plane_first):
        ref, mine, half = out[i], local[i], size // 2
        part, low, high = pl.ds(start, size), pl.ds(start, half), pl.ds(start + half, half)
        last = []
        if not plane_first:
            along = [copies.start(mine.at[part], ref.at[z, y, x, c, part], t) for t in to_z]
            yield
            for copy in along:
                copy.wait_recv()
            own_there(i)
            first = pass_on(ref, (ALL, y, x, c, low), to_x)
            second = pass_on(ref, (ALL, y, x, c, high), to_y)
            last.append(pass_on(ref, (ALL, y, x, c, part), to_core))
            yield
            first.wait_recv()
            second.wait_recv()
            first = pass_on(ref, (ALL, y, ALL, c, low), to_y)
            second = pass_on(ref, (ALL, ALL, x, c, high), to_x)
            last.append(pass_on(ref, (ALL, y, 1 - x, c, low), to_core))
            last.append(pass_on(ref, (ALL, 1 - y, x, c, high), to_core))
            yield
            first.wait_recv()
            second.wait_recv()
            last.append(pass_on(ref, (ALL, 1 - y, ALL, c, low), to_core))
            last.append(pass_on(ref, (ALL, ALL, 1 - x, c, high), to_core))
        else:
            first = copies.start(mine.at[low], ref.at[z, y, x, c, low], to_x)
            second = copies.start(mine.at[high], ref.at[z, y, x, c, high], to_y)
            last.append(copies.start(mine.at[part], ref.at[z, y, x, c, part], to_core))
            yield
            first.wait_recv()
            second.wait_recv()
            own_there(i)
            first = pass_on(ref, (z, y, ALL, c, low), to_y)
            second = pass_on(ref, (z, ALL, x, c, high), to_x)
            last.append(pass_on(ref, (z, y, 1 - x, c, low), to_core))
            last.append(pass_on(ref, (z, 1 - y, x, c, high), to_core))
            yield
            first.wait_recv()
            second.wait_recv()
            along = [pass_on(ref, (z, ALL, ALL, c, part), t) for t in to_z]
            last.append(pass_on(ref, (z, 1 - y, ALL, c, low), to_core))
            last.append(pass_on(ref, (z, ALL, 1 - x, c, high), to_core))
            yield
            for k in (1, 2, 3):
                along[k - 1].wait_recv()
                last.append(pass_on(ref, ((z + 4 - k) % 4, ALL, ALL, c, part), to_core))
        yield
        for copy in last:
            copy.wait_recv()
        yield

    chunks = [chunk(*p) for p in plan]
    exchange_start(found, rows, row_send, row_recv, n)
    pipeline(gather_order(plan), chunks)
    for live in chunks:
        next(live, None)
    exchange_wait(found, rows, row_send, row_recv, n)
    copies.drain()
    for i in range(count + 1):
        own_there(i)


def gather_plan(heights, plane_rows):
    plan = []
    for i, height in enumerate(heights):
        start = 0
        for size in plane_rows.get(i, ()):
            plan.append((i, start, size, True))
            start += size
        while start < height:
            size = 64 if height - start >= 64 else height - start
            plan.append((i, start, size, False))
            start += size
    return plan


def gather_weights(arrays, found):
    count = len(arrays)
    plan = gather_plan([a.shape[0] for a in arrays], {1: (32,)})
    total = sum(15 if p[3] else 12 for p in plan)
    hbm = pl.BlockSpec(memory_space=pl.ANY)
    vmem = pl.BlockSpec(memory_space=pltpu.VMEM)
    dma = pltpu.SemaphoreType.DMA
    return pl.pallas_call(
        functools.partial(gather_kernel, plan, count),
        name="gather_weights",
        out_shape=tuple(jax.ShapeDtypeStruct((4, 2, 2, 2) + a.shape, a.dtype) for a in arrays)
        + (jax.ShapeDtypeStruct(found.shape, found.dtype),),
        in_specs=[vmem] * count + [hbm],
        out_specs=tuple([hbm] * (count + 1)),
        scratch_shapes=[dma((total,)), dma((total,)), dma((count + 1,)), dma((32,)), dma((32,))],
        compiler_params=pltpu.CompilerParams(collective_id=0, has_side_effects=True),
    )(*arrays, found)


def add_blocks(dst, other, shape, at_dst, at_other):
    def body(index, carry):
        where = []
        for extent in reversed(shape):
            where.append(index % extent)
            index = index // extent
        where = tuple(reversed(where))
        d, o = at_dst(*where), at_other(*where)
        total = dst[d].astype(jnp.float32) + other[o].astype(jnp.float32)
        dst[d] = total.astype(dst.dtype)
        return carry

    lax.fori_loop(0, math.prod(shape), body, 0)


def scatter_kernel(plan, count, *refs):
    grads, buckets, vector = refs[:count], refs[count], refs[count + 1]
    out = refs[count + 2 : 2 * count + 2]
    arrived, vector_all = refs[2 * count + 2 : 2 * count + 4]
    rest = refs[2 * count + 4 :]
    scratch = [rest[7 * i : 7 * i + 7] for i in range(count)]
    send, recv, load, own_sem, row_send, row_recv, vec_send, vec_recv = rest[7 * count :]
    z, y, x, c = place()
    n = 32
    me = my_rank()
    enter(n)
    copies = Copies(send, recv)
    to_x, to_y, to_core, to_z = neighbours(z, y, x, c)
    own = [
        pltpu.make_async_copy(buckets.at[me], arrived.at[me], own_sem.at[0]),
        pltpu.make_async_copy(vector.at[me], vector_all.at[me], own_sem.at[1]),
    ]
    for copy in own:
        copy.start()

    def chunk(slot, i, start, low_size, high_size):
        held, from_core, low_1, high_1, low_2, high_2, from_z = scratch[i]
        grad, size = grads[i], low_size + high_size
        part = pl.ds(start, size)
        low, high = pl.ds(start, low_size), pl.ds(start + low_size, high_size)
        core = copies.start(grad.at[:, :, :, 1 - c, part], from_core.at[:, :, :, part], to_core)
        mine = pltpu.make_async_copy(
            grad.at[:, :, :, c, part], held.at[:, :, :, part], load.at[slot]
        )
        mine.start()
        yield
        mine.wait()
        core.wait_recv()

        add_blocks(
            held,
            from_core,
            (4, 2, 2),
            lambda a, b, d: (a, b, d, part),
            lambda a, b, d: (a, b, d, part),
        )
        first = copies.start(held.at[:, 1 - y, :, low], low_1.at[:, :, low], to_y)
        second = copies.start(held.at[:, :, 1 - x, high], high_1.at[:, :, high], to_x)
        yield
        first.wait_recv()
        second.wait_recv()
        add_blocks(
            held, low_1, (4, 2), lambda a, d: (a, y, d, low), lambda a, d: (a, d, low)
        )
        add_blocks(
            held, high_1, (4, 2), lambda a, b: (a, b, x, high), lambda a, b: (a, b, high)
        )
        first = copies.start(held.at[:, y, 1 - x, low], low_2.at[:, low], to_x)
        second = copies.start(held.at[:, 1 - y, x, high], high_2.at[:, high], to_y)
        yield
        first.wait_recv()
        second.wait_recv()
        add_blocks(held, low_2, (4,), lambda a: (a, y, x, low), lambda a: (a, low))
        add_blocks(held, high_2, (4,), lambda a: (a, y, x, high), lambda a: (a, high))
        along = [
            copies.start(held.at[(z + k) % 4, y, x, part], from_z.at[k - 1, part], to_z[k - 1])
            for k in (1, 2, 3)
        ]
        yield
        for copy in along:
            copy.wait_recv()
        total = held[z, y, x, part].astype(jnp.float32)
        for k in range(3):
            total = total + from_z[k, part].astype(jnp.float32)
        out[i][part] = total
        yield

    chunks = [chunk(slot, *p) for slot, p in enumerate(plan)]
    order = list(range(len(plan)))
    for step in range(len(plan) + 4):
        order += [i for i in range(min(step, len(plan) - 1), -1, -1) if 0 <= step - i < 4]
    exchange_start(vector, vector_all, vec_send, vec_recv, n)
    live = [iter(one) for one in chunks]
    for index in order[: len(plan)]:
        next(live[index])
    exchange_start(buckets, arrived, row_send, row_recv, n)
    for index in order[len(plan) :]:
        next(live[index])
    exchange_wait(vector, vector_all, vec_send, vec_recv, n)
    exchange_wait(buckets, arrived, row_send, row_recv, n)
    copies.drain()
    for copy in own:
        copy.wait()


def scatter_plan(heights):
    plan = []
    for i, height in enumerate(heights):
        start = 0
        while start < height:
            size = min(64, height - start)
            low = (size // 2 + 15) // 16 * 16
            plan.append((i, start, low, size - low))
            start += size
    return plan


def scatter_grads(arrays, buckets, vector):
    count = len(arrays)
    heights = [a.shape[4] for a in arrays]
    plan = scatter_plan(heights)
    total = 8 * len(plan)
    hbm = pl.BlockSpec(memory_space=pl.ANY)
    vmem = pl.BlockSpec(memory_space=pltpu.VMEM)
    dma = pltpu.SemaphoreType.DMA
    scratch = []
    for h in heights:
        for lead in ((4, 2, 2), (4, 2, 2), (4, 2), (4, 2), (4,), (4,), (3,)):
            scratch.append(pltpu.VMEM(lead + (h, D), LOW))
    return pl.pallas_call(
        functools.partial(scatter_kernel, plan, count),
        name="scatter_grads",
        out_shape=tuple(jax.ShapeDtypeStruct((h, D), jnp.float32) for h in heights)
        + (
            jax.ShapeDtypeStruct(buckets.shape, buckets.dtype),
            jax.ShapeDtypeStruct(vector.shape, vector.dtype),
        ),
        in_specs=[hbm] * (count + 2),
        out_specs=tuple([vmem] * count + [hbm, hbm]),
        scratch_shapes=scratch
        + [
            dma((total,)),
            dma((total,)),
            dma((len(plan),)),
            dma((2,)),
            dma((32,)),
            dma((32,)),
            dma((32,)),
            dma((32,)),
        ],
        compiler_params=pltpu.CompilerParams(
            collective_id=1, has_side_effects=True, vmem_limit_bytes=60 * 1024 * 1024
        ),
    )(*arrays, buckets, vector)


def sum_kernel(values, out, landed, total, send, recv, send_again, recv_again):
    n = 32
    me = my_rank()
    enter(n)
    exchange_start(values, landed, send, recv, n)
    landed[me] = values[me]
    exchange_wait(values, landed, send, recv, n)

    def add(index, carry):
        return carry + landed[index]

    total[...] = lax.fori_loop(0, n, add, jnp.zeros(total.shape, jnp.float32))
    out[me] = total[...]

    def copy(step):
        target = (me + step) % n
        return pltpu.make_async_remote_copy(
            src_ref=total,
            dst_ref=out.at[me],
            send_sem=send_again.at[step],
            recv_sem=recv_again.at[step],
            device_id=by_rank(target),
            device_id_type=MESH,
        )

    def begin(step, carry):
        copy(step).start()
        return carry

    def finish(step, carry):
        copy(step).wait()
        return carry

    lax.fori_loop(1, n, begin, 0)
    lax.fori_loop(1, n, finish, 0)


def sum_over_devices(flat):
    n = lax.axis_size(BOTH)
    if not special():
        return lax.psum(flat, BOTH)
    unit = n * 128
    lines = -(-flat.shape[0] // unit)
    values = jnp.pad(flat, (0, lines * unit - flat.shape[0])).reshape(n, lines, 128)
    vmem = pl.BlockSpec(memory_space=pltpu.VMEM)
    dma = pltpu.SemaphoreType.DMA
    result = pl.pallas_call(
        sum_kernel,
        name="sum_over_devices",
        out_shape=jax.ShapeDtypeStruct(values.shape, jnp.float32),
        in_specs=[vmem],
        out_specs=vmem,
        scratch_shapes=[
            pltpu.VMEM(values.shape, jnp.float32),
            pltpu.VMEM(values.shape[1:], jnp.float32),
            dma((n,)),
            dma((n,)),
            dma((n,)),
            dma((n,)),
        ],
        compiler_params=pltpu.CompilerParams(collective_id=2, has_side_effects=True),
    )(values)
    return result.reshape(-1)[: flat.shape[0]]


def special():
    return lax.axis_size("fsdp") == 16 and lax.axis_size("dp") == 2


def swap(blocks):
    shape = blocks.shape
    n_fsdp, n_dp = lax.axis_size("fsdp"), lax.axis_size("dp")
    split = blocks.reshape((n_fsdp, n_dp) + shape[1:])
    half = lax.all_to_all(split, "fsdp", split_axis=0, concat_axis=0, tiled=True)
    return lax.all_to_all(half, "dp", split_axis=1, concat_axis=1, tiled=True).reshape(shape)

def gather_blocks(arrays, found):
    if special():
        gathered = gather_weights(arrays, found)
        return [g.reshape((-1, a.shape[-1])) for g, a in zip(gathered, arrays)], gathered[-1]
    full = [lax.all_gather(a, BOTH, axis=0, tiled=True) for a in arrays]
    return full, swap(found)


def reduce_blocks(grads, buckets, vector):
    n = lax.axis_size(BOTH)
    if special():
        blocks = [g.astype(LOW).reshape(4, 2, 2, 2, -1, g.shape[-1]) for g in grads]
        shaped = vector.reshape(n, -1, 128)
        *parts, arrived, pieces = scatter_grads(blocks, buckets, shaped)
        return parts, arrived, jnp.sum(pieces, axis=0).reshape(-1)
    parts = [
        lax.psum_scatter(g.astype(jnp.float32), BOTH, scatter_dimension=0, tiled=True)
        for g in grads
    ]
    return (
        parts,
        swap(buckets),
        lax.psum_scatter(vector, BOTH, scatter_dimension=0, tiled=True),
    )


def factor_stats(gradient, rows_new):
    square = gradient * gradient
    return jnp.sum(square + tiny_square, axis=0), jnp.sum(square / rows_new[:, None], axis=0)


def clip_of(weighted, cols_new, mean_rows, size):
    mean_square = jnp.sum(weighted / cols_new, axis=-1) * mean_rows / size
    return jnp.maximum(1.0, jnp.sqrt(mean_square))


def local(
    token_ids,
    labels,
    loss_mask,
    batch_of,
    layer_in,
    layer_down,
    word_table,
    side_mat,
    vectors,
    in_rows,
    in_cols,
    down_rows,
    down_cols,
    word_rows,
    word_cols,
    side_rows,
    side_cols,
    vec_moment,
):
    seq_dev, length = token_ids.shape
    tokens = seq_dev * length
    n_blocks = lax.axis_size(BOTH)
    my_index = lax.axis_index(BOTH)
    mask_float = loss_mask.astype(jnp.float32)
    member = batch_of[:, None] == jnp.arange(MICRO)[None, :]
    local_counts = jnp.sum(member * jnp.sum(loss_mask, axis=1)[:, None], axis=0)
    block_rows = word_table.shape[0]
    capacity = max(2, 2 * tokens // n_blocks)
    flat_ids = token_ids.reshape(tokens)
    blocks = flat_ids // block_rows
    onehot = (blocks[:, None] == jnp.arange(n_blocks)[None, :]).astype(jnp.int32)
    rank = jnp.sum(jnp.cumsum(onehot, axis=0) * onehot, axis=1) - 1
    slot = blocks * capacity + rank
    bucket_ids = jnp.full((n_blocks * capacity,), -1, jnp.int32).at[slot].set(flat_ids)
    message = jnp.concatenate(
        [
            bucket_ids.reshape(n_blocks, capacity),
            jnp.broadcast_to(local_counts.astype(jnp.int32)[None, :], (n_blocks, MICRO)),
        ],
        axis=1,
    )
    answer = swap(message)
    asked = answer[:, :capacity].reshape(-1)
    counts = jnp.sum(answer[:, capacity:], axis=0).astype(jnp.float32)
    asked_row = jnp.where(asked >= 0, asked - my_index * block_rows, -1)
    found = jnp.take(
        word_table.astype(LOW), jnp.clip(asked_row, 0, block_rows - 1), axis=0
    ).reshape(n_blocks, capacity, D)
    seq_count = jnp.sum(member * counts[None, :], axis=1)
    token_weight = (mask_float / (seq_count * MICRO)[:, None]).reshape(tokens)
    label_float = labels.astype(jnp.float32).reshape(tokens)

    side_rows_local = side_mat.shape[0]
    vec_local = vectors.shape[0]
    vector_row = jnp.pad(vectors.astype(LOW).reshape(1, -1), ((0, 15), (0, D - vec_local)))
    (side_all, weight_in, weight_down), returned = gather_blocks(
        [
            jnp.concatenate([side_mat.astype(LOW), vector_row], axis=0),
            layer_in[0].astype(LOW).T,
            layer_down[0].astype(LOW),
        ],
        found,
    )
    side_all = side_all.reshape(n_blocks, side_rows_local + 16, D)
    side_full = side_all[:, :side_rows_local].reshape(-1, D)
    vector_full = side_all[:, side_rows_local, :vec_local].reshape(-1)
    all_vectors = vector_full.astype(jnp.float32)
    pos_rows = side_full[:SEQ_LEN].astype(jnp.float32)
    head_mat = side_full[SEQ_LEN:]
    global_offset = LAYERS * (8 * D + FF)
    gain_emb = all_vectors[global_offset : global_offset + D]
    shift_emb = all_vectors[global_offset + D : global_offset + 2 * D]
    head_bias = all_vectors[global_offset + 2 * D : global_offset + 3 * D]
    predictor = all_vectors[global_offset + 3 * D : global_offset + 4 * D]
    predictor_low = vector_full[global_offset + 3 * D : global_offset + 4 * D]
    to_slot = (slot[:, None] == jnp.arange(n_blocks * capacity)[None, :]).astype(LOW)
    own_rows = multiply(to_slot, returned.reshape(n_blocks * capacity, D))
    embedded = (own_rows.reshape(seq_dev, length, D) + pos_rows[None, :, :]).reshape(tokens, D)
    hidden = layer_norm(embedded, gain_emb, shift_emb)
    pieces = layer_slices(all_vectors, 0)
    hidden, kept = layer_forward(hidden, weight_in, weight_down, pieces, seq_dev)
    final_low = hidden.astype(LOW)
    head_pre = multiply(final_low, head_mat) + head_bias
    head_act_low = exact_gelu(head_pre).astype(LOW)
    logits = multiply(head_act_low, predictor_low)
    local_loss = jnp.sum(token_weight * (jax.nn.softplus(logits) - label_float * logits))
    d_logits = token_weight * (jax.nn.sigmoid(logits) - label_float)
    d_predictor = jnp.sum(d_logits[:, None] * head_act_low.astype(jnp.float32), axis=0)
    d_head_low = gelu_back(head_pre, d_logits[:, None] * predictor[None, :]).astype(LOW)
    grad_head = multiply_left(final_low, d_head_low)
    d_head_bias = jnp.sum(d_head_low.astype(jnp.float32), axis=0)
    d_hidden = multiply_right(d_head_low, head_mat)
    d_hidden, grads_in, grad_down, grad_pieces = layer_backward(
        d_hidden, weight_in, weight_down, pieces, kept, seq_dev
    )
    d_embedded, d_gain_emb, d_shift_emb = norm_back(embedded, gain_emb, shift_emb, d_hidden)
    grad_pos = jnp.sum(d_embedded.reshape(seq_dev, length, D), axis=0)
    grad_vector = jnp.concatenate([grad_pieces, d_gain_emb, d_shift_emb, d_head_bias, d_predictor])
    buckets = (
        multiply_left(to_slot, d_embedded.astype(LOW))
        .astype(LOW)
        .reshape(n_blocks, capacity, D)
    )
    kind = LOW if special() else jnp.float32
    (grad_side, grad_in_t, grad_down), arrived, grad_vec = reduce_blocks(
        [
            jnp.concatenate([grad_pos.astype(kind), grad_head.astype(kind)], axis=0),
            jnp.concatenate([g.astype(kind) for g in grads_in], axis=0),
            grad_down,
        ],
        buckets,
        grad_vector,
    )
    from_slot = (asked_row[None, :] == jnp.arange(block_rows)[:, None]).astype(LOW)
    grad_word = multiply(from_slot, arrived.reshape(n_blocks * capacity, D))
    grad_in = grad_in_t.T

    col_local = layer_in.shape[2]
    col_global = my_index * col_local + jnp.arange(col_local)
    sub_cols = jnp.stack(
        [col_global < 3 * D, (col_global >= 3 * D) & (col_global < 4 * D), col_global >= 4 * D]
    ).astype(jnp.float32)
    sub_width = jnp.array([3 * D, D, FF], jnp.float32)
    square_in = grad_in * grad_in
    in_cols_new = decay_rate * in_cols[0] + (1.0 - decay_rate) * jnp.mean(
        square_in + tiny_square, axis=0
    )
    row_part_in = jnp.stack(
        [jnp.sum((square_in + tiny_square) * pick[None, :], axis=1) for pick in sub_cols]
    )
    row_weighted_in = jnp.stack(
        [jnp.sum(square_in * (pick / in_cols_new)[None, :], axis=1) for pick in sub_cols]
    )

    def rows_of(gradient, rows_old):
        return decay_rate * rows_old + (1.0 - decay_rate) * jnp.mean(
            gradient * gradient + tiny_square, axis=1
        )

    rows_new_down = rows_of(grad_down, down_rows[0])
    col_down, weighted_down = factor_stats(grad_down, rows_new_down)
    rows_new_word = rows_of(grad_word, word_rows)
    col_word, weighted_word = factor_stats(grad_word, rows_new_word)
    row_global = my_index * side_rows_local + jnp.arange(side_rows_local)
    is_pos = row_global < SEQ_LEN
    which = jnp.stack([is_pos, jnp.logical_not(is_pos)]).astype(jnp.float32)
    side_counts = jnp.array([SEQ_LEN, D], jnp.float32)
    rows_new_side = rows_of(grad_side, side_rows)
    square_side = grad_side * grad_side
    col_side = jnp.stack(
        [jnp.sum((square_side + tiny_square) * pick[:, None], axis=0) for pick in which]
    )
    weighted_side = jnp.stack(
        [jnp.sum(square_side * (pick / rows_new_side)[:, None], axis=0) for pick in which]
    )
    total_side = jnp.sum(which * rows_new_side[None, :], axis=1)
    seg_onehot = (
        segment_index(my_index * vec_local + jnp.arange(vec_local))[:, None]
        == jnp.arange(9 * LAYERS + 4)[None, :]
    )
    new_moment = decay_rate * vec_moment + (1.0 - decay_rate) * (grad_vec * grad_vec + tiny_square)
    vec_update = grad_vec * lax.rsqrt(new_moment)
    seg_part = jnp.sum(jnp.where(seg_onehot, (vec_update * vec_update)[:, None], 0.0), axis=0)
    parts = [
        row_part_in,
        row_weighted_in,
        col_down,
        weighted_down,
        col_word,
        weighted_word,
        col_side,
        weighted_side,
        total_side,
        jnp.sum(rows_new_down)[None],
        jnp.sum(rows_new_word)[None],
        seg_part,
        local_loss[None],
    ]
    summed = sum_over_devices(jnp.concatenate([p.reshape(-1) for p in parts]))
    sums, offset = [], 0
    for p in parts:
        sums.append(summed[offset : offset + p.size].reshape(p.shape))
        offset += p.size
    (
        row_sum_in,
        row_weighted_in,
        col_down,
        weighted_down,
        col_word,
        weighted_word,
        col_side,
        weighted_side,
        total_side,
        total_down,
        total_word,
        seg_squares,
        loss_total,
    ) = sums
    half = 1.0 - decay_rate
    rows_new_in = decay_rate * in_rows[0] + half * row_sum_in / sub_width[:, None]
    mean_in = jnp.mean(rows_new_in, axis=1)
    scale_in = clip_of(row_weighted_in, rows_new_in, mean_in, D * sub_width)

    def choose(options):
        return jnp.sum(sub_cols[:, None, :] * options[:, :, None], axis=0)

    row_sel_in = choose(rows_new_in)
    factor_in = jnp.sum(sub_cols * (learn_rate / scale_in)[:, None], axis=0)
    mean_sel_in = jnp.sum(sub_cols * mean_in[:, None], axis=0)
    new_in = layer_in[0] - factor_in[None, :] * grad_in * lax.rsqrt(
        row_sel_in * in_cols_new[None, :] / mean_sel_in[None, :]
    )
    cols_new_down = decay_rate * down_cols[0] + half * col_down / FF
    mean_down = total_down[0] / FF
    scale_down = clip_of(weighted_down, cols_new_down, mean_down, FF * D)
    new_down = layer_down[0] - (learn_rate / scale_down) * grad_down * lax.rsqrt(
        rows_new_down[:, None] * cols_new_down[None, :] / mean_down
    )
    cols_new_word = decay_rate * word_cols + half * col_word / VOCAB
    mean_word = total_word[0] / VOCAB
    scale_word = clip_of(weighted_word, cols_new_word, mean_word, VOCAB * D)
    new_word = word_table - (learn_rate / scale_word) * grad_word * lax.rsqrt(
        rows_new_word[:, None] * cols_new_word[None, :] / mean_word
    )
    cols_new_side = decay_rate * side_cols + half * col_side / side_counts[:, None]
    mean_side = total_side / side_counts
    scale_side = clip_of(weighted_side, cols_new_side, mean_side, side_counts * D)
    col_sel_side = jnp.where(is_pos[:, None], cols_new_side[0][None, :], cols_new_side[1][None, :])
    mean_sel_side = jnp.where(is_pos, mean_side[0], mean_side[1])
    factor_side = learn_rate / jnp.where(is_pos, scale_side[0], scale_side[1])
    new_side = side_mat - factor_side[:, None] * grad_side * lax.rsqrt(
        rows_new_side[:, None] * col_sel_side / mean_sel_side[:, None]
    )
    seg_scale = jnp.maximum(1.0, jnp.sqrt(seg_squares / segment_sizes()))
    vec_scale = jnp.sum(jnp.where(seg_onehot, seg_scale[None, :], 0.0), axis=1)
    new_vectors = vectors - learn_rate * vec_update / vec_scale
    return (
        loss_total[0],
        new_in[None],
        rows_new_in[None],
        in_cols_new[None],
        new_in.astype(LOW)[None],
        new_down[None],
        rows_new_down[None],
        cols_new_down[None],
        new_down.astype(LOW)[None],
        new_word,
        rows_new_word,
        cols_new_word,
        new_word.astype(LOW),
        new_side,
        rows_new_side,
        cols_new_side,
        new_side.astype(LOW),
        new_vectors,
        new_moment,
        new_vectors.astype(LOW),
    )


def solution(mesh):
    return jax.shard_map(
        local,
        mesh=mesh,
        in_specs=(
            P(("fsdp", "dp"), None),
            P(("fsdp", "dp"), None),
            P(("fsdp", "dp"), None),
            P(("fsdp", "dp")),
            P(None, None, ("fsdp", "dp")),
            P(None, ("fsdp", "dp"), None),
            P(("fsdp", "dp"), None),
            P(("fsdp", "dp"), None),
            P(("fsdp", "dp")),
            P(),
            P(None, ("fsdp", "dp")),
            P(None, ("fsdp", "dp")),
            P(),
            P(("fsdp", "dp")),
            P(),
            P(("fsdp", "dp")),
            P(),
            P(("fsdp", "dp")),
        ),
        out_specs=(
            P(),
            P(None, None, ("fsdp", "dp")),
            P(),
            P(None, ("fsdp", "dp")),
            P(None, None, ("fsdp", "dp")),
            P(None, ("fsdp", "dp"), None),
            P(None, ("fsdp", "dp")),
            P(),
            P(None, ("fsdp", "dp"), None),
            P(("fsdp", "dp"), None),
            P(("fsdp", "dp")),
            P(),
            P(("fsdp", "dp"), None),
            P(("fsdp", "dp"), None),
            P(("fsdp", "dp")),
            P(),
            P(("fsdp", "dp"), None),
            P(("fsdp", "dp")),
            P(("fsdp", "dp")),
            P(("fsdp", "dp")),
        ),
        check_vma=False,
    )
```

```python
import functools
import math

import jax
import jax.numpy as jnp
from jax import lax
from jax.experimental import pallas as pl
from jax.experimental.pallas import tpu as pltpu
from jax.sharding import PartitionSpec as P

D = 1024
HEADS = 16
HEAD_DIM = 64
FF = 4096
VOCAB = 30720
SEQ_LEN = 512
LAYERS = 1
MICRO = 2
BOTH = ("fsdp", "dp")
LOW = jnp.bfloat16
MESH = pl.DeviceIdType.MESH
ALL = slice(None)


learn_rate = 0.02
decay_rate = 0.5
tiny_square = 1e-30
norm_epsilon = 1e-12
precise = lax.Precision.HIGHEST


def layer_norm(inputs, norm_gain, norm_shift):
    center = inputs - jnp.mean(inputs, axis=-1, keepdims=True)
    spread = jnp.mean(center * center, axis=-1, keepdims=True)
    return center * lax.rsqrt(spread + norm_epsilon) * norm_gain + norm_shift


def norm_back(inputs, norm_gain, norm_shift, cotangent):
    result, pull = jax.vjp(layer_norm, inputs, norm_gain, norm_shift)
    return pull(cotangent)


def exact_gelu(inputs):
    return jax.nn.gelu(inputs, approximate=False)


def gelu_back(inputs, cotangent):
    result, pull = jax.vjp(exact_gelu, inputs)
    return pull(cotangent)[0]


def multiply(left_side, right_side):
    return jnp.dot(left_side, right_side, preferred_element_type=jnp.float32)


def multiply_left(left_side, right_side):
    return lax.dot_general(
        left_side, right_side, (((0,), (0,)), ((), ())), preferred_element_type=jnp.float32
    )


def multiply_right(left_side, right_side):
    return lax.dot_general(
        left_side, right_side, (((1,), (1,)), ((), ())), preferred_element_type=jnp.float32
    )


def piece_bounds():
    return [0, D, 2 * D, 3 * D, 4 * D, 5 * D, 5 * D + FF, 6 * D + FF, 7 * D + FF, 8 * D + FF]


def layer_slices(all_vectors, layer_index):
    bounds = piece_bounds()
    offset = layer_index * (8 * D + FF)
    return [
        all_vectors[offset + bounds[slot_index] : offset + bounds[slot_index + 1]]
        for slot_index in range(9)
    ]


def segment_index(position):
    piece_width = 8 * D + FF
    inner = position % piece_width
    layer_of = position // piece_width
    bounds = piece_bounds()[1:-1]
    local_segment = sum(((inner >= bound).astype(jnp.int32) for bound in bounds))
    tail = 9 * LAYERS + (position - LAYERS * piece_width) // D
    return jnp.where(position < LAYERS * piece_width, 9 * layer_of + local_segment, tail)


def segment_sizes():
    sizes = []
    sizes = sizes + [D, D, D, D, D, FF, D, D, D]
    return jnp.array(sizes + [D, D, D, D], jnp.float32)


def attend(queries, key_rows, values):
    scores = jnp.einsum(
        "qhe,khe->hqk", queries, key_rows, preferred_element_type=jnp.float32
    ) * HEAD_DIM ** (-0.5)
    peak_score = jnp.max(scores, axis=-1, keepdims=True)
    exponent = jnp.exp(scores - peak_score)
    running = jnp.sum(exponent, axis=-1, keepdims=True)
    soft_probs = exponent / running
    context = jnp.einsum(
        "hqk,khe->qhe", soft_probs.astype(jnp.bfloat16), values, preferred_element_type=jnp.float32
    )
    return (context, peak_score + jnp.log(running))


def attend_back(queries, key_rows, values, log_total, d_context):
    score_scale = HEAD_DIM ** (-0.5)
    scores = (
        jnp.einsum("qhe,khe->hqk", queries, key_rows, preferred_element_type=jnp.float32)
        * score_scale
    )
    soft_probs = jnp.exp(scores - log_total)
    d_values = jnp.einsum(
        "hqk,qhe->khe",
        soft_probs.astype(jnp.bfloat16),
        d_context,
        preferred_element_type=jnp.float32,
    )
    d_probs = jnp.einsum("qhe,khe->hqk", d_context, values, preferred_element_type=jnp.float32)
    d_scores = soft_probs * (d_probs - jnp.sum(d_probs * soft_probs, axis=-1, keepdims=True))
    d_scores_low = d_scores.astype(jnp.bfloat16)
    d_queries = (
        jnp.einsum("hqk,khe->qhe", d_scores_low, key_rows, preferred_element_type=jnp.float32)
        * score_scale
    )
    d_keys = (
        jnp.einsum("hqk,qhe->khe", d_scores_low, queries, preferred_element_type=jnp.float32)
        * score_scale
    )
    return jnp.stack([d_queries, d_keys, d_values], axis=1)


def layer_forward(hidden, weight_in, weight_down, pieces, seq_dev):
    bias_q, bias_v, bias_o, gain_a, shift_a, bias_up, bias_down, gain_b, shift_b = pieces
    tokens = hidden.shape[0]
    length = tokens // seq_dev
    hidden_low = hidden.astype(jnp.bfloat16)
    joint_bias = jnp.concatenate([bias_q, jnp.zeros_like(bias_q), bias_v])
    projected = (multiply_right(hidden_low, weight_in[: 3 * D]) + joint_bias).astype(jnp.bfloat16)
    heads_view = projected.reshape(seq_dev, length, 3, HEADS, HEAD_DIM)
    context, log_total = jax.vmap(attend)(
        heads_view[:, :, 0], heads_view[:, :, 1], heads_view[:, :, 2]
    )
    context_low = context.reshape(tokens, D).astype(jnp.bfloat16)
    mid_in = hidden + (multiply_right(context_low, weight_in[3 * D : 4 * D]) + bias_o)
    middle = layer_norm(mid_in, gain_a, shift_a)
    middle_low = middle.astype(jnp.bfloat16)
    lifted = multiply_right(weight_in[4 * D :], middle_low) + bias_up[:, None]
    active_low = exact_gelu(lifted).astype(jnp.bfloat16)
    out_in = middle + (multiply_left(active_low, weight_down) + bias_down)
    output = layer_norm(out_in, gain_b, shift_b)
    return (
        output,
        (
            hidden_low,
            projected,
            log_total,
            context_low,
            mid_in,
            middle_low,
            lifted,
            active_low,
            out_in,
        ),
    )


def layer_backward(grad_out, weight_in, weight_down, pieces, kept, seq_dev):
    bias_q, bias_v, bias_o, gain_a, shift_a, bias_up, bias_down, gain_b, shift_b = pieces
    (
        hidden_low,
        projected,
        log_total,
        context_low,
        mid_in,
        middle_low,
        lifted,
        active_low,
        out_in,
    ) = kept
    tokens = mid_in.shape[0]
    length = tokens // seq_dev
    d_out_in, d_gain_b, d_shift_b = norm_back(out_in, gain_b, shift_b, grad_out)
    d_down_low = d_out_in.astype(jnp.bfloat16)
    d_lifted_low = gelu_back(lifted, multiply_right(weight_down, d_down_low)).astype(jnp.bfloat16)
    d_middle = d_out_in + multiply_left(d_lifted_low, weight_in[4 * D :])
    d_mid_in, d_gain_a, d_shift_a = norm_back(mid_in, gain_a, shift_a, d_middle)
    d_attended_low = d_mid_in.astype(jnp.bfloat16)
    d_context_low = multiply(d_attended_low, weight_in[3 * D : 4 * D]).astype(jnp.bfloat16)
    heads_view = projected.reshape(seq_dev, length, 3, HEADS, HEAD_DIM)
    d_heads = jax.vmap(attend_back)(
        heads_view[:, :, 0],
        heads_view[:, :, 1],
        heads_view[:, :, 2],
        log_total,
        d_context_low.reshape(seq_dev, length, HEADS, HEAD_DIM),
    )
    d_projected_low = d_heads.reshape(tokens, 3 * D).astype(jnp.bfloat16)
    d_hidden = d_mid_in + multiply(d_projected_low, weight_in[: 3 * D])
    joint_sums = jnp.sum(d_projected_low.astype(jnp.float32), axis=0)
    grad_pieces = jnp.concatenate(
        [
            joint_sums[:D],
            joint_sums[2 * D :],
            jnp.sum(d_attended_low.astype(jnp.float32), axis=0),
            d_gain_a,
            d_shift_a,
            jnp.sum(d_lifted_low.astype(jnp.float32), axis=1),
            jnp.sum(d_down_low.astype(jnp.float32), axis=0),
            d_gain_b,
            d_shift_b,
        ]
    )
    return (
        d_hidden,
        (
            active_low,
            d_down_low,
            d_lifted_low,
            middle_low,
            d_projected_low.T,
            hidden_low,
            d_attended_low.T,
            context_low,
        ),
        grad_pieces,
    )


def place():
    block = lax.axis_index("fsdp")
    return block // 4, (block // 2) % 2, block % 2, lax.axis_index("dp")


def device(z, y, x, c):
    return ((z * 2 + y) * 2 + x, c)


def my_rank():
    return lax.axis_index("fsdp") * 2 + lax.axis_index("dp")


def by_rank(index):
    return (index // 2, index % 2)


def neighbours(z, y, x, c):
    return (
        device(z, y, 1 - x, c),
        device(z, 1 - y, x, c),
        device(z, y, x, 1 - c),
        [device((z + k) % 4, y, x, c) for k in (1, 2, 3)],
    )


def greet(n):
    me = my_rank()
    barrier = pltpu.get_barrier_semaphore()

    def one(step, carry):
        pl.semaphore_signal(
            barrier, inc=1, device_id=by_rank((me + step) % n), device_id_type=MESH
        )
        return carry

    lax.fori_loop(1, n, one, 0)


def welcome(n):
    pl.semaphore_wait(pltpu.get_barrier_semaphore(), n - 1)


def enter(n):
    greet(n)
    welcome(n)


class Copies:
    def __init__(self, send, recv):
        self.send, self.recv, self.begun, self.count = send, recv, {}, 0

    def start(self, src, dst, target):
        slot = self.count
        self.count += 1
        copy = pltpu.make_async_remote_copy(
            src_ref=src,
            dst_ref=dst,
            send_sem=self.send.at[slot],
            recv_sem=self.recv.at[slot],
            device_id=target,
            device_id_type=MESH,
        )
        copy.start()
        self.begun[id(copy)] = copy
        return copy

    def sent(self, copy):
        self.begun.pop(id(copy)).wait_send()

    def drain(self):
        for copy in self.begun.values():
            copy.wait_send()


def exchange_copy(src, dst, send, recv, step, n):
    me = my_rank()
    target = (me + step) % n
    return pltpu.make_async_remote_copy(
        src_ref=src.at[target],
        dst_ref=dst.at[me],
        send_sem=send.at[step],
        recv_sem=recv.at[step],
        device_id=by_rank(target),
        device_id_type=MESH,
    )


def exchange_start(src, dst, send, recv, n):
    def begin(step, carry):
        exchange_copy(src, dst, send, recv, step, n).start()
        return carry

    lax.fori_loop(1, n, begin, 0)


def exchange_wait(src, dst, send, recv, n):
    def finish(step, carry):
        exchange_copy(src, dst, send, recv, step, n).wait()
        return carry

    lax.fori_loop(1, n, finish, 0)


LEAD, LOOK = 3, 2
TILES = ((64,), (64, 64, 64), (64, 64))
PLANE = {1: 64}


def gather_steps(plan):
    first = [i for i, p in enumerate(plan) if p[3]]
    rest = [i for i, p in enumerate(plan) if not p[3]]
    order, task = first + rest[:LEAD] + first, 0
    for step in range(len(rest) + 4):
        if step + LEAD < len(rest):
            order.append(rest[step + LEAD])
        order += [rest[i] for i in range(min(step, len(rest) - 1), -1, -1) if step - i < 4]
        if step == LOOK:
            order += first
        if step >= LOOK and task < 4:
            task += 1
            order.append(-task)
    return order + first + first


def count_from(index, shape, axis):
    return lax.broadcasted_iota(jnp.int32, shape, axis) == index


def one_hot(mask):
    return jnp.where(mask, 1.0, 0.0).astype(LOW)


def fill_slots(blocks, values, tally, to_slot, message):
    n, capacity, lanes = message.shape
    tokens = blocks.shape[1]
    owner = blocks[...]
    member = count_from(owner, (n, tokens), 0)
    earlier = one_hot(
        lax.broadcasted_iota(jnp.int32, (tokens, tokens), 0)
        < lax.broadcasted_iota(jnp.int32, (tokens, tokens), 1)
    )
    ahead = multiply(one_hot(member), earlier)
    rank = jnp.sum(jnp.where(member, ahead, 0.0), axis=0, keepdims=True).astype(jnp.int32)
    slot = owner * capacity + rank
    to_slot[...] = one_hot(count_from(slot, (n * capacity, tokens), 0))
    listed = multiply(to_slot[...], values[...]) + tally[...]
    message[...] = listed.reshape(n, capacity, lanes)


def look_up(index, answer, table, from_slot, found):
    n, capacity, lanes = answer.shape
    group = n // 4
    part = pl.ds(index * group, group)
    wanted = answer[part].reshape(group * capacity, lanes)
    row = (wanted[:, 0:1] * 256.0 + wanted[:, 1:2]).astype(jnp.int32)
    row = jnp.where(wanted[:, 2:3] > 0.5, row, -1)
    hot = one_hot(count_from(row, (group * capacity, table.shape[0]), 1))
    from_slot[part] = hot.reshape(group, capacity, -1)
    found[part] = multiply(hot, table[...]).astype(LOW).reshape(group, capacity, -1)


def gather_kernel(plan, count, *refs):
    local = refs[:count]
    blocks, values, tally, table = refs[count : count + 4]
    out = refs[count + 4 : 2 * count + 4]
    rows, to_slot, from_slot, answer = refs[2 * count + 4 : 2 * count + 8]
    message, found, send, recv, own_sem, ask_send, ask_recv, row_send, row_recv = refs[
        2 * count + 8 :
    ]
    z, y, x, c = place()
    n = 32
    me = my_rank()
    greet(n)
    fill_slots(blocks, values, tally, to_slot, message)
    answer[me] = message[me]
    welcome(n)
    copies = Copies(send, recv)
    exchange_start(message, answer, ask_send, ask_recv, n)
    own = []
    for i in range(count):
        own.append(pltpu.make_async_copy(local[i], out[i].at[z, y, x, c], own_sem.at[i]))
        own[i].start()
    to_x, to_y, to_core, to_z = neighbours(z, y, x, c)

    def pass_on(ref, where, target):
        return copies.start(ref.at[where], ref.at[where], target)

    landed = set()

    def own_there(i):
        if i not in landed:
            own[i].wait()
            landed.add(i)

    def chunk(i, start, size, plane_first):
        ref, mine, half = out[i], local[i], size // 2
        part, low, high = pl.ds(start, size), pl.ds(start, half), pl.ds(start + half, half)
        last = []
        if not plane_first:
            along = [copies.start(mine.at[part], ref.at[z, y, x, c, part], t) for t in to_z]
            yield
            for copy in along:
                copy.wait_recv()
            own_there(i)
            first = pass_on(ref, (ALL, y, x, c, low), to_x)
            second = pass_on(ref, (ALL, y, x, c, high), to_y)
            last.append(pass_on(ref, (ALL, y, x, c, part), to_core))
            yield
            first.wait_recv()
            second.wait_recv()
            first = pass_on(ref, (ALL, y, ALL, c, low), to_y)
            second = pass_on(ref, (ALL, ALL, x, c, high), to_x)
            last.append(pass_on(ref, (ALL, y, 1 - x, c, low), to_core))
            last.append(pass_on(ref, (ALL, 1 - y, x, c, high), to_core))
            yield
            first.wait_recv()
            second.wait_recv()
            last.append(pass_on(ref, (ALL, 1 - y, ALL, c, low), to_core))
            last.append(pass_on(ref, (ALL, ALL, 1 - x, c, high), to_core))
        else:
            first = copies.start(mine.at[low], ref.at[z, y, x, c, low], to_x)
            second = copies.start(mine.at[high], ref.at[z, y, x, c, high], to_y)
            last.append(copies.start(mine.at[part], ref.at[z, y, x, c, part], to_core))
            yield
            first.wait_recv()
            second.wait_recv()
            own_there(i)
            first = pass_on(ref, (z, y, ALL, c, low), to_y)
            second = pass_on(ref, (z, ALL, x, c, high), to_x)
            last.append(pass_on(ref, (z, y, 1 - x, c, low), to_core))
            last.append(pass_on(ref, (z, 1 - y, x, c, high), to_core))
            yield
            first.wait_recv()
            second.wait_recv()
            along = [pass_on(ref, (z, ALL, ALL, c, part), t) for t in to_z]
            last.append(pass_on(ref, (z, 1 - y, ALL, c, low), to_core))
            last.append(pass_on(ref, (z, ALL, 1 - x, c, high), to_core))
            yield
            for k in (1, 2, 3):
                along[k - 1].wait_recv()
                last.append(pass_on(ref, ((z + 4 - k) % 4, ALL, ALL, c, part), to_core))
        yield
        for copy in last:
            copy.wait_recv()
        yield

    chunks = [chunk(*p) for p in plan]
    keep = pltpu.make_async_copy(found.at[me], rows.at[me], own_sem.at[count])
    for index in gather_steps(plan):
        if index >= 0:
            next(chunks[index], None)
            continue
        task = -index - 1
        if task == 0:
            exchange_wait(message, answer, ask_send, ask_recv, n)
        look_up(task, answer, table, from_slot, found)
        if task == 3:
            keep.start()
            exchange_start(found, rows, row_send, row_recv, n)
    exchange_wait(found, rows, row_send, row_recv, n)
    keep.wait()
    copies.drain()
    for i in range(count):
        own_there(i)


def gather_plan(heights):
    plan = []
    for i, height in enumerate(heights):
        start = 0
        if i in PLANE:
            plan.append((i, 0, PLANE[i], True))
            start = PLANE[i]
        for size in TILES[i]:
            plan.append((i, start, size, False))
            start += size
        assert start == height
    return plan


def gather_weights(arrays, blocks, values, tally, table):
    count = len(arrays)
    n, capacity = 32, 32
    tokens = blocks.shape[1]
    plan = gather_plan([a.shape[0] for a in arrays])
    total = sum(15 if p[3] else 12 for p in plan)
    hbm = pl.BlockSpec(memory_space=pl.ANY)
    vmem = pl.BlockSpec(memory_space=pltpu.VMEM)
    dma = pltpu.SemaphoreType.DMA
    shape = jax.ShapeDtypeStruct
    return pl.pallas_call(
        functools.partial(gather_kernel, plan, count),
        name="gather_weights",
        out_shape=tuple(shape((4, 2, 2, 2) + a.shape, a.dtype) for a in arrays)
        + (
            shape((n, capacity, D), LOW),
            shape((n * capacity, tokens), LOW),
            shape((n, capacity, table.shape[0]), LOW),
            shape((n, capacity, 128), jnp.float32),
        ),
        in_specs=[vmem] * (count + 4),
        out_specs=tuple([hbm] * (count + 1) + [vmem] * 3),
        scratch_shapes=[
            pltpu.VMEM((n, capacity, 128), jnp.float32),
            pltpu.VMEM((n, capacity, D), LOW),
            dma((total,)),
            dma((total,)),
            dma((count + 1,)),
        ]
        + [dma((n,))] * 4,
        compiler_params=pltpu.CompilerParams(collective_id=0, has_side_effects=True),
    )(*arrays, blocks, values, tally, table)


def add_blocks(dst, other, shape, at_dst, at_other):
    def body(index, carry):
        where = []
        for extent in reversed(shape):
            where.append(index % extent)
            index = index // extent
        where = tuple(reversed(where))
        d, o = at_dst(*where), at_other(*where)
        total = dst[d].astype(jnp.float32) + other[o].astype(jnp.float32)
        dst[d] = total.astype(dst.dtype)
        return carry

    lax.fori_loop(0, math.prod(shape), body, 0)


WIDE = 256


class Group:
    def __init__(self, z0, nz, height, sources, out):
        self.z0, self.nz, self.height, self.sources, self.out = z0, nz, height, sources, out

    def scratch(self):
        nz, h, n = self.nz, self.height, D // WIDE
        shapes = [(2, nz, 2, 2, h), (n, nz, 2, 2, h)] + [(n, nz, 2, h // 2)] * 2
        shapes += [(n, nz, h // 2)] * 2 + [(n, 3, h)]
        return [pltpu.VMEM(shape + (WIDE,), LOW) for shape in shapes]


def each_block(group, refs, wide, core, body):
    for start, stop, left, right, base, together in group.sources:
        def one(step, carry, left=left, right=right, base=base, together=together):
            index = step * together
            part = refs[left][pl.ds(index - base, together), core]
            product = multiply(part.reshape(-1, part.shape[-1]), refs[right][:, wide])
            product = product.reshape(together, group.height, WIDE)
            for k in range(together):
                at = index + k
                body((at // 4, (at // 2) % 2, at % 2), product[k])
            return carry

        lax.fori_loop(start // together, stop // together, one, 0)


def scatter_kernel(groups, n_left, *refs):
    operands = refs[:n_left]
    side, buckets, vector = refs[n_left : n_left + 3]
    out = refs[n_left + 3 : n_left + 6]
    arrived, vector_all = refs[n_left + 6 : n_left + 8]
    rest = refs[n_left + 8 :]
    scratch = [rest[7 * i : 7 * i + 7] for i in range(len(groups))]
    side_scratch = rest[7 * len(groups) : 7 * len(groups) + 7]
    (send, recv, z_send, z_recv, load, row_send, row_recv, vec_send, vec_recv) = rest[
        7 * len(groups) + 7 :
    ]
    z, y, x, c = place()
    n = 32
    me = my_rank()
    enter(n)
    copies = Copies(send, recv)
    to_x, to_y, to_core, to_z = neighbours(z, y, x, c)
    own = [
        pltpu.make_async_copy(buckets.at[me], arrived.at[me], load.at[0]),
        pltpu.make_async_copy(vector.at[me], vector_all.at[me], load.at[1]),
    ]
    for copy in own:
        copy.start()
    sent_before = {}

    def product_chunk(slot, which, index):
        group = groups[which]
        outgoing, held, low_1, high_1, low_2, high_2, from_z = scratch[which]
        nz, h = group.nz, group.height
        wide = pl.ds(index * WIDE, WIDE)
        low, high = pl.ds(0, h // 2), pl.ds(h // 2, h // 2)
        here = index % 2
        if index >= 2:
            copies.sent(sent_before[which, index - 2])

        def send_off(where, value):
            outgoing[(here,) + where] = value.astype(LOW)

        each_block(group, operands, wide, 1 - c, send_off)
        core = copies.start(outgoing.at[here], held.at[index], to_core)
        sent_before[which, index] = core
        yield
        core.wait_recv()

        def add_own(where, value):
            spot = (index,) + where
            held[spot] = (value + held[spot].astype(jnp.float32)).astype(LOW)

        each_block(group, operands, wide, c, add_own)
        first = copies.start(held.at[index, :, 1 - y, :, low], low_1.at[index], to_y)
        second = copies.start(held.at[index, :, :, 1 - x, high], high_1.at[index], to_x)
        yield
        first.wait_recv()
        second.wait_recv()
        add_blocks(
            held, low_1, (nz, 2), lambda a, d: (index, a, y, d, low), lambda a, d: (index, a, d)
        )
        add_blocks(
            held, high_1, (nz, 2), lambda a, b: (index, a, b, x, high), lambda a, b: (index, a, b)
        )
        first = copies.start(held.at[index, :, y, 1 - x, low], low_2.at[index], to_x)
        second = copies.start(held.at[index, :, 1 - y, x, high], high_2.at[index], to_y)
        yield
        first.wait_recv()
        second.wait_recv()
        add_blocks(held, low_2, (nz,), lambda a: (index, a, y, x, low), lambda a: (index, a))
        add_blocks(held, high_2, (nz,), lambda a: (index, a, y, x, high), lambda a: (index, a))

        def along(level, back):
            return pltpu.make_async_remote_copy(
                src_ref=held.at[index, level, y, x],
                dst_ref=from_z.at[index, back],
                send_sem=z_send.at[slot, level],
                recv_sem=z_recv.at[slot, back],
                device_id=device(group.z0 + level, y, x, c),
                device_id_type=MESH,
            )

        for level in range(nz):
            away = z != group.z0 + level

            @pl.when(away)
            def _(level=level):
                along(level, (z - group.z0 - level + 3) % 4).start()

        yield

        def finish():
            for back in range(3):
                along(0, back).wait_recv()
            mine = held[index, z - group.z0, y, x].astype(jnp.float32)
            for back in range(3):
                mine = mine + from_z[index, back].astype(jnp.float32)
            out[group.out][:, wide] = mine

        if nz == 4:
            finish()
        else:
            pl.when((z >= group.z0) & (z < group.z0 + nz))(finish)
        yield
        for level in range(nz):
            away = z != group.z0 + level

            @pl.when(away)
            def _(level=level):
                along(level, (z - group.z0 - level + 3) % 4).wait_send()

        yield

    def side_chunk():
        held, from_core, low_1, high_1, low_2, high_2, from_z = side_scratch
        size = held.shape[3]
        half = size // 32 * 16 + 16
        low, high = pl.ds(0, half), pl.ds(half, size - half)
        core = copies.start(side.at[:, :, :, 1 - c], from_core, to_core)
        mine = pltpu.make_async_copy(side.at[:, :, :, c], held, load.at[2])
        mine.start()
        yield
        mine.wait()
        core.wait_recv()
        add_blocks(held, from_core, (4, 2, 2), lambda *w: w, lambda *w: w)
        first = copies.start(held.at[:, 1 - y, :, low], low_1, to_y)
        second = copies.start(held.at[:, :, 1 - x, high], high_1, to_x)
        yield
        first.wait_recv()
        second.wait_recv()
        add_blocks(held, low_1, (4, 2), lambda a, d: (a, y, d, low), lambda a, d: (a, d))
        add_blocks(held, high_1, (4, 2), lambda a, b: (a, b, x, high), lambda a, b: (a, b))
        first = copies.start(held.at[:, y, 1 - x, low], low_2, to_x)
        second = copies.start(held.at[:, 1 - y, x, high], high_2, to_y)
        yield
        first.wait_recv()
        second.wait_recv()
        add_blocks(held, low_2, (4,), lambda a: (a, y, x, low), lambda a: (a,))
        add_blocks(held, high_2, (4,), lambda a: (a, y, x, high), lambda a: (a,))
        along = [
            copies.start(held.at[(z + k) % 4, y, x], from_z.at[k - 1], to_z[k - 1])
            for k in (1, 2, 3)
        ]
        yield
        for copy in along:
            copy.wait_recv()
        total = held[z, y, x].astype(jnp.float32)
        for k in range(3):
            total = total + from_z[k].astype(jnp.float32)
        out[2][...] = total
        yield
        yield

    parts = [(which, index) for index in range(D // WIDE) for which in ORDER]
    chunks = [side_chunk()] + [product_chunk(slot, *p) for slot, p in enumerate(parts)]
    exchange_start(vector, vector_all, vec_send, vec_recv, n)
    for step in range(len(chunks) + 5):
        for index in range(min(step, len(chunks) - 1), -1, -1):
            if step - index < 6:
                next(chunks[index], None)
        if step == ROWS_AT:
            exchange_start(buckets, arrived, row_send, row_recv, n)
    exchange_wait(vector, vector_all, vec_send, vec_recv, n)
    exchange_wait(buckets, arrived, row_send, row_recv, n)
    copies.drain()
    for copy in own:
        copy.wait()


ROWS_AT = 0
ORDER = (0, 1, 2)


def scatter_grads(pairs, side, buckets, vector):
    blocked = []
    for i, pair in enumerate(pairs):
        height = FF // 32 if i == 0 else 256
        blocked.append(pair if i % 2 else pair.reshape(-1, 2, height, pair.shape[1]))
    groups = [
        Group(0, 4, FF // 32, [(0, 16, 0, 1, 0, 2)], 1),
        Group(2, 2, 256, [(0, 8, 2, 3, 0, 1)], 0),
        Group(0, 2, 256, [(0, 6, 4, 5, 0, 1), (6, 8, 6, 7, 6, 1)], 0),
    ]
    height = side.shape[4]
    half = height // 32 * 16 + 16
    hbm = pl.BlockSpec(memory_space=pl.ANY)
    vmem = pl.BlockSpec(memory_space=pltpu.VMEM)
    dma = pltpu.SemaphoreType.DMA
    scratch = [shape for group in groups for shape in group.scratch()]
    for lead in (
        (4, 2, 2, height),
        (4, 2, 2, height),
        (4, 2, half),
        (4, 2, height - half),
        (4, half),
        (4, height - half),
        (3, height),
    ):
        scratch.append(pltpu.VMEM(lead + (D,), LOW))
    chunks = len(groups) * D // WIDE
    total = 5 * chunks + 8
    shape = jax.ShapeDtypeStruct
    return pl.pallas_call(
        functools.partial(scatter_kernel, groups, len(pairs)),
        name="scatter_grads",
        out_shape=(
            shape((256, D), jnp.float32),
            shape((FF // 32, D), jnp.float32),
            shape((height, D), jnp.float32),
            shape(buckets.shape, buckets.dtype),
            shape(vector.shape, vector.dtype),
        ),
        in_specs=[vmem] * len(pairs) + [hbm] * 3,
        out_specs=(vmem, vmem, vmem, hbm, hbm),
        scratch_shapes=scratch
        + [
            dma((total,)),
            dma((total,)),
            dma((chunks, 4)),
            dma((chunks, 3)),
            dma((3,)),
        ]
        + [dma((32,))] * 4,
        compiler_params=pltpu.CompilerParams(
            collective_id=1, has_side_effects=True, vmem_limit_bytes=64000 * 1024
        ),
    )(*blocked, side, buckets, vector)


def sum_kernel(values, out, landed, total, send, recv, send_again, recv_again):
    n = 32
    me = my_rank()
    enter(n)
    exchange_start(values, landed, send, recv, n)
    landed[me] = values[me]
    exchange_wait(values, landed, send, recv, n)

    def add(index, carry):
        return carry + landed[index]

    total[...] = lax.fori_loop(0, n, add, jnp.zeros(total.shape, jnp.float32))
    out[me] = total[...]

    def copy(step):
        target = (me + step) % n
        return pltpu.make_async_remote_copy(
            src_ref=total,
            dst_ref=out.at[me],
            send_sem=send_again.at[step],
            recv_sem=recv_again.at[step],
            device_id=by_rank(target),
            device_id_type=MESH,
        )

    def begin(step, carry):
        copy(step).start()
        return carry

    def finish(step, carry):
        copy(step).wait()
        return carry

    lax.fori_loop(1, n, begin, 0)
    lax.fori_loop(1, n, finish, 0)


def sum_over_devices(flat):
    n = lax.axis_size(BOTH)
    if not special():
        return lax.psum(flat, BOTH)
    unit = n * 128
    lines = -(-flat.shape[0] // unit)
    values = jnp.pad(flat, (0, lines * unit - flat.shape[0])).reshape(n, lines, 128)
    vmem = pl.BlockSpec(memory_space=pltpu.VMEM)
    dma = pltpu.SemaphoreType.DMA
    result = pl.pallas_call(
        sum_kernel,
        name="sum_over_devices",
        out_shape=jax.ShapeDtypeStruct(values.shape, jnp.float32),
        in_specs=[vmem],
        out_specs=vmem,
        scratch_shapes=[
            pltpu.VMEM(values.shape, jnp.float32),
            pltpu.VMEM(values.shape[1:], jnp.float32),
            dma((n,)),
            dma((n,)),
            dma((n,)),
            dma((n,)),
        ],
        compiler_params=pltpu.CompilerParams(collective_id=2, has_side_effects=True),
    )(values)
    return result.reshape(-1)[: flat.shape[0]]


def special():
    return lax.axis_size("fsdp") == 16 and lax.axis_size("dp") == 2


def swap(blocks):
    shape = blocks.shape
    n_fsdp, n_dp = lax.axis_size("fsdp"), lax.axis_size("dp")
    split = blocks.reshape((n_fsdp, n_dp) + shape[1:])
    half = lax.all_to_all(split, "fsdp", split_axis=0, concat_axis=0, tiled=True)
    return lax.all_to_all(half, "dp", split_axis=1, concat_axis=1, tiled=True).reshape(shape)

def ask_rows(blocks, local_row, local_counts, block_rows, capacity):
    n = lax.axis_size(BOTH)
    onehot = (blocks[:, None] == jnp.arange(n)[None, :]).astype(jnp.int32)
    rank = jnp.sum(jnp.cumsum(onehot, axis=0) * onehot, axis=1) - 1
    slot = blocks * capacity + rank
    bucket_ids = jnp.full((n * capacity,), -1, jnp.int32).at[slot].set(local_row)
    message = jnp.concatenate(
        [
            bucket_ids.reshape(n, capacity),
            jnp.broadcast_to(local_counts[None, :], (n, MICRO)),
        ],
        axis=1,
    )
    answer = swap(message)
    asked = answer[:, :capacity].reshape(-1)
    to_slot = (jnp.arange(n * capacity)[:, None] == slot[None, :]).astype(LOW)
    from_slot = (asked[:, None] == jnp.arange(block_rows)[None, :]).astype(LOW)
    return to_slot, from_slot, jnp.sum(answer[:, capacity:], axis=0)


def gather_blocks(arrays, blocks, local_row, local_counts, table, capacity):
    n = lax.axis_size(BOTH)
    if special():
        row = local_row.astype(jnp.int32)
        values = jnp.stack([row // 256, row % 256, jnp.ones_like(row)], axis=1).astype(LOW)
        tally = jnp.pad(local_counts.astype(jnp.float32), (3, 125 - MICRO)).reshape(1, 128)
        *gathered, rows, to_slot, from_slot, answer = gather_weights(
            arrays, blocks.reshape(1, -1), jnp.pad(values, ((0, 0), (0, 125))), tally, table
        )
        full = [g.reshape((-1, a.shape[-1])) for g, a in zip(gathered, arrays)]
        counts = jnp.sum(answer[:, 0, 3 : 3 + MICRO], axis=0)
        return full, rows, to_slot, from_slot.reshape(n * capacity, -1), counts
    to_slot, from_slot, counts = ask_rows(
        blocks, local_row, local_counts, table.shape[0], capacity
    )
    found = multiply(from_slot, table).astype(LOW).reshape(n, capacity, D)
    full = [lax.all_gather(a, BOTH, axis=0, tiled=True) for a in arrays]
    return full, swap(found), to_slot, from_slot, counts.astype(jnp.float32)


def reduce_blocks(pairs, grad_pos, grad_head, buckets, vector):
    n = lax.axis_size(BOTH)
    if special():
        side = jnp.concatenate([grad_pos.astype(LOW), grad_head.astype(LOW)], axis=0)
        grad_in, grad_down, grad_side, arrived, pieces = scatter_grads(
            pairs, side.reshape(4, 2, 2, 2, -1, D), buckets, vector.reshape(n, -1, 128)
        )
        return grad_side, grad_in, grad_down, arrived, jnp.sum(pieces, axis=0).reshape(-1)
    down, up, joint, attended = [
        multiply(pairs[2 * i], pairs[2 * i + 1]) for i in range(4)
    ]

    def own(value):
        return lax.psum_scatter(value, BOTH, scatter_dimension=0, tiled=True)

    return (
        own(jnp.concatenate([grad_pos, grad_head], axis=0)),
        own(jnp.concatenate([joint, attended, up], axis=0)),
        own(down),
        swap(buckets),
        own(vector),
    )


def factor_stats(gradient, rows_new):
    square = gradient * gradient
    return jnp.sum(square + tiny_square, axis=0), jnp.sum(square / rows_new[:, None], axis=0)


def clip_of(weighted, cols_new, mean_rows, size):
    mean_square = jnp.sum(weighted / cols_new, axis=-1) * mean_rows / size
    return jnp.maximum(1.0, jnp.sqrt(mean_square))


def local(
    token_ids,
    labels,
    loss_mask,
    batch_of,
    layer_in,
    layer_down,
    word_table,
    side_mat,
    vectors,
    in_rows,
    in_cols,
    down_rows,
    down_cols,
    word_rows,
    word_cols,
    side_rows,
    side_cols,
    vec_moment,
):
    seq_dev, length = token_ids.shape
    tokens = seq_dev * length
    n_blocks = lax.axis_size(BOTH)
    my_index = lax.axis_index(BOTH)
    mask_float = loss_mask.astype(jnp.float32)
    member = batch_of[:, None] == jnp.arange(MICRO)[None, :]
    local_counts = jnp.sum(member * jnp.sum(loss_mask, axis=1)[:, None], axis=0)
    block_rows = word_table.shape[0]
    capacity = max(2, 2 * tokens // n_blocks)
    flat_ids = token_ids.reshape(tokens)
    blocks = flat_ids // block_rows
    label_float = labels.astype(jnp.float32).reshape(tokens)

    side_rows_local = side_mat.shape[0]
    vec_local = vectors.shape[0]
    vector_row = jnp.pad(vectors.astype(LOW).reshape(1, -1), ((0, 15), (0, D - vec_local)))
    (side_all, weight_in, weight_down), returned, to_slot, from_slot, counts = gather_blocks(
        [
            jnp.concatenate([side_mat.astype(LOW), vector_row], axis=0),
            layer_in[0].astype(LOW).T,
            layer_down[0].astype(LOW),
        ],
        blocks,
        flat_ids - blocks * block_rows,
        local_counts.astype(jnp.int32),
        word_table.astype(LOW),
        capacity,
    )
    seq_count = jnp.sum(member * counts[None, :], axis=1)
    token_weight = (mask_float / (seq_count * MICRO)[:, None]).reshape(tokens)
    side_all = side_all.reshape(n_blocks, side_rows_local + 16, D)
    side_full = side_all[:, :side_rows_local].reshape(-1, D)
    vector_full = side_all[:, side_rows_local, :vec_local].reshape(-1)
    all_vectors = vector_full.astype(jnp.float32)
    pos_rows = side_full[:SEQ_LEN].astype(jnp.float32)
    head_mat = side_full[SEQ_LEN:]
    global_offset = LAYERS * (8 * D + FF)
    gain_emb = all_vectors[global_offset : global_offset + D]
    shift_emb = all_vectors[global_offset + D : global_offset + 2 * D]
    head_bias = all_vectors[global_offset + 2 * D : global_offset + 3 * D]
    predictor = all_vectors[global_offset + 3 * D : global_offset + 4 * D]
    predictor_low = vector_full[global_offset + 3 * D : global_offset + 4 * D]
    own_rows = multiply_left(to_slot, returned.reshape(n_blocks * capacity, D))
    embedded = (own_rows.reshape(seq_dev, length, D) + pos_rows[None, :, :]).reshape(tokens, D)
    hidden = layer_norm(embedded, gain_emb, shift_emb)
    pieces = layer_slices(all_vectors, 0)
    hidden, kept = layer_forward(hidden, weight_in, weight_down, pieces, seq_dev)
    final_low = hidden.astype(LOW)
    head_pre = multiply(final_low, head_mat) + head_bias
    head_act_low = exact_gelu(head_pre).astype(LOW)
    logits = multiply(head_act_low, predictor_low)
    local_loss = jnp.sum(token_weight * (jax.nn.softplus(logits) - label_float * logits))
    d_logits = token_weight * (jax.nn.sigmoid(logits) - label_float)
    d_predictor = jnp.sum(d_logits[:, None] * head_act_low.astype(jnp.float32), axis=0)
    d_head_low = gelu_back(head_pre, d_logits[:, None] * predictor[None, :]).astype(LOW)
    grad_head = multiply_left(final_low, d_head_low)
    d_head_bias = jnp.sum(d_head_low.astype(jnp.float32), axis=0)
    d_hidden = multiply_right(d_head_low, head_mat)
    d_hidden, pairs, grad_pieces = layer_backward(
        d_hidden, weight_in, weight_down, pieces, kept, seq_dev
    )
    d_embedded, d_gain_emb, d_shift_emb = norm_back(embedded, gain_emb, shift_emb, d_hidden)
    grad_pos = jnp.sum(d_embedded.reshape(seq_dev, length, D), axis=0)
    grad_vector = jnp.concatenate([grad_pieces, d_gain_emb, d_shift_emb, d_head_bias, d_predictor])
    buckets = (
        multiply(to_slot, d_embedded.astype(LOW))
        .astype(LOW)
        .reshape(n_blocks, capacity, D)
    )
    grad_side, grad_in_t, grad_down, arrived, grad_vec = reduce_blocks(
        pairs, grad_pos, grad_head, buckets, grad_vector
    )
    grad_word = multiply_left(from_slot, arrived.reshape(n_blocks * capacity, D))
    grad_in = grad_in_t.T

    col_local = layer_in.shape[2]
    col_global = my_index * col_local + jnp.arange(col_local)
    sub_cols = jnp.stack(
        [col_global < 3 * D, (col_global >= 3 * D) & (col_global < 4 * D), col_global >= 4 * D]
    ).astype(jnp.float32)
    sub_width = jnp.array([3 * D, D, FF], jnp.float32)
    square_in = grad_in * grad_in
    in_cols_new = decay_rate * in_cols[0] + (1.0 - decay_rate) * jnp.mean(
        square_in + tiny_square, axis=0
    )
    row_part_in = jnp.stack(
        [jnp.sum((square_in + tiny_square) * pick[None, :], axis=1) for pick in sub_cols]
    )
    row_weighted_in = jnp.stack(
        [jnp.sum(square_in * (pick / in_cols_new)[None, :], axis=1) for pick in sub_cols]
    )

    def rows_of(gradient, rows_old):
        return decay_rate * rows_old + (1.0 - decay_rate) * jnp.mean(
            gradient * gradient + tiny_square, axis=1
        )

    rows_new_down = rows_of(grad_down, down_rows[0])
    col_down, weighted_down = factor_stats(grad_down, rows_new_down)
    rows_new_word = rows_of(grad_word, word_rows)
    col_word, weighted_word = factor_stats(grad_word, rows_new_word)
    row_global = my_index * side_rows_local + jnp.arange(side_rows_local)
    is_pos = row_global < SEQ_LEN
    which = jnp.stack([is_pos, jnp.logical_not(is_pos)]).astype(jnp.float32)
    side_counts = jnp.array([SEQ_LEN, D], jnp.float32)
    rows_new_side = rows_of(grad_side, side_rows)
    square_side = grad_side * grad_side
    col_side = jnp.stack(
        [jnp.sum((square_side + tiny_square) * pick[:, None], axis=0) for pick in which]
    )
    weighted_side = jnp.stack(
        [jnp.sum(square_side * (pick / rows_new_side)[:, None], axis=0) for pick in which]
    )
    total_side = jnp.sum(which * rows_new_side[None, :], axis=1)
    seg_onehot = (
        segment_index(my_index * vec_local + jnp.arange(vec_local))[:, None]
        == jnp.arange(9 * LAYERS + 4)[None, :]
    )
    new_moment = decay_rate * vec_moment + (1.0 - decay_rate) * (grad_vec * grad_vec + tiny_square)
    vec_update = grad_vec * lax.rsqrt(new_moment)
    seg_part = jnp.sum(jnp.where(seg_onehot, (vec_update * vec_update)[:, None], 0.0), axis=0)
    parts = [
        row_part_in,
        row_weighted_in,
        col_down,
        weighted_down,
        col_word,
        weighted_word,
        col_side,
        weighted_side,
        total_side,
        jnp.sum(rows_new_down)[None],
        jnp.sum(rows_new_word)[None],
        seg_part,
        local_loss[None],
    ]
    summed = sum_over_devices(jnp.concatenate([p.reshape(-1) for p in parts]))
    sums, offset = [], 0
    for p in parts:
        sums.append(summed[offset : offset + p.size].reshape(p.shape))
        offset += p.size
    (
        row_sum_in,
        row_weighted_in,
        col_down,
        weighted_down,
        col_word,
        weighted_word,
        col_side,
        weighted_side,
        total_side,
        total_down,
        total_word,
        seg_squares,
        loss_total,
    ) = sums
    half = 1.0 - decay_rate
    rows_new_in = decay_rate * in_rows[0] + half * row_sum_in / sub_width[:, None]
    mean_in = jnp.mean(rows_new_in, axis=1)
    scale_in = clip_of(row_weighted_in, rows_new_in, mean_in, D * sub_width)

    def choose(options):
        return jnp.sum(sub_cols[:, None, :] * options[:, :, None], axis=0)

    row_sel_in = choose(rows_new_in)
    factor_in = jnp.sum(sub_cols * (learn_rate / scale_in)[:, None], axis=0)
    mean_sel_in = jnp.sum(sub_cols * mean_in[:, None], axis=0)
    new_in = layer_in[0] - factor_in[None, :] * grad_in * lax.rsqrt(
        row_sel_in * in_cols_new[None, :] / mean_sel_in[None, :]
    )
    cols_new_down = decay_rate * down_cols[0] + half * col_down / FF
    mean_down = total_down[0] / FF
    scale_down = clip_of(weighted_down, cols_new_down, mean_down, FF * D)
    new_down = layer_down[0] - (learn_rate / scale_down) * grad_down * lax.rsqrt(
        rows_new_down[:, None] * cols_new_down[None, :] / mean_down
    )
    cols_new_word = decay_rate * word_cols + half * col_word / VOCAB
    mean_word = total_word[0] / VOCAB
    scale_word = clip_of(weighted_word, cols_new_word, mean_word, VOCAB * D)
    new_word = word_table - (learn_rate / scale_word) * grad_word * lax.rsqrt(
        rows_new_word[:, None] * cols_new_word[None, :] / mean_word
    )
    cols_new_side = decay_rate * side_cols + half * col_side / side_counts[:, None]
    mean_side = total_side / side_counts
    scale_side = clip_of(weighted_side, cols_new_side, mean_side, side_counts * D)
    col_sel_side = jnp.where(is_pos[:, None], cols_new_side[0][None, :], cols_new_side[1][None, :])
    mean_sel_side = jnp.where(is_pos, mean_side[0], mean_side[1])
    factor_side = learn_rate / jnp.where(is_pos, scale_side[0], scale_side[1])
    new_side = side_mat - factor_side[:, None] * grad_side * lax.rsqrt(
        rows_new_side[:, None] * col_sel_side / mean_sel_side[:, None]
    )
    seg_scale = jnp.maximum(1.0, jnp.sqrt(seg_squares / segment_sizes()))
    vec_scale = jnp.sum(jnp.where(seg_onehot, seg_scale[None, :], 0.0), axis=1)
    new_vectors = vectors - learn_rate * vec_update / vec_scale
    return (
        loss_total[0],
        new_in[None],
        rows_new_in[None],
        in_cols_new[None],
        new_in.astype(LOW)[None],
        new_down[None],
        rows_new_down[None],
        cols_new_down[None],
        new_down.astype(LOW)[None],
        new_word,
        rows_new_word,
        cols_new_word,
        new_word.astype(LOW),
        new_side,
        rows_new_side,
        cols_new_side,
        new_side.astype(LOW),
        new_vectors,
        new_moment,
        new_vectors.astype(LOW),
    )


def solution(mesh):
    return jax.shard_map(
        local,
        mesh=mesh,
        in_specs=(
            P(("fsdp", "dp"), None),
            P(("fsdp", "dp"), None),
            P(("fsdp", "dp"), None),
            P(("fsdp", "dp")),
            P(None, None, ("fsdp", "dp")),
            P(None, ("fsdp", "dp"), None),
            P(("fsdp", "dp"), None),
            P(("fsdp", "dp"), None),
            P(("fsdp", "dp")),
            P(),
            P(None, ("fsdp", "dp")),
            P(None, ("fsdp", "dp")),
            P(),
            P(("fsdp", "dp")),
            P(),
            P(("fsdp", "dp")),
            P(),
            P(("fsdp", "dp")),
        ),
        out_specs=(
            P(),
            P(None, None, ("fsdp", "dp")),
            P(),
            P(None, ("fsdp", "dp")),
            P(None, None, ("fsdp", "dp")),
            P(None, ("fsdp", "dp"), None),
            P(None, ("fsdp", "dp")),
            P(),
            P(None, ("fsdp", "dp"), None),
            P(("fsdp", "dp"), None),
            P(("fsdp", "dp")),
            P(),
            P(("fsdp", "dp"), None),
            P(("fsdp", "dp"), None),
            P(("fsdp", "dp")),
            P(),
            P(("fsdp", "dp"), None),
            P(("fsdp", "dp")),
            P(("fsdp", "dp")),
            P(("fsdp", "dp")),
        ),
        check_vma=False,
    )
```

```python
import functools
import math

import jax
import jax.numpy as jnp
from jax import lax
from jax.experimental import pallas as pl
from jax.experimental.pallas import tpu as pltpu
from jax.sharding import PartitionSpec as P

D = 1024
HEADS = 16
HEAD_DIM = 64
FF = 4096
VOCAB = 30720
SEQ_LEN = 512
LAYERS = 1
MICRO = 2
BOTH = ("fsdp", "dp")
LOW = jnp.bfloat16
MESH = pl.DeviceIdType.MESH
ALL = slice(None)


learn_rate = 0.02
decay_rate = 0.5
tiny_square = 1e-30
norm_epsilon = 1e-12
precise = lax.Precision.HIGHEST


def layer_norm(inputs, norm_gain, norm_shift):
    center = inputs - jnp.mean(inputs, axis=-1, keepdims=True)
    spread = jnp.mean(center * center, axis=-1, keepdims=True)
    return center * lax.rsqrt(spread + norm_epsilon) * norm_gain + norm_shift


def norm_back(inputs, norm_gain, norm_shift, cotangent):
    result, pull = jax.vjp(layer_norm, inputs, norm_gain, norm_shift)
    return pull(cotangent)


def exact_gelu(inputs):
    return jax.nn.gelu(inputs, approximate=False)


def gelu_back(inputs, cotangent):
    result, pull = jax.vjp(exact_gelu, inputs)
    return pull(cotangent)[0]


def multiply(left_side, right_side):
    return jnp.dot(left_side, right_side, preferred_element_type=jnp.float32)


def multiply_left(left_side, right_side):
    return lax.dot_general(
        left_side, right_side, (((0,), (0,)), ((), ())), preferred_element_type=jnp.float32
    )


def multiply_right(left_side, right_side):
    return lax.dot_general(
        left_side, right_side, (((1,), (1,)), ((), ())), preferred_element_type=jnp.float32
    )


def piece_bounds():
    return [0, D, 2 * D, 3 * D, 4 * D, 5 * D, 5 * D + FF, 6 * D + FF, 7 * D + FF, 8 * D + FF]


def layer_slices(all_vectors, layer_index):
    bounds = piece_bounds()
    offset = layer_index * (8 * D + FF)
    return [
        all_vectors[offset + bounds[slot_index] : offset + bounds[slot_index + 1]]
        for slot_index in range(9)
    ]


def segment_index(position):
    piece_width = 8 * D + FF
    inner = position % piece_width
    layer_of = position // piece_width
    bounds = piece_bounds()[1:-1]
    local_segment = sum(((inner >= bound).astype(jnp.int32) for bound in bounds))
    tail = 9 * LAYERS + (position - LAYERS * piece_width) // D
    return jnp.where(position < LAYERS * piece_width, 9 * layer_of + local_segment, tail)


def segment_sizes():
    sizes = []
    sizes = sizes + [D, D, D, D, D, FF, D, D, D]
    return jnp.array(sizes + [D, D, D, D], jnp.float32)


def head_parts(ref):
    both = ref[...]
    return both[:, :HEAD_DIM], both[:, HEAD_DIM:]


def key_scores(queries, key_rows):
    return multiply_right(key_rows, queries) * HEAD_DIM ** (-0.5)


def attend_kernel(q_ref, k_ref, v_ref, context_ref, total_ref):
    contexts = []
    for head, (queries, key_rows, values) in enumerate(
        zip(head_parts(q_ref), head_parts(k_ref), head_parts(v_ref))
    ):
        scores = key_scores(queries, key_rows)
        peak = jnp.max(scores, axis=0, keepdims=True)
        exponent = jnp.exp(scores - peak)
        running = jnp.sum(exponent, axis=0, keepdims=True)
        soft_probs = (exponent / running).astype(LOW)
        contexts.append(multiply_left(values, soft_probs))
        total_ref[head] = peak + jnp.log(running)
    context_ref[...] = jnp.concatenate(contexts, axis=0).T.astype(LOW)


def attend_back_kernel(q_ref, k_ref, v_ref, d_ref, total_ref, out_ref):
    scale = HEAD_DIM ** (-0.5)
    for head, (queries, key_rows, values, d_context) in enumerate(
        zip(head_parts(q_ref), head_parts(k_ref), head_parts(v_ref), head_parts(d_ref))
    ):
        soft_probs = jnp.exp(key_scores(queries, key_rows) - total_ref[head])
        d_values = multiply(soft_probs.astype(LOW), d_context)
        d_probs = multiply_right(values, d_context)
        inner = jnp.sum(d_probs * soft_probs, axis=0, keepdims=True)
        d_scores = (soft_probs * (d_probs - inner)).astype(LOW)
        part = pl.ds(head * HEAD_DIM, HEAD_DIM)
        out_ref[0, part] = (multiply_left(key_rows, d_scores) * scale).astype(LOW)
        out_ref[1, part] = (multiply(d_scores, queries) * scale).T.astype(LOW)
        out_ref[2, part] = d_values.T.astype(LOW)


def attention_specs(tokens, length):
    pairs = HEADS // 2
    wide = 2 * HEAD_DIM

    def joint(third):
        return pl.BlockSpec((length, wide), lambda s, i: (s, third * pairs + i))

    total = pl.BlockSpec((2, 1, length), lambda s, i: (i, 0, s))
    return (tokens // length, pairs), [joint(0), joint(1), joint(2)], joint(0), total


def attend(projected, seq_dev):
    tokens = projected.shape[0]
    grid, ins, context, total = attention_specs(tokens, tokens // seq_dev)
    return pl.pallas_call(
        attend_kernel,
        name="attend",
        grid=grid,
        in_specs=ins,
        out_specs=(context, total),
        out_shape=(
            jax.ShapeDtypeStruct((tokens, D), LOW),
            jax.ShapeDtypeStruct((HEADS, 1, tokens), jnp.float32),
        ),
    )(projected, projected, projected)


def attend_back(projected, log_total, d_context, seq_dev):
    tokens = projected.shape[0]
    length = tokens // seq_dev
    grid, ins, context, total = attention_specs(tokens, length)
    return pl.pallas_call(
        attend_back_kernel,
        name="attend_back",
        grid=grid,
        in_specs=ins + [context, total],
        out_specs=pl.BlockSpec((3, 2 * HEAD_DIM, length), lambda s, i: (0, i, s)),
        out_shape=jax.ShapeDtypeStruct((3, D, tokens), LOW),
    )(projected, projected, projected, d_context, log_total).reshape(3 * D, tokens)


def lift_kernel(weight_ref, bias_ref, middle_ref, active_ref, slope_ref):
    lifted = multiply_right(weight_ref[...], middle_ref[...]) + bias_ref[...]
    cumulative = 0.5 + 0.5 * lax.erf(lifted * (0.5**0.5))
    density = jnp.exp(-0.5 * lifted * lifted) * ((0.5 / math.pi) ** 0.5)
    active_ref[...] = (lifted * cumulative).astype(LOW)
    slope_ref[...] = cumulative + lifted * density


def lift(weight_in, bias_up, middle_low):
    tokens = middle_low.shape[0]
    rows = 512
    return pl.pallas_call(
        lift_kernel,
        name="lift",
        grid=(FF // rows,),
        in_specs=[
            pl.BlockSpec((rows, D), lambda i: (4 * D // rows + i, 0)),
            pl.BlockSpec((rows, 1), lambda i: (i, 0)),
            pl.BlockSpec((tokens, D), lambda i: (0, 0)),
        ],
        out_specs=(
            pl.BlockSpec((rows, tokens), lambda i: (i, 0)),
            pl.BlockSpec((rows, tokens), lambda i: (i, 0)),
        ),
        out_shape=(
            jax.ShapeDtypeStruct((FF, tokens), LOW),
            jax.ShapeDtypeStruct((FF, tokens), jnp.float32),
        ),
    )(weight_in, bias_up[:, None], middle_low)


def layer_forward(hidden, weight_in, weight_down, pieces, seq_dev):
    bias_q, bias_v, bias_o, gain_a, shift_a, bias_up, bias_down, gain_b, shift_b = pieces
    hidden_low = hidden.astype(jnp.bfloat16)
    joint_bias = jnp.concatenate([bias_q, jnp.zeros_like(bias_q), bias_v])
    projected = (multiply_right(hidden_low, weight_in[: 3 * D]) + joint_bias).astype(jnp.bfloat16)
    context_low, log_total = attend(projected, seq_dev)
    mid_in = hidden + (multiply_right(context_low, weight_in[3 * D : 4 * D]) + bias_o)
    middle = layer_norm(mid_in, gain_a, shift_a)
    middle_low = middle.astype(jnp.bfloat16)
    active_low, slope = lift(weight_in, bias_up, middle_low)
    out_in = middle + (multiply_left(active_low, weight_down) + bias_down)
    output = layer_norm(out_in, gain_b, shift_b)
    return (
        output,
        (
            hidden_low,
            projected,
            log_total,
            context_low,
            mid_in,
            middle_low,
            slope,
            active_low,
            out_in,
        ),
    )


def layer_backward(grad_out, weight_in, weight_down, pieces, kept, seq_dev):
    bias_q, bias_v, bias_o, gain_a, shift_a, bias_up, bias_down, gain_b, shift_b = pieces
    (
        hidden_low,
        projected,
        log_total,
        context_low,
        mid_in,
        middle_low,
        slope,
        active_low,
        out_in,
    ) = kept
    d_out_in, d_gain_b, d_shift_b = norm_back(out_in, gain_b, shift_b, grad_out)
    d_down_low = d_out_in.astype(jnp.bfloat16)
    d_lifted_low = (multiply_right(weight_down, d_down_low) * slope).astype(jnp.bfloat16)
    d_middle = d_out_in + multiply_left(d_lifted_low, weight_in[4 * D :])
    d_mid_in, d_gain_a, d_shift_a = norm_back(mid_in, gain_a, shift_a, d_middle)
    d_attended_low = d_mid_in.astype(jnp.bfloat16)
    d_context_low = multiply(d_attended_low, weight_in[3 * D : 4 * D]).astype(jnp.bfloat16)
    d_projected_low = attend_back(projected, log_total, d_context_low, seq_dev)
    d_hidden = d_mid_in + multiply_left(d_projected_low, weight_in[: 3 * D])
    joint_sums = jnp.sum(d_projected_low.astype(jnp.float32), axis=1)
    grad_pieces = jnp.concatenate(
        [
            joint_sums[:D],
            joint_sums[2 * D :],
            jnp.sum(d_attended_low.astype(jnp.float32), axis=0),
            d_gain_a,
            d_shift_a,
            jnp.sum(d_lifted_low.astype(jnp.float32), axis=1),
            jnp.sum(d_down_low.astype(jnp.float32), axis=0),
            d_gain_b,
            d_shift_b,
        ]
    )
    return (
        d_hidden,
        (
            active_low,
            d_down_low,
            d_lifted_low,
            middle_low,
            d_projected_low,
            hidden_low,
            d_attended_low.T,
            context_low,
        ),
        grad_pieces,
    )


def place():
    block = lax.axis_index("fsdp")
    return block // 4, (block // 2) % 2, block % 2, lax.axis_index("dp")


def device(z, y, x, c):
    return ((z * 2 + y) * 2 + x, c)


def my_rank():
    return lax.axis_index("fsdp") * 2 + lax.axis_index("dp")


def by_rank(index):
    return (index // 2, index % 2)


def neighbours(z, y, x, c):
    return (
        device(z, y, 1 - x, c),
        device(z, 1 - y, x, c),
        device(z, y, x, 1 - c),
        [device((z + k) % 4, y, x, c) for k in (1, 2, 3)],
    )


def greet(n):
    me = my_rank()
    barrier = pltpu.get_barrier_semaphore()

    def one(step, carry):
        pl.semaphore_signal(
            barrier, inc=1, device_id=by_rank((me + step) % n), device_id_type=MESH
        )
        return carry

    lax.fori_loop(1, n, one, 0)


def welcome(n):
    pl.semaphore_wait(pltpu.get_barrier_semaphore(), n - 1)


def enter(n):
    greet(n)
    welcome(n)


class Copies:
    def __init__(self, send, recv):
        self.send, self.recv, self.begun, self.count = send, recv, {}, 0

    def start(self, src, dst, target):
        slot = self.count
        self.count += 1
        copy = pltpu.make_async_remote_copy(
            src_ref=src,
            dst_ref=dst,
            send_sem=self.send.at[slot],
            recv_sem=self.recv.at[slot],
            device_id=target,
            device_id_type=MESH,
        )
        copy.start()
        self.begun[id(copy)] = copy
        return copy

    def sent(self, copy):
        self.begun.pop(id(copy)).wait_send()

    def drain(self):
        for copy in self.begun.values():
            copy.wait_send()


def exchange_copy(src, dst, send, recv, step, n):
    me = my_rank()
    target = (me + step) % n
    return pltpu.make_async_remote_copy(
        src_ref=src.at[target],
        dst_ref=dst.at[me],
        send_sem=send.at[step],
        recv_sem=recv.at[step],
        device_id=by_rank(target),
        device_id_type=MESH,
    )


def exchange_start(src, dst, send, recv, n):
    def begin(step, carry):
        exchange_copy(src, dst, send, recv, step, n).start()
        return carry

    lax.fori_loop(1, n, begin, 0)


def exchange_wait(src, dst, send, recv, n):
    def finish(step, carry):
        exchange_copy(src, dst, send, recv, step, n).wait()
        return carry

    lax.fori_loop(1, n, finish, 0)


LEAD, LOOK = 3, 2
TILES = ((64,), (64, 64, 64), (64, 64))
PLANE = {1: 64}


def gather_steps(plan):
    first = [i for i, p in enumerate(plan) if p[3]]
    rest = [i for i, p in enumerate(plan) if not p[3]]
    order, task = first + rest[:LEAD] + first, 0
    for step in range(len(rest) + 4):
        if step + LEAD < len(rest):
            order.append(rest[step + LEAD])
        order += [rest[i] for i in range(min(step, len(rest) - 1), -1, -1) if step - i < 4]
        if step == LOOK:
            order += first
        if step >= LOOK and task < 4:
            task += 1
            order.append(-task)
    return order + first + first


def count_from(index, shape, axis):
    return lax.broadcasted_iota(jnp.int32, shape, axis) == index


def one_hot(mask):
    return jnp.where(mask, 1.0, 0.0).astype(LOW)


def fill_slots(blocks, values, tally, to_slot, message):
    n, capacity, lanes = message.shape
    tokens = blocks.shape[1]
    owner = blocks[...]
    member = count_from(owner, (n, tokens), 0)
    earlier = one_hot(
        lax.broadcasted_iota(jnp.int32, (tokens, tokens), 0)
        < lax.broadcasted_iota(jnp.int32, (tokens, tokens), 1)
    )
    ahead = multiply(one_hot(member), earlier)
    rank = jnp.sum(jnp.where(member, ahead, 0.0), axis=0, keepdims=True).astype(jnp.int32)
    slot = owner * capacity + rank
    to_slot[...] = one_hot(count_from(slot, (n * capacity, tokens), 0))
    listed = multiply(to_slot[...], values[...]) + tally[...]
    message[...] = listed.reshape(n, capacity, lanes)


def look_up(index, answer, table, from_slot, found):
    n, capacity, lanes = answer.shape
    group = n // 4
    part = pl.ds(index * group, group)
    wanted = answer[part].reshape(group * capacity, lanes)
    row = (wanted[:, 0:1] * 256.0 + wanted[:, 1:2]).astype(jnp.int32)
    row = jnp.where(wanted[:, 2:3] > 0.5, row, -1)
    hot = one_hot(count_from(row, (group * capacity, table.shape[0]), 1))
    from_slot[part] = hot.reshape(group, capacity, -1)
    found[part] = multiply(hot, table[...]).astype(LOW).reshape(group, capacity, -1)


def gather_kernel(plan, count, *refs):
    local = refs[:count]
    blocks, values, tally, table = refs[count : count + 4]
    out = refs[count + 4 : 2 * count + 4]
    rows, to_slot, from_slot, answer = refs[2 * count + 4 : 2 * count + 8]
    message, found, send, recv, own_sem, ask_send, ask_recv, row_send, row_recv = refs[
        2 * count + 8 :
    ]
    z, y, x, c = place()
    n = 32
    me = my_rank()
    greet(n)
    fill_slots(blocks, values, tally, to_slot, message)
    answer[me] = message[me]
    welcome(n)
    copies = Copies(send, recv)
    exchange_start(message, answer, ask_send, ask_recv, n)
    own = []
    for i in range(count):
        own.append(pltpu.make_async_copy(local[i], out[i].at[z, y, x, c], own_sem.at[i]))
        own[i].start()
    to_x, to_y, to_core, to_z = neighbours(z, y, x, c)

    def pass_on(ref, where, target):
        return copies.start(ref.at[where], ref.at[where], target)

    landed = set()

    def own_there(i):
        if i not in landed:
            own[i].wait()
            landed.add(i)

    def chunk(i, start, size, plane_first):
        ref, mine, half = out[i], local[i], size // 2
        part, low, high = pl.ds(start, size), pl.ds(start, half), pl.ds(start + half, half)
        last = []
        if not plane_first:
            along = [copies.start(mine.at[part], ref.at[z, y, x, c, part], t) for t in to_z]
            yield
            for copy in along:
                copy.wait_recv()
            own_there(i)
            first = pass_on(ref, (ALL, y, x, c, low), to_x)
            second = pass_on(ref, (ALL, y, x, c, high), to_y)
            last.append(pass_on(ref, (ALL, y, x, c, part), to_core))
            yield
            first.wait_recv()
            second.wait_recv()
            first = pass_on(ref, (ALL, y, ALL, c, low), to_y)
            second = pass_on(ref, (ALL, ALL, x, c, high), to_x)
            last.append(pass_on(ref, (ALL, y, 1 - x, c, low), to_core))
            last.append(pass_on(ref, (ALL, 1 - y, x, c, high), to_core))
            yield
            first.wait_recv()
            second.wait_recv()
            last.append(pass_on(ref, (ALL, 1 - y, ALL, c, low), to_core))
            last.append(pass_on(ref, (ALL, ALL, 1 - x, c, high), to_core))
        else:
            first = copies.start(mine.at[low], ref.at[z, y, x, c, low], to_x)
            second = copies.start(mine.at[high], ref.at[z, y, x, c, high], to_y)
            last.append(copies.start(mine.at[part], ref.at[z, y, x, c, part], to_core))
            yield
            first.wait_recv()
            second.wait_recv()
            own_there(i)
            first = pass_on(ref, (z, y, ALL, c, low), to_y)
            second = pass_on(ref, (z, ALL, x, c, high), to_x)
            last.append(pass_on(ref, (z, y, 1 - x, c, low), to_core))
            last.append(pass_on(ref, (z, 1 - y, x, c, high), to_core))
            yield
            first.wait_recv()
            second.wait_recv()
            along = [pass_on(ref, (z, ALL, ALL, c, part), t) for t in to_z]
            last.append(pass_on(ref, (z, 1 - y, ALL, c, low), to_core))
            last.append(pass_on(ref, (z, ALL, 1 - x, c, high), to_core))
            yield
            for k in (1, 2, 3):
                along[k - 1].wait_recv()
                last.append(pass_on(ref, ((z + 4 - k) % 4, ALL, ALL, c, part), to_core))
        yield
        for copy in last:
            copy.wait_recv()
        yield

    chunks = [chunk(*p) for p in plan]
    keep = pltpu.make_async_copy(found.at[me], rows.at[me], own_sem.at[count])

    def row_copy(slot, target, source):
        return pltpu.make_async_remote_copy(
            src_ref=found.at[target],
            dst_ref=rows.at[source],
            send_sem=row_send.at[slot],
            recv_sem=row_recv.at[source],
            device_id=by_rank(target),
            device_id_type=MESH,
        )

    def plane_rank(slot):
        return (z + slot // 8) % 4 * 8 + (me + slot) % 8

    def send_row(slot, carry):
        row_copy(slot, plane_rank(slot), me).start()
        return carry

    for index in gather_steps(plan):
        if index >= 0:
            next(chunks[index], None)
            continue
        task = -index - 1
        if task == 0:
            exchange_wait(message, answer, ask_send, ask_recv, n)
        look_up((z + task) % 4, answer, table, from_slot, found)
        if task == 0:
            keep.start()
        lax.fori_loop(max(task * 8, 1), task * 8 + 8, send_row, 0)

    def finish_row(slot, carry):
        row_copy(slot, plane_rank(slot), me).wait_send()
        row_copy(slot, me, (me + slot) % n).wait_recv()
        return carry

    lax.fori_loop(1, n, finish_row, 0)
    keep.wait()
    copies.drain()
    for i in range(count):
        own_there(i)


def gather_plan(heights):
    plan = []
    for i, height in enumerate(heights):
        start = 0
        if i in PLANE:
            plan.append((i, 0, PLANE[i], True))
            start = PLANE[i]
        for size in TILES[i]:
            plan.append((i, start, size, False))
            start += size
        assert start == height
    return plan


def gather_weights(arrays, blocks, values, tally, table):
    count = len(arrays)
    n, capacity = 32, 32
    tokens = blocks.shape[1]
    plan = gather_plan([a.shape[0] for a in arrays])
    total = sum(15 if p[3] else 12 for p in plan)
    hbm = pl.BlockSpec(memory_space=pl.ANY)
    vmem = pl.BlockSpec(memory_space=pltpu.VMEM)
    dma = pltpu.SemaphoreType.DMA
    shape = jax.ShapeDtypeStruct
    return pl.pallas_call(
        functools.partial(gather_kernel, plan, count),
        name="gather_weights",
        out_shape=tuple(shape((4, 2, 2, 2) + a.shape, a.dtype) for a in arrays)
        + (
            shape((n, capacity, D), LOW),
            shape((n * capacity, tokens), LOW),
            shape((n, capacity, table.shape[0]), LOW),
            shape((n, capacity, 128), jnp.float32),
        ),
        in_specs=[vmem] * (count + 4),
        out_specs=tuple([hbm] * (count + 1) + [vmem] * 3),
        scratch_shapes=[
            pltpu.VMEM((n, capacity, 128), jnp.float32),
            pltpu.VMEM((n, capacity, D), LOW),
            dma((total,)),
            dma((total,)),
            dma((count + 1,)),
        ]
        + [dma((n,))] * 4,
        compiler_params=pltpu.CompilerParams(collective_id=0, has_side_effects=True),
    )(*arrays, blocks, values, tally, table)


def add_blocks(dst, other, shape, at_dst, at_other):
    def body(index, carry):
        where = []
        for extent in reversed(shape):
            where.append(index % extent)
            index = index // extent
        where = tuple(reversed(where))
        d, o = at_dst(*where), at_other(*where)
        total = dst[d].astype(jnp.float32) + other[o].astype(jnp.float32)
        dst[d] = total.astype(dst.dtype)
        return carry

    lax.fori_loop(0, math.prod(shape), body, 0)


WIDE = 256


class Group:
    def __init__(self, z0, nz, height, sources, out):
        self.z0, self.nz, self.height, self.sources, self.out = z0, nz, height, sources, out

    def scratch(self):
        nz, h, n = self.nz, self.height, D // WIDE
        shapes = [(2, nz, 2, 2, h), (n, nz, 2, 2, h)] + [(n, nz, 2, h // 2)] * 2
        shapes += [(n, nz, h // 2)] * 2 + [(n, 3, h)]
        return [pltpu.VMEM(shape + (WIDE,), LOW) for shape in shapes]


def each_block(group, refs, wide, core, body):
    for start, stop, left, right, base, together in group.sources:
        def one(step, carry, left=left, right=right, base=base, together=together):
            index = step * together
            part = refs[left][pl.ds(index - base, together), core]
            product = multiply(part.reshape(-1, part.shape[-1]), refs[right][:, wide])
            product = product.reshape(together, group.height, WIDE)
            for k in range(together):
                at = index + k
                body((at // 4, (at // 2) % 2, at % 2), product[k])
            return carry

        lax.fori_loop(start // together, stop // together, one, 0)


def scatter_kernel(groups, n_left, *refs):
    operands = refs[:n_left]
    side, buckets, vector = refs[n_left : n_left + 3]
    out = refs[n_left + 3 : n_left + 6]
    arrived, vector_all = refs[n_left + 6 : n_left + 8]
    rest = refs[n_left + 8 :]
    scratch = [rest[7 * i : 7 * i + 7] for i in range(len(groups))]
    side_scratch = rest[7 * len(groups) : 7 * len(groups) + 7]
    (send, recv, z_send, z_recv, load, row_send, row_recv, vec_send, vec_recv) = rest[
        7 * len(groups) + 7 :
    ]
    z, y, x, c = place()
    n = 32
    me = my_rank()
    enter(n)
    copies = Copies(send, recv)
    to_x, to_y, to_core, to_z = neighbours(z, y, x, c)
    own = [
        pltpu.make_async_copy(buckets.at[me], arrived.at[me], load.at[0]),
        pltpu.make_async_copy(vector.at[me], vector_all.at[me], load.at[1]),
    ]
    for copy in own:
        copy.start()
    sent_before = {}

    def product_chunk(slot, which, index):
        group = groups[which]
        outgoing, held, low_1, high_1, low_2, high_2, from_z = scratch[which]
        nz, h = group.nz, group.height
        wide = pl.ds(index * WIDE, WIDE)
        low, high = pl.ds(0, h // 2), pl.ds(h // 2, h // 2)
        here = index % 2
        if index >= 2:
            copies.sent(sent_before[which, index - 2])

        def send_off(where, value):
            outgoing[(here,) + where] = value.astype(LOW)

        each_block(group, operands, wide, 1 - c, send_off)
        core = copies.start(outgoing.at[here], held.at[index], to_core)
        sent_before[which, index] = core
        yield
        core.wait_recv()

        def add_own(where, value):
            spot = (index,) + where
            held[spot] = (value + held[spot].astype(jnp.float32)).astype(LOW)

        each_block(group, operands, wide, c, add_own)
        first = copies.start(held.at[index, :, 1 - y, :, low], low_1.at[index], to_y)
        second = copies.start(held.at[index, :, :, 1 - x, high], high_1.at[index], to_x)
        yield
        first.wait_recv()
        second.wait_recv()
        add_blocks(
            held, low_1, (nz, 2), lambda a, d: (index, a, y, d, low), lambda a, d: (index, a, d)
        )
        add_blocks(
            held, high_1, (nz, 2), lambda a, b: (index, a, b, x, high), lambda a, b: (index, a, b)
        )
        first = copies.start(held.at[index, :, y, 1 - x, low], low_2.at[index], to_x)
        second = copies.start(held.at[index, :, 1 - y, x, high], high_2.at[index], to_y)
        yield
        first.wait_recv()
        second.wait_recv()
        add_blocks(held, low_2, (nz,), lambda a: (index, a, y, x, low), lambda a: (index, a))
        add_blocks(held, high_2, (nz,), lambda a: (index, a, y, x, high), lambda a: (index, a))

        def along(level, back):
            return pltpu.make_async_remote_copy(
                src_ref=held.at[index, level, y, x],
                dst_ref=from_z.at[index, back],
                send_sem=z_send.at[slot, level],
                recv_sem=z_recv.at[slot, back],
                device_id=device(group.z0 + level, y, x, c),
                device_id_type=MESH,
            )

        for level in range(nz):
            away = z != group.z0 + level

            @pl.when(away)
            def _(level=level):
                along(level, (z - group.z0 - level + 3) % 4).start()

        yield

        def finish():
            for back in range(3):
                along(0, back).wait_recv()
            mine = held[index, z - group.z0, y, x].astype(jnp.float32)
            for back in range(3):
                mine = mine + from_z[index, back].astype(jnp.float32)
            out[group.out][:, wide] = mine

        if nz == 4:
            finish()
        else:
            pl.when((z >= group.z0) & (z < group.z0 + nz))(finish)
        yield
        for level in range(nz):
            away = z != group.z0 + level

            @pl.when(away)
            def _(level=level):
                along(level, (z - group.z0 - level + 3) % 4).wait_send()

        yield

    def side_chunk():
        held, from_core, low_1, high_1, low_2, high_2, from_z = side_scratch
        size = held.shape[3]
        half = size // 32 * 16 + 16
        low, high = pl.ds(0, half), pl.ds(half, size - half)
        core = copies.start(side.at[:, :, :, 1 - c], from_core, to_core)
        mine = pltpu.make_async_copy(side.at[:, :, :, c], held, load.at[2])
        mine.start()
        yield
        mine.wait()
        core.wait_recv()
        add_blocks(held, from_core, (4, 2, 2), lambda *w: w, lambda *w: w)
        first = copies.start(held.at[:, 1 - y, :, low], low_1, to_y)
        second = copies.start(held.at[:, :, 1 - x, high], high_1, to_x)
        yield
        first.wait_recv()
        second.wait_recv()
        add_blocks(held, low_1, (4, 2), lambda a, d: (a, y, d, low), lambda a, d: (a, d))
        add_blocks(held, high_1, (4, 2), lambda a, b: (a, b, x, high), lambda a, b: (a, b))
        first = copies.start(held.at[:, y, 1 - x, low], low_2, to_x)
        second = copies.start(held.at[:, 1 - y, x, high], high_2, to_y)
        yield
        first.wait_recv()
        second.wait_recv()
        add_blocks(held, low_2, (4,), lambda a: (a, y, x, low), lambda a: (a,))
        add_blocks(held, high_2, (4,), lambda a: (a, y, x, high), lambda a: (a,))
        along = [
            copies.start(held.at[(z + k) % 4, y, x], from_z.at[k - 1], to_z[k - 1])
            for k in (1, 2, 3)
        ]
        yield
        for copy in along:
            copy.wait_recv()
        total = held[z, y, x].astype(jnp.float32)
        for k in range(3):
            total = total + from_z[k].astype(jnp.float32)
        out[2][...] = total
        yield
        yield

    parts = [(which, index) for index in range(D // WIDE) for which in ORDER]
    chunks = [side_chunk()] + [product_chunk(slot, *p) for slot, p in enumerate(parts)]
    exchange_start(vector, vector_all, vec_send, vec_recv, n)
    for step in range(len(chunks) + 5):
        for index in range(min(step, len(chunks) - 1), -1, -1):
            if step - index < 6:
                next(chunks[index], None)
        if step == ROWS_AT:
            exchange_start(buckets, arrived, row_send, row_recv, n)
    exchange_wait(vector, vector_all, vec_send, vec_recv, n)
    exchange_wait(buckets, arrived, row_send, row_recv, n)
    copies.drain()
    for copy in own:
        copy.wait()


ROWS_AT = 0
ORDER = (0, 1, 2)


def scatter_grads(pairs, side, buckets, vector):
    blocked = []
    for i, pair in enumerate(pairs):
        height = FF // 32 if i == 0 else 256
        blocked.append(pair if i % 2 else pair.reshape(-1, 2, height, pair.shape[1]))
    groups = [
        Group(0, 4, FF // 32, [(0, 16, 0, 1, 0, 2)], 1),
        Group(2, 2, 256, [(0, 8, 2, 3, 0, 1)], 0),
        Group(0, 2, 256, [(0, 6, 4, 5, 0, 1), (6, 8, 6, 7, 6, 1)], 0),
    ]
    height = side.shape[4]
    half = height // 32 * 16 + 16
    hbm = pl.BlockSpec(memory_space=pl.ANY)
    vmem = pl.BlockSpec(memory_space=pltpu.VMEM)
    dma = pltpu.SemaphoreType.DMA
    scratch = [shape for group in groups for shape in group.scratch()]
    for lead in (
        (4, 2, 2, height),
        (4, 2, 2, height),
        (4, 2, half),
        (4, 2, height - half),
        (4, half),
        (4, height - half),
        (3, height),
    ):
        scratch.append(pltpu.VMEM(lead + (D,), LOW))
    chunks = len(groups) * D // WIDE
    total = 5 * chunks + 8
    shape = jax.ShapeDtypeStruct
    return pl.pallas_call(
        functools.partial(scatter_kernel, groups, len(pairs)),
        name="scatter_grads",
        out_shape=(
            shape((256, D), jnp.float32),
            shape((FF // 32, D), jnp.float32),
            shape((height, D), jnp.float32),
            shape(buckets.shape, buckets.dtype),
            shape(vector.shape, vector.dtype),
        ),
        in_specs=[vmem] * len(pairs) + [hbm] * 3,
        out_specs=(vmem, vmem, vmem, hbm, hbm),
        scratch_shapes=scratch
        + [
            dma((total,)),
            dma((total,)),
            dma((chunks, 4)),
            dma((chunks, 3)),
            dma((3,)),
        ]
        + [dma((32,))] * 4,
        compiler_params=pltpu.CompilerParams(
            collective_id=1, has_side_effects=True, vmem_limit_bytes=64000 * 1024
        ),
    )(*blocked, side, buckets, vector)


def sum_kernel(values, out, landed, total, send, recv, send_again, recv_again):
    n = 32
    me = my_rank()
    enter(n)
    exchange_start(values, landed, send, recv, n)
    landed[me] = values[me]
    exchange_wait(values, landed, send, recv, n)

    def add(index, carry):
        return carry + landed[index]

    total[...] = lax.fori_loop(0, n, add, jnp.zeros(total.shape, jnp.float32))
    out[me] = total[...]

    def copy(step):
        target = (me + step) % n
        return pltpu.make_async_remote_copy(
            src_ref=total,
            dst_ref=out.at[me],
            send_sem=send_again.at[step],
            recv_sem=recv_again.at[step],
            device_id=by_rank(target),
            device_id_type=MESH,
        )

    def begin(step, carry):
        copy(step).start()
        return carry

    def finish(step, carry):
        copy(step).wait()
        return carry

    lax.fori_loop(1, n, begin, 0)
    lax.fori_loop(1, n, finish, 0)


def sum_over_devices(flat):
    n = lax.axis_size(BOTH)
    if not special():
        return lax.psum(flat, BOTH)
    unit = n * 128
    lines = -(-flat.shape[0] // unit)
    values = jnp.pad(flat, (0, lines * unit - flat.shape[0])).reshape(n, lines, 128)
    vmem = pl.BlockSpec(memory_space=pltpu.VMEM)
    dma = pltpu.SemaphoreType.DMA
    result = pl.pallas_call(
        sum_kernel,
        name="sum_over_devices",
        out_shape=jax.ShapeDtypeStruct(values.shape, jnp.float32),
        in_specs=[vmem],
        out_specs=vmem,
        scratch_shapes=[
            pltpu.VMEM(values.shape, jnp.float32),
            pltpu.VMEM(values.shape[1:], jnp.float32),
            dma((n,)),
            dma((n,)),
            dma((n,)),
            dma((n,)),
        ],
        compiler_params=pltpu.CompilerParams(collective_id=2, has_side_effects=True),
    )(values)
    return result.reshape(-1)[: flat.shape[0]]


def special():
    return lax.axis_size("fsdp") == 16 and lax.axis_size("dp") == 2


def swap(blocks):
    shape = blocks.shape
    n_fsdp, n_dp = lax.axis_size("fsdp"), lax.axis_size("dp")
    split = blocks.reshape((n_fsdp, n_dp) + shape[1:])
    half = lax.all_to_all(split, "fsdp", split_axis=0, concat_axis=0, tiled=True)
    return lax.all_to_all(half, "dp", split_axis=1, concat_axis=1, tiled=True).reshape(shape)

def ask_rows(blocks, local_row, local_counts, block_rows, capacity):
    n = lax.axis_size(BOTH)
    onehot = (blocks[:, None] == jnp.arange(n)[None, :]).astype(jnp.int32)
    rank = jnp.sum(jnp.cumsum(onehot, axis=0) * onehot, axis=1) - 1
    slot = blocks * capacity + rank
    bucket_ids = jnp.full((n * capacity,), -1, jnp.int32).at[slot].set(local_row)
    message = jnp.concatenate(
        [
            bucket_ids.reshape(n, capacity),
            jnp.broadcast_to(local_counts[None, :], (n, MICRO)),
        ],
        axis=1,
    )
    answer = swap(message)
    asked = answer[:, :capacity].reshape(-1)
    to_slot = (jnp.arange(n * capacity)[:, None] == slot[None, :]).astype(LOW)
    from_slot = (asked[:, None] == jnp.arange(block_rows)[None, :]).astype(LOW)
    return to_slot, from_slot, jnp.sum(answer[:, capacity:], axis=0)


def gather_blocks(arrays, blocks, local_row, local_counts, table, capacity):
    n = lax.axis_size(BOTH)
    if special():
        row = local_row.astype(jnp.int32)
        values = jnp.stack([row // 256, row % 256, jnp.ones_like(row)], axis=1).astype(LOW)
        tally = jnp.pad(local_counts.astype(jnp.float32), (3, 125 - MICRO)).reshape(1, 128)
        *gathered, rows, to_slot, from_slot, answer = gather_weights(
            arrays, blocks.reshape(1, -1), jnp.pad(values, ((0, 0), (0, 125))), tally, table
        )
        full = [g.reshape((-1, a.shape[-1])) for g, a in zip(gathered, arrays)]
        counts = jnp.sum(answer[:, 0, 3 : 3 + MICRO], axis=0)
        return full, rows, to_slot, from_slot.reshape(n * capacity, -1), counts
    to_slot, from_slot, counts = ask_rows(
        blocks, local_row, local_counts, table.shape[0], capacity
    )
    found = multiply(from_slot, table).astype(LOW).reshape(n, capacity, D)
    full = [lax.all_gather(a, BOTH, axis=0, tiled=True) for a in arrays]
    return full, swap(found), to_slot, from_slot, counts.astype(jnp.float32)


def reduce_blocks(pairs, grad_pos, grad_head, buckets, vector):
    n = lax.axis_size(BOTH)
    if special():
        side = jnp.concatenate([grad_pos.astype(LOW), grad_head.astype(LOW)], axis=0)
        grad_in, grad_down, grad_side, arrived, pieces = scatter_grads(
            pairs, side.reshape(4, 2, 2, 2, -1, D), buckets, vector.reshape(n, -1, 128)
        )
        return grad_side, grad_in, grad_down, arrived, jnp.sum(pieces, axis=0).reshape(-1)
    down, up, joint, attended = [
        multiply(pairs[2 * i], pairs[2 * i + 1]) for i in range(4)
    ]

    def own(value):
        return lax.psum_scatter(value, BOTH, scatter_dimension=0, tiled=True)

    return (
        own(jnp.concatenate([grad_pos, grad_head], axis=0)),
        own(jnp.concatenate([joint, attended, up], axis=0)),
        own(down),
        swap(buckets),
        own(vector),
    )


def factor_stats(gradient, rows_new):
    square = gradient * gradient
    return jnp.sum(square + tiny_square, axis=0), jnp.sum(square / rows_new[:, None], axis=0)


def clip_of(weighted, cols_new, mean_rows, size):
    mean_square = jnp.sum(weighted / cols_new, axis=-1) * mean_rows / size
    return jnp.maximum(1.0, jnp.sqrt(mean_square))


def local(
    token_ids,
    labels,
    loss_mask,
    batch_of,
    layer_in,
    layer_down,
    word_table,
    side_mat,
    vectors,
    in_rows,
    in_cols,
    down_rows,
    down_cols,
    word_rows,
    word_cols,
    side_rows,
    side_cols,
    vec_moment,
):
    seq_dev, length = token_ids.shape
    tokens = seq_dev * length
    n_blocks = lax.axis_size(BOTH)
    my_index = lax.axis_index(BOTH)
    mask_float = loss_mask.astype(jnp.float32)
    member = batch_of[:, None] == jnp.arange(MICRO)[None, :]
    local_counts = jnp.sum(member * jnp.sum(loss_mask, axis=1)[:, None], axis=0)
    block_rows = word_table.shape[0]
    capacity = max(2, 2 * tokens // n_blocks)
    flat_ids = token_ids.reshape(tokens)
    blocks = flat_ids // block_rows
    label_float = labels.astype(jnp.float32).reshape(tokens)

    side_rows_local = side_mat.shape[0]
    vec_local = vectors.shape[0]
    vector_row = jnp.pad(vectors.astype(LOW).reshape(1, -1), ((0, 15), (0, D - vec_local)))
    (side_all, weight_in, weight_down), returned, to_slot, from_slot, counts = gather_blocks(
        [
            jnp.concatenate([side_mat.astype(LOW), vector_row], axis=0),
            layer_in[0].astype(LOW).T,
            layer_down[0].astype(LOW),
        ],
        blocks,
        flat_ids - blocks * block_rows,
        local_counts.astype(jnp.int32),
        word_table.astype(LOW),
        capacity,
    )
    seq_count = jnp.sum(member * counts[None, :], axis=1)
    token_weight = (mask_float / (seq_count * MICRO)[:, None]).reshape(tokens)
    side_all = side_all.reshape(n_blocks, side_rows_local + 16, D)
    side_full = side_all[:, :side_rows_local].reshape(-1, D)
    vector_full = side_all[:, side_rows_local, :vec_local].reshape(-1)
    all_vectors = vector_full.astype(jnp.float32)
    pos_rows = side_full[:SEQ_LEN].astype(jnp.float32)
    head_mat = side_full[SEQ_LEN:]
    global_offset = LAYERS * (8 * D + FF)
    gain_emb = all_vectors[global_offset : global_offset + D]
    shift_emb = all_vectors[global_offset + D : global_offset + 2 * D]
    head_bias = all_vectors[global_offset + 2 * D : global_offset + 3 * D]
    predictor = all_vectors[global_offset + 3 * D : global_offset + 4 * D]
    predictor_low = vector_full[global_offset + 3 * D : global_offset + 4 * D]
    own_rows = multiply_left(to_slot, returned.reshape(n_blocks * capacity, D))
    embedded = (own_rows.reshape(seq_dev, length, D) + pos_rows[None, :, :]).reshape(tokens, D)
    hidden = layer_norm(embedded, gain_emb, shift_emb)
    pieces = layer_slices(all_vectors, 0)
    hidden, kept = layer_forward(hidden, weight_in, weight_down, pieces, seq_dev)
    final_low = hidden.astype(LOW)
    head_pre = multiply(final_low, head_mat) + head_bias
    head_act_low = exact_gelu(head_pre).astype(LOW)
    logits = multiply(head_act_low, predictor_low)
    local_loss = jnp.sum(token_weight * (jax.nn.softplus(logits) - label_float * logits))
    d_logits = token_weight * (jax.nn.sigmoid(logits) - label_float)
    d_predictor = jnp.sum(d_logits[:, None] * head_act_low.astype(jnp.float32), axis=0)
    d_head_low = gelu_back(head_pre, d_logits[:, None] * predictor[None, :]).astype(LOW)
    grad_head = multiply_left(final_low, d_head_low)
    d_head_bias = jnp.sum(d_head_low.astype(jnp.float32), axis=0)
    d_hidden = multiply_right(d_head_low, head_mat)
    d_hidden, pairs, grad_pieces = layer_backward(
        d_hidden, weight_in, weight_down, pieces, kept, seq_dev
    )
    d_embedded, d_gain_emb, d_shift_emb = norm_back(embedded, gain_emb, shift_emb, d_hidden)
    grad_pos = jnp.sum(d_embedded.reshape(seq_dev, length, D), axis=0)
    grad_vector = jnp.concatenate([grad_pieces, d_gain_emb, d_shift_emb, d_head_bias, d_predictor])
    buckets = (
        multiply(to_slot, d_embedded.astype(LOW))
        .astype(LOW)
        .reshape(n_blocks, capacity, D)
    )
    grad_side, grad_in_t, grad_down, arrived, grad_vec = reduce_blocks(
        pairs, grad_pos, grad_head, buckets, grad_vector
    )
    grad_word = multiply_left(from_slot, arrived.reshape(n_blocks * capacity, D))
    grad_in = grad_in_t.T

    col_local = layer_in.shape[2]
    col_global = my_index * col_local + jnp.arange(col_local)
    sub_cols = jnp.stack(
        [col_global < 3 * D, (col_global >= 3 * D) & (col_global < 4 * D), col_global >= 4 * D]
    ).astype(jnp.float32)
    sub_width = jnp.array([3 * D, D, FF], jnp.float32)
    square_in = grad_in * grad_in
    in_cols_new = decay_rate * in_cols[0] + (1.0 - decay_rate) * jnp.mean(
        square_in + tiny_square, axis=0
    )
    row_part_in = jnp.stack(
        [jnp.sum((square_in + tiny_square) * pick[None, :], axis=1) for pick in sub_cols]
    )
    row_weighted_in = jnp.stack(
        [jnp.sum(square_in * (pick / in_cols_new)[None, :], axis=1) for pick in sub_cols]
    )

    def rows_of(gradient, rows_old):
        return decay_rate * rows_old + (1.0 - decay_rate) * jnp.mean(
            gradient * gradient + tiny_square, axis=1
        )

    rows_new_down = rows_of(grad_down, down_rows[0])
    col_down, weighted_down = factor_stats(grad_down, rows_new_down)
    rows_new_word = rows_of(grad_word, word_rows)
    col_word, weighted_word = factor_stats(grad_word, rows_new_word)
    row_global = my_index * side_rows_local + jnp.arange(side_rows_local)
    is_pos = row_global < SEQ_LEN
    which = jnp.stack([is_pos, jnp.logical_not(is_pos)]).astype(jnp.float32)
    side_counts = jnp.array([SEQ_LEN, D], jnp.float32)
    rows_new_side = rows_of(grad_side, side_rows)
    square_side = grad_side * grad_side
    col_side = jnp.stack(
        [jnp.sum((square_side + tiny_square) * pick[:, None], axis=0) for pick in which]
    )
    weighted_side = jnp.stack(
        [jnp.sum(square_side * (pick / rows_new_side)[:, None], axis=0) for pick in which]
    )
    total_side = jnp.sum(which * rows_new_side[None, :], axis=1)
    seg_onehot = (
        segment_index(my_index * vec_local + jnp.arange(vec_local))[:, None]
        == jnp.arange(9 * LAYERS + 4)[None, :]
    )
    new_moment = decay_rate * vec_moment + (1.0 - decay_rate) * (grad_vec * grad_vec + tiny_square)
    vec_update = grad_vec * lax.rsqrt(new_moment)
    seg_part = jnp.sum(jnp.where(seg_onehot, (vec_update * vec_update)[:, None], 0.0), axis=0)
    parts = [
        row_part_in,
        row_weighted_in,
        col_down,
        weighted_down,
        col_word,
        weighted_word,
        col_side,
        weighted_side,
        total_side,
        jnp.sum(rows_new_down)[None],
        jnp.sum(rows_new_word)[None],
        seg_part,
        local_loss[None],
    ]
    summed = sum_over_devices(jnp.concatenate([p.reshape(-1) for p in parts]))
    sums, offset = [], 0
    for p in parts:
        sums.append(summed[offset : offset + p.size].reshape(p.shape))
        offset += p.size
    (
        row_sum_in,
        row_weighted_in,
        col_down,
        weighted_down,
        col_word,
        weighted_word,
        col_side,
        weighted_side,
        total_side,
        total_down,
        total_word,
        seg_squares,
        loss_total,
    ) = sums
    half = 1.0 - decay_rate
    rows_new_in = decay_rate * in_rows[0] + half * row_sum_in / sub_width[:, None]
    mean_in = jnp.mean(rows_new_in, axis=1)
    scale_in = clip_of(row_weighted_in, rows_new_in, mean_in, D * sub_width)

    def choose(options):
        return jnp.sum(sub_cols[:, None, :] * options[:, :, None], axis=0)

    row_sel_in = choose(rows_new_in)
    factor_in = jnp.sum(sub_cols * (learn_rate / scale_in)[:, None], axis=0)
    mean_sel_in = jnp.sum(sub_cols * mean_in[:, None], axis=0)
    new_in = layer_in[0] - factor_in[None, :] * grad_in * lax.rsqrt(
        row_sel_in * in_cols_new[None, :] / mean_sel_in[None, :]
    )
    cols_new_down = decay_rate * down_cols[0] + half * col_down / FF
    mean_down = total_down[0] / FF
    scale_down = clip_of(weighted_down, cols_new_down, mean_down, FF * D)
    new_down = layer_down[0] - (learn_rate / scale_down) * grad_down * lax.rsqrt(
        rows_new_down[:, None] * cols_new_down[None, :] / mean_down
    )
    cols_new_word = decay_rate * word_cols + half * col_word / VOCAB
    mean_word = total_word[0] / VOCAB
    scale_word = clip_of(weighted_word, cols_new_word, mean_word, VOCAB * D)
    new_word = word_table - (learn_rate / scale_word) * grad_word * lax.rsqrt(
        rows_new_word[:, None] * cols_new_word[None, :] / mean_word
    )
    cols_new_side = decay_rate * side_cols + half * col_side / side_counts[:, None]
    mean_side = total_side / side_counts
    scale_side = clip_of(weighted_side, cols_new_side, mean_side, side_counts * D)
    col_sel_side = jnp.where(is_pos[:, None], cols_new_side[0][None, :], cols_new_side[1][None, :])
    mean_sel_side = jnp.where(is_pos, mean_side[0], mean_side[1])
    factor_side = learn_rate / jnp.where(is_pos, scale_side[0], scale_side[1])
    new_side = side_mat - factor_side[:, None] * grad_side * lax.rsqrt(
        rows_new_side[:, None] * col_sel_side / mean_sel_side[:, None]
    )
    seg_scale = jnp.maximum(1.0, jnp.sqrt(seg_squares / segment_sizes()))
    vec_scale = jnp.sum(jnp.where(seg_onehot, seg_scale[None, :], 0.0), axis=1)
    new_vectors = vectors - learn_rate * vec_update / vec_scale
    return (
        loss_total[0],
        new_in[None],
        rows_new_in[None],
        in_cols_new[None],
        new_in.astype(LOW)[None],
        new_down[None],
        rows_new_down[None],
        cols_new_down[None],
        new_down.astype(LOW)[None],
        new_word,
        rows_new_word,
        cols_new_word,
        new_word.astype(LOW),
        new_side,
        rows_new_side,
        cols_new_side,
        new_side.astype(LOW),
        new_vectors,
        new_moment,
        new_vectors.astype(LOW),
    )


def solution(mesh):
    return jax.shard_map(
        local,
        mesh=mesh,
        in_specs=(
            P(("fsdp", "dp"), None),
            P(("fsdp", "dp"), None),
            P(("fsdp", "dp"), None),
            P(("fsdp", "dp")),
            P(None, None, ("fsdp", "dp")),
            P(None, ("fsdp", "dp"), None),
            P(("fsdp", "dp"), None),
            P(("fsdp", "dp"), None),
            P(("fsdp", "dp")),
            P(),
            P(None, ("fsdp", "dp")),
            P(None, ("fsdp", "dp")),
            P(),
            P(("fsdp", "dp")),
            P(),
            P(("fsdp", "dp")),
            P(),
            P(("fsdp", "dp")),
        ),
        out_specs=(
            P(),
            P(None, None, ("fsdp", "dp")),
            P(),
            P(None, ("fsdp", "dp")),
            P(None, None, ("fsdp", "dp")),
            P(None, ("fsdp", "dp"), None),
            P(None, ("fsdp", "dp")),
            P(),
            P(None, ("fsdp", "dp"), None),
            P(("fsdp", "dp"), None),
            P(("fsdp", "dp")),
            P(),
            P(("fsdp", "dp"), None),
            P(("fsdp", "dp"), None),
            P(("fsdp", "dp")),
            P(),
            P(("fsdp", "dp"), None),
            P(("fsdp", "dp")),
            P(("fsdp", "dp")),
            P(("fsdp", "dp")),
        ),
        check_vma=False,
    )
```

```python
import functools
import math

import jax
import jax.numpy as jnp
from jax import lax
from jax.experimental import pallas as pl
from jax.experimental.pallas import tpu as pltpu
from jax.sharding import PartitionSpec as P

D = 1024
HEADS = 16
HEAD_DIM = 64
FF = 4096
VOCAB = 30720
SEQ_LEN = 512
LAYERS = 1
MICRO = 2
BOTH = ("fsdp", "dp")
LOW = jnp.bfloat16
MESH = pl.DeviceIdType.MESH
ALL = slice(None)


learn_rate = 0.02
decay_rate = 0.5
tiny_square = 1e-30
norm_epsilon = 1e-12
precise = lax.Precision.HIGHEST


def layer_norm(inputs, norm_gain, norm_shift):
    center = inputs - jnp.mean(inputs, axis=-1, keepdims=True)
    spread = jnp.mean(center * center, axis=-1, keepdims=True)
    return center * lax.rsqrt(spread + norm_epsilon) * norm_gain + norm_shift


def norm_back(inputs, norm_gain, norm_shift, cotangent):
    result, pull = jax.vjp(layer_norm, inputs, norm_gain, norm_shift)
    return pull(cotangent)


def exact_gelu(inputs):
    return jax.nn.gelu(inputs, approximate=False)


def gelu_back(inputs, cotangent):
    result, pull = jax.vjp(exact_gelu, inputs)
    return pull(cotangent)[0]


def multiply(left_side, right_side):
    return jnp.dot(left_side, right_side, preferred_element_type=jnp.float32)


def multiply_left(left_side, right_side):
    return lax.dot_general(
        left_side, right_side, (((0,), (0,)), ((), ())), preferred_element_type=jnp.float32
    )


def multiply_right(left_side, right_side):
    return lax.dot_general(
        left_side, right_side, (((1,), (1,)), ((), ())), preferred_element_type=jnp.float32
    )


def piece_bounds():
    return [0, D, 2 * D, 3 * D, 4 * D, 5 * D, 5 * D + FF, 6 * D + FF, 7 * D + FF, 8 * D + FF]


def layer_slices(all_vectors, layer_index):
    bounds = piece_bounds()
    offset = layer_index * (8 * D + FF)
    return [
        all_vectors[offset + bounds[slot_index] : offset + bounds[slot_index + 1]]
        for slot_index in range(9)
    ]


def segment_index(position):
    piece_width = 8 * D + FF
    inner = position % piece_width
    layer_of = position // piece_width
    bounds = piece_bounds()[1:-1]
    local_segment = sum(((inner >= bound).astype(jnp.int32) for bound in bounds))
    tail = 9 * LAYERS + (position - LAYERS * piece_width) // D
    return jnp.where(position < LAYERS * piece_width, 9 * layer_of + local_segment, tail)


def segment_sizes():
    sizes = []
    sizes = sizes + [D, D, D, D, D, FF, D, D, D]
    return jnp.array(sizes + [D, D, D, D], jnp.float32)


def head_parts(ref):
    both = ref[...]
    return both[:, :HEAD_DIM], both[:, HEAD_DIM:]


def key_scores(queries, key_rows):
    return multiply_right(key_rows, queries) * HEAD_DIM ** (-0.5)


def attend_kernel(q_ref, k_ref, v_ref, context_ref, total_ref):
    contexts = []
    for head, (queries, key_rows, values) in enumerate(
        zip(head_parts(q_ref), head_parts(k_ref), head_parts(v_ref))
    ):
        scores = key_scores(queries, key_rows)
        peak = jnp.max(scores, axis=0, keepdims=True)
        exponent = jnp.exp(scores - peak)
        running = jnp.sum(exponent, axis=0, keepdims=True)
        soft_probs = (exponent / running).astype(LOW)
        contexts.append(multiply_left(values, soft_probs))
        total_ref[head] = peak + jnp.log(running)
    context_ref[...] = jnp.concatenate(contexts, axis=0).T.astype(LOW)


def attend_back_kernel(q_ref, k_ref, v_ref, d_ref, total_ref, out_ref):
    scale = HEAD_DIM ** (-0.5)
    for head, (queries, key_rows, values, d_context) in enumerate(
        zip(head_parts(q_ref), head_parts(k_ref), head_parts(v_ref), head_parts(d_ref))
    ):
        soft_probs = jnp.exp(key_scores(queries, key_rows) - total_ref[head])
        d_values = multiply(soft_probs.astype(LOW), d_context)
        d_probs = multiply_right(values, d_context)
        inner = jnp.sum(d_probs * soft_probs, axis=0, keepdims=True)
        d_scores = (soft_probs * (d_probs - inner)).astype(LOW)
        part = pl.ds(head * HEAD_DIM, HEAD_DIM)
        out_ref[0, part] = (multiply_left(key_rows, d_scores) * scale).astype(LOW)
        out_ref[1, part] = (multiply(d_scores, queries) * scale).T.astype(LOW)
        out_ref[2, part] = d_values.T.astype(LOW)


def attention_specs(tokens, length):
    pairs = HEADS // 2
    wide = 2 * HEAD_DIM

    def joint(third):
        return pl.BlockSpec((length, wide), lambda s, i: (s, third * pairs + i))

    total = pl.BlockSpec((2, 1, length), lambda s, i: (i, 0, s))
    return (tokens // length, pairs), [joint(0), joint(1), joint(2)], joint(0), total


def attend(projected, seq_dev):
    tokens = projected.shape[0]
    grid, ins, context, total = attention_specs(tokens, tokens // seq_dev)
    return pl.pallas_call(
        attend_kernel,
        name="attend",
        grid=grid,
        in_specs=ins,
        out_specs=(context, total),
        out_shape=(
            jax.ShapeDtypeStruct((tokens, D), LOW),
            jax.ShapeDtypeStruct((HEADS, 1, tokens), jnp.float32),
        ),
    )(projected, projected, projected)


def attend_back(projected, log_total, d_context, seq_dev):
    tokens = projected.shape[0]
    length = tokens // seq_dev
    grid, ins, context, total = attention_specs(tokens, length)
    return pl.pallas_call(
        attend_back_kernel,
        name="attend_back",
        grid=grid,
        in_specs=ins + [context, total],
        out_specs=pl.BlockSpec((3, 2 * HEAD_DIM, length), lambda s, i: (0, i, s)),
        out_shape=jax.ShapeDtypeStruct((3, D, tokens), LOW),
    )(projected, projected, projected, d_context, log_total).reshape(3 * D, tokens)


def lift_kernel(weight_ref, bias_ref, middle_ref, active_ref, slope_ref):
    lifted = multiply_right(weight_ref[...], middle_ref[...]) + bias_ref[...]
    cumulative = 0.5 + 0.5 * lax.erf(lifted * (0.5**0.5))
    density = jnp.exp(-0.5 * lifted * lifted) * ((0.5 / math.pi) ** 0.5)
    active_ref[...] = (lifted * cumulative).astype(LOW)
    slope_ref[...] = cumulative + lifted * density


def lift(weight_in, bias_up, middle_low):
    tokens = middle_low.shape[0]
    rows = 512
    return pl.pallas_call(
        lift_kernel,
        name="lift",
        grid=(FF // rows,),
        in_specs=[
            pl.BlockSpec((rows, D), lambda i: (4 * D // rows + i, 0)),
            pl.BlockSpec((rows, 1), lambda i: (i, 0)),
            pl.BlockSpec((tokens, D), lambda i: (0, 0)),
        ],
        out_specs=(
            pl.BlockSpec((rows, tokens), lambda i: (i, 0)),
            pl.BlockSpec((rows, tokens), lambda i: (i, 0)),
        ),
        out_shape=(
            jax.ShapeDtypeStruct((FF, tokens), LOW),
            jax.ShapeDtypeStruct((FF, tokens), jnp.float32),
        ),
    )(weight_in, bias_up[:, None], middle_low)


def lift_back_kernel(down_ref, d_ref, slope_ref, up_ref, out_ref, total_ref, sums_ref):
    d_lifted = (multiply_right(down_ref[...], d_ref[...]) * slope_ref[...]).astype(LOW)
    out_ref[...] = d_lifted
    sums_ref[...] = jnp.sum(d_lifted.astype(jnp.float32), axis=1, keepdims=True)
    part = multiply_left(d_lifted, up_ref[...])

    @pl.when(pl.program_id(0) == 0)
    def _():
        total_ref[...] = part

    @pl.when(pl.program_id(0) > 0)
    def _():
        total_ref[...] += part


def lift_back(weight_in, weight_down, slope, d_down_low):
    tokens = d_down_low.shape[0]
    rows = 512
    block = pl.BlockSpec((rows, D), lambda i: (i, 0))
    whole = pl.BlockSpec((tokens, D), lambda i: (0, 0))
    hidden = pl.BlockSpec((rows, tokens), lambda i: (i, 0))
    d_lifted, d_middle, sums = pl.pallas_call(
        lift_back_kernel,
        name="lift_back",
        grid=(FF // rows,),
        in_specs=[block, whole, hidden, pl.BlockSpec((rows, D), lambda i: (4 * D // rows + i, 0))],
        out_specs=(hidden, whole, pl.BlockSpec((rows, 1), lambda i: (i, 0))),
        out_shape=(
            jax.ShapeDtypeStruct((FF, tokens), LOW),
            jax.ShapeDtypeStruct((tokens, D), jnp.float32),
            jax.ShapeDtypeStruct((FF, 1), jnp.float32),
        ),
    )(weight_down, d_down_low, slope, weight_in)
    return d_lifted, d_middle, sums[:, 0]


def layer_forward(hidden, weight_in, weight_down, pieces, seq_dev):
    bias_q, bias_v, bias_o, gain_a, shift_a, bias_up, bias_down, gain_b, shift_b = pieces
    hidden_low = hidden.astype(jnp.bfloat16)
    joint_bias = jnp.concatenate([bias_q, jnp.zeros_like(bias_q), bias_v])
    projected = (multiply_right(hidden_low, weight_in[: 3 * D]) + joint_bias).astype(jnp.bfloat16)
    context_low, log_total = attend(projected, seq_dev)
    mid_in = hidden + (multiply_right(context_low, weight_in[3 * D : 4 * D]) + bias_o)
    middle = layer_norm(mid_in, gain_a, shift_a)
    middle_low = middle.astype(jnp.bfloat16)
    active_low, slope = lift(weight_in, bias_up, middle_low)
    out_in = middle + (multiply_left(active_low, weight_down) + bias_down)
    output = layer_norm(out_in, gain_b, shift_b)
    return (
        output,
        (
            hidden_low,
            projected,
            log_total,
            context_low,
            mid_in,
            middle_low,
            slope,
            active_low,
            out_in,
        ),
    )


def layer_backward(grad_out, weight_in, weight_down, pieces, kept, seq_dev):
    bias_q, bias_v, bias_o, gain_a, shift_a, bias_up, bias_down, gain_b, shift_b = pieces
    (
        hidden_low,
        projected,
        log_total,
        context_low,
        mid_in,
        middle_low,
        slope,
        active_low,
        out_in,
    ) = kept
    d_out_in, d_gain_b, d_shift_b = norm_back(out_in, gain_b, shift_b, grad_out)
    d_down_low = d_out_in.astype(jnp.bfloat16)
    d_lifted_low, d_from_up, d_bias_up = lift_back(weight_in, weight_down, slope, d_down_low)
    d_middle = d_out_in + d_from_up
    d_mid_in, d_gain_a, d_shift_a = norm_back(mid_in, gain_a, shift_a, d_middle)
    d_attended_low = d_mid_in.astype(jnp.bfloat16)
    d_context_low = multiply(d_attended_low, weight_in[3 * D : 4 * D]).astype(jnp.bfloat16)
    d_projected_low = attend_back(projected, log_total, d_context_low, seq_dev)
    d_hidden = d_mid_in + multiply_left(d_projected_low, weight_in[: 3 * D])
    joint_sums = jnp.sum(d_projected_low.astype(jnp.float32), axis=1)
    grad_pieces = jnp.concatenate(
        [
            joint_sums[:D],
            joint_sums[2 * D :],
            jnp.sum(d_attended_low.astype(jnp.float32), axis=0),
            d_gain_a,
            d_shift_a,
            d_bias_up,
            jnp.sum(d_down_low.astype(jnp.float32), axis=0),
            d_gain_b,
            d_shift_b,
        ]
    )
    return (
        d_hidden,
        (
            active_low,
            d_down_low,
            d_lifted_low,
            middle_low,
            d_projected_low,
            hidden_low,
            d_attended_low.T,
            context_low,
        ),
        grad_pieces,
    )


def place():
    block = lax.axis_index("fsdp")
    return block // 4, (block // 2) % 2, block % 2, lax.axis_index("dp")


def device(z, y, x, c):
    return ((z * 2 + y) * 2 + x, c)


def my_rank():
    return lax.axis_index("fsdp") * 2 + lax.axis_index("dp")


def by_rank(index):
    return (index // 2, index % 2)


def neighbours(z, y, x, c):
    return (
        device(z, y, 1 - x, c),
        device(z, 1 - y, x, c),
        device(z, y, x, 1 - c),
        [device((z + k) % 4, y, x, c) for k in (1, 2, 3)],
    )


def greet(n):
    me = my_rank()
    barrier = pltpu.get_barrier_semaphore()

    def one(step, carry):
        pl.semaphore_signal(
            barrier, inc=1, device_id=by_rank((me + step) % n), device_id_type=MESH
        )
        return carry

    lax.fori_loop(1, n, one, 0)


def welcome(n):
    pl.semaphore_wait(pltpu.get_barrier_semaphore(), n - 1)


def enter(n):
    greet(n)
    welcome(n)


class Copies:
    def __init__(self, send, recv):
        self.send, self.recv, self.begun, self.count = send, recv, {}, 0

    def start(self, src, dst, target):
        slot = self.count
        self.count += 1
        copy = pltpu.make_async_remote_copy(
            src_ref=src,
            dst_ref=dst,
            send_sem=self.send.at[slot],
            recv_sem=self.recv.at[slot],
            device_id=target,
            device_id_type=MESH,
        )
        copy.start()
        self.begun[id(copy)] = copy
        return copy

    def sent(self, copy):
        self.begun.pop(id(copy)).wait_send()

    def drain(self):
        for copy in self.begun.values():
            copy.wait_send()


def exchange_copy(src, dst, send, recv, step, n):
    me = my_rank()
    target = (me + step) % n
    return pltpu.make_async_remote_copy(
        src_ref=src.at[target],
        dst_ref=dst.at[me],
        send_sem=send.at[step],
        recv_sem=recv.at[step],
        device_id=by_rank(target),
        device_id_type=MESH,
    )


def exchange_start(src, dst, send, recv, n):
    def begin(step, carry):
        exchange_copy(src, dst, send, recv, step, n).start()
        return carry

    lax.fori_loop(1, n, begin, 0)


def exchange_wait(src, dst, send, recv, n):
    def finish(step, carry):
        exchange_copy(src, dst, send, recv, step, n).wait()
        return carry

    lax.fori_loop(1, n, finish, 0)


LEAD, LOOK = 3, 2
TILES = ((64,), (64, 64, 64), (64, 64))
PLANE = {1: 64}


def gather_steps(plan):
    first = [i for i, p in enumerate(plan) if p[3]]
    rest = [i for i, p in enumerate(plan) if not p[3]]
    order, task = first + rest[:LEAD] + first, 0
    for step in range(len(rest) + 4):
        if step + LEAD < len(rest):
            order.append(rest[step + LEAD])
        order += [rest[i] for i in range(min(step, len(rest) - 1), -1, -1) if step - i < 4]
        if step == LOOK:
            order += first
        if step >= LOOK and task < 4:
            task += 1
            order.append(-task)
    return order + first + first


def count_from(index, shape, axis):
    return lax.broadcasted_iota(jnp.int32, shape, axis) == index


def one_hot(mask):
    return jnp.where(mask, 1.0, 0.0).astype(LOW)


def fill_slots(blocks, values, tally, to_slot, message):
    n, capacity, lanes = message.shape
    tokens = blocks.shape[1]
    owner = blocks[...]
    member = count_from(owner, (n, tokens), 0)
    earlier = one_hot(
        lax.broadcasted_iota(jnp.int32, (tokens, tokens), 0)
        < lax.broadcasted_iota(jnp.int32, (tokens, tokens), 1)
    )
    ahead = multiply(one_hot(member), earlier)
    rank = jnp.sum(jnp.where(member, ahead, 0.0), axis=0, keepdims=True).astype(jnp.int32)
    slot = owner * capacity + rank
    to_slot[...] = one_hot(count_from(slot, (n * capacity, tokens), 0))
    listed = multiply(to_slot[...], values[...]) + tally[...]
    message[...] = listed.reshape(n, capacity, lanes)


def look_up(index, answer, table, from_slot, found):
    n, capacity, lanes = answer.shape
    group = n // 4
    part = pl.ds(index * group, group)
    wanted = answer[part].reshape(group * capacity, lanes)
    row = (wanted[:, 0:1] * 256.0 + wanted[:, 1:2]).astype(jnp.int32)
    row = jnp.where(wanted[:, 2:3] > 0.5, row, -1)
    hot = one_hot(count_from(row, (group * capacity, table.shape[0]), 1))
    from_slot[part] = hot.reshape(group, capacity, -1)
    found[part] = multiply(hot, table[...]).astype(LOW).reshape(group, capacity, -1)


def gather_kernel(plan, count, *refs):
    local = refs[:count]
    blocks, values, tally, table = refs[count : count + 4]
    out = refs[count + 4 : 2 * count + 4]
    rows, to_slot, from_slot, answer = refs[2 * count + 4 : 2 * count + 8]
    message, found, send, recv, own_sem, ask_send, ask_recv, row_send, row_recv = refs[
        2 * count + 8 :
    ]
    z, y, x, c = place()
    n = 32
    me = my_rank()
    greet(n)
    fill_slots(blocks, values, tally, to_slot, message)
    answer[me] = message[me]
    welcome(n)
    copies = Copies(send, recv)
    exchange_start(message, answer, ask_send, ask_recv, n)
    own = []
    for i in range(count):
        own.append(pltpu.make_async_copy(local[i], out[i].at[z, y, x, c], own_sem.at[i]))
        own[i].start()
    to_x, to_y, to_core, to_z = neighbours(z, y, x, c)

    def pass_on(ref, where, target):
        return copies.start(ref.at[where], ref.at[where], target)

    landed = set()

    def own_there(i):
        if i not in landed:
            own[i].wait()
            landed.add(i)

    def chunk(i, start, size, plane_first):
        ref, mine, half = out[i], local[i], size // 2
        part, low, high = pl.ds(start, size), pl.ds(start, half), pl.ds(start + half, half)
        last = []
        if not plane_first:
            along = [copies.start(mine.at[part], ref.at[z, y, x, c, part], t) for t in to_z]
            yield
            for copy in along:
                copy.wait_recv()
            own_there(i)
            first = pass_on(ref, (ALL, y, x, c, low), to_x)
            second = pass_on(ref, (ALL, y, x, c, high), to_y)
            last.append(pass_on(ref, (ALL, y, x, c, part), to_core))
            yield
            first.wait_recv()
            second.wait_recv()
            first = pass_on(ref, (ALL, y, ALL, c, low), to_y)
            second = pass_on(ref, (ALL, ALL, x, c, high), to_x)
            last.append(pass_on(ref, (ALL, y, 1 - x, c, low), to_core))
            last.append(pass_on(ref, (ALL, 1 - y, x, c, high), to_core))
            yield
            first.wait_recv()
            second.wait_recv()
            last.append(pass_on(ref, (ALL, 1 - y, ALL, c, low), to_core))
            last.append(pass_on(ref, (ALL, ALL, 1 - x, c, high), to_core))
        else:
            first = copies.start(mine.at[low], ref.at[z, y, x, c, low], to_x)
            second = copies.start(mine.at[high], ref.at[z, y, x, c, high], to_y)
            last.append(copies.start(mine.at[part], ref.at[z, y, x, c, part], to_core))
            yield
            first.wait_recv()
            second.wait_recv()
            own_there(i)
            first = pass_on(ref, (z, y, ALL, c, low), to_y)
            second = pass_on(ref, (z, ALL, x, c, high), to_x)
            last.append(pass_on(ref, (z, y, 1 - x, c, low), to_core))
            last.append(pass_on(ref, (z, 1 - y, x, c, high), to_core))
            yield
            first.wait_recv()
            second.wait_recv()
            along = [pass_on(ref, (z, ALL, ALL, c, part), t) for t in to_z]
            last.append(pass_on(ref, (z, 1 - y, ALL, c, low), to_core))
            last.append(pass_on(ref, (z, ALL, 1 - x, c, high), to_core))
            yield
            for k in (1, 2, 3):
                along[k - 1].wait_recv()
                last.append(pass_on(ref, ((z + 4 - k) % 4, ALL, ALL, c, part), to_core))
        yield
        for copy in last:
            copy.wait_recv()
        yield

    chunks = [chunk(*p) for p in plan]
    keep = pltpu.make_async_copy(found.at[me], rows.at[me], own_sem.at[count])

    def row_copy(slot, target, source):
        return pltpu.make_async_remote_copy(
            src_ref=found.at[target],
            dst_ref=rows.at[source],
            send_sem=row_send.at[slot],
            recv_sem=row_recv.at[source],
            device_id=by_rank(target),
            device_id_type=MESH,
        )

    def plane_rank(slot):
        return (z + slot // 8) % 4 * 8 + (me + slot) % 8

    def send_row(slot, carry):
        row_copy(slot, plane_rank(slot), me).start()
        return carry

    for index in gather_steps(plan):
        if index >= 0:
            next(chunks[index], None)
            continue
        task = -index - 1
        if task == 0:
            exchange_wait(message, answer, ask_send, ask_recv, n)
        look_up((z + task) % 4, answer, table, from_slot, found)
        if task == 0:
            keep.start()
        lax.fori_loop(max(task * 8, 1), task * 8 + 8, send_row, 0)

    def finish_row(slot, carry):
        row_copy(slot, plane_rank(slot), me).wait_send()
        row_copy(slot, me, (me + slot) % n).wait_recv()
        return carry

    lax.fori_loop(1, n, finish_row, 0)
    keep.wait()
    copies.drain()
    for i in range(count):
        own_there(i)


def gather_plan(heights):
    plan = []
    for i, height in enumerate(heights):
        start = 0
        if i in PLANE:
            plan.append((i, 0, PLANE[i], True))
            start = PLANE[i]
        for size in TILES[i]:
            plan.append((i, start, size, False))
            start += size
        assert start == height
    return plan


def gather_weights(arrays, blocks, values, tally, table):
    count = len(arrays)
    n, capacity = 32, 32
    tokens = blocks.shape[1]
    plan = gather_plan([a.shape[0] for a in arrays])
    total = sum(15 if p[3] else 12 for p in plan)
    hbm = pl.BlockSpec(memory_space=pl.ANY)
    vmem = pl.BlockSpec(memory_space=pltpu.VMEM)
    dma = pltpu.SemaphoreType.DMA
    shape = jax.ShapeDtypeStruct
    return pl.pallas_call(
        functools.partial(gather_kernel, plan, count),
        name="gather_weights",
        out_shape=tuple(shape((4, 2, 2, 2) + a.shape, a.dtype) for a in arrays)
        + (
            shape((n, capacity, D), LOW),
            shape((n * capacity, tokens), LOW),
            shape((n, capacity, table.shape[0]), LOW),
            shape((n, capacity, 128), jnp.float32),
        ),
        in_specs=[vmem] * (count + 4),
        out_specs=tuple([hbm] * (count + 1) + [vmem] * 3),
        scratch_shapes=[
            pltpu.VMEM((n, capacity, 128), jnp.float32),
            pltpu.VMEM((n, capacity, D), LOW),
            dma((total,)),
            dma((total,)),
            dma((count + 1,)),
        ]
        + [dma((n,))] * 4,
        compiler_params=pltpu.CompilerParams(collective_id=0, has_side_effects=True),
    )(*arrays, blocks, values, tally, table)


def add_blocks(dst, other, shape, at_dst, at_other):
    def body(index, carry):
        where = []
        for extent in reversed(shape):
            where.append(index % extent)
            index = index // extent
        where = tuple(reversed(where))
        d, o = at_dst(*where), at_other(*where)
        total = dst[d].astype(jnp.float32) + other[o].astype(jnp.float32)
        dst[d] = total.astype(dst.dtype)
        return carry

    lax.fori_loop(0, math.prod(shape), body, 0)


WIDE = 256


class Group:
    def __init__(self, z0, nz, height, sources, out):
        self.z0, self.nz, self.height, self.sources, self.out = z0, nz, height, sources, out

    def scratch(self):
        nz, h, n = self.nz, self.height, D // WIDE
        shapes = [(2, nz, 2, 2, h), (n, nz, 2, 2, h)] + [(n, nz, 2, h // 2)] * 2
        shapes += [(n, nz, h // 2)] * 2 + [(n, 3, h)]
        return [pltpu.VMEM(shape + (WIDE,), LOW) for shape in shapes]


def each_block(group, refs, wide, core, body):
    for start, stop, left, right, base, together in group.sources:
        def one(step, carry, left=left, right=right, base=base, together=together):
            index = step * together
            part = refs[left][pl.ds(index - base, together), core]
            product = multiply(part.reshape(-1, part.shape[-1]), refs[right][:, wide])
            product = product.reshape(together, group.height, WIDE)
            for k in range(together):
                at = index + k
                body((at // 4, (at // 2) % 2, at % 2), product[k])
            return carry

        lax.fori_loop(start // together, stop // together, one, 0)


def scatter_kernel(groups, n_left, *refs):
    operands = refs[:n_left]
    side, buckets, vector = refs[n_left : n_left + 3]
    out = refs[n_left + 3 : n_left + 6]
    arrived, vector_all = refs[n_left + 6 : n_left + 8]
    rest = refs[n_left + 8 :]
    scratch = [rest[7 * i : 7 * i + 7] for i in range(len(groups))]
    side_scratch = rest[7 * len(groups) : 7 * len(groups) + 7]
    (send, recv, z_send, z_recv, load, row_send, row_recv, vec_send, vec_recv) = rest[
        7 * len(groups) + 7 :
    ]
    z, y, x, c = place()
    n = 32
    me = my_rank()
    enter(n)
    copies = Copies(send, recv)
    to_x, to_y, to_core, to_z = neighbours(z, y, x, c)
    own = [
        pltpu.make_async_copy(buckets.at[me], arrived.at[me], load.at[0]),
        pltpu.make_async_copy(vector.at[me], vector_all.at[me], load.at[1]),
    ]
    for copy in own:
        copy.start()
    sent_before = {}

    def product_chunk(slot, which, index):
        group = groups[which]
        outgoing, held, low_1, high_1, low_2, high_2, from_z = scratch[which]
        nz, h = group.nz, group.height
        wide = pl.ds(index * WIDE, WIDE)
        low, high = pl.ds(0, h // 2), pl.ds(h // 2, h // 2)
        here = index % 2
        if index >= 2:
            copies.sent(sent_before[which, index - 2])

        def send_off(where, value):
            outgoing[(here,) + where] = value.astype(LOW)

        each_block(group, operands, wide, 1 - c, send_off)
        core = copies.start(outgoing.at[here], held.at[index], to_core)
        sent_before[which, index] = core
        yield
        core.wait_recv()

        def add_own(where, value):
            spot = (index,) + where
            held[spot] = (value + held[spot].astype(jnp.float32)).astype(LOW)

        each_block(group, operands, wide, c, add_own)
        first = copies.start(held.at[index, :, 1 - y, :, low], low_1.at[index], to_y)
        second = copies.start(held.at[index, :, :, 1 - x, high], high_1.at[index], to_x)
        yield
        first.wait_recv()
        second.wait_recv()
        add_blocks(
            held, low_1, (nz, 2), lambda a, d: (index, a, y, d, low), lambda a, d: (index, a, d)
        )
        add_blocks(
            held, high_1, (nz, 2), lambda a, b: (index, a, b, x, high), lambda a, b: (index, a, b)
        )
        first = copies.start(held.at[index, :, y, 1 - x, low], low_2.at[index], to_x)
        second = copies.start(held.at[index, :, 1 - y, x, high], high_2.at[index], to_y)
        yield
        first.wait_recv()
        second.wait_recv()
        add_blocks(held, low_2, (nz,), lambda a: (index, a, y, x, low), lambda a: (index, a))
        add_blocks(held, high_2, (nz,), lambda a: (index, a, y, x, high), lambda a: (index, a))

        def along(level, back):
            return pltpu.make_async_remote_copy(
                src_ref=held.at[index, level, y, x],
                dst_ref=from_z.at[index, back],
                send_sem=z_send.at[slot, level],
                recv_sem=z_recv.at[slot, back],
                device_id=device(group.z0 + level, y, x, c),
                device_id_type=MESH,
            )

        for level in range(nz):
            away = z != group.z0 + level

            @pl.when(away)
            def _(level=level):
                along(level, (z - group.z0 - level + 3) % 4).start()

        yield

        def finish():
            for back in range(3):
                along(0, back).wait_recv()
            mine = held[index, z - group.z0, y, x].astype(jnp.float32)
            for back in range(3):
                mine = mine + from_z[index, back].astype(jnp.float32)
            out[group.out][:, wide] = mine

        if nz == 4:
            finish()
        else:
            pl.when((z >= group.z0) & (z < group.z0 + nz))(finish)
        yield
        for level in range(nz):
            away = z != group.z0 + level

            @pl.when(away)
            def _(level=level):
                along(level, (z - group.z0 - level + 3) % 4).wait_send()

        yield

    def side_chunk():
        held, from_core, low_1, high_1, low_2, high_2, from_z = side_scratch
        size = held.shape[3]
        half = size // 32 * 16 + 16
        low, high = pl.ds(0, half), pl.ds(half, size - half)
        core = copies.start(side.at[:, :, :, 1 - c], from_core, to_core)
        mine = pltpu.make_async_copy(side.at[:, :, :, c], held, load.at[2])
        mine.start()
        yield
        mine.wait()
        core.wait_recv()
        add_blocks(held, from_core, (4, 2, 2), lambda *w: w, lambda *w: w)
        first = copies.start(held.at[:, 1 - y, :, low], low_1, to_y)
        second = copies.start(held.at[:, :, 1 - x, high], high_1, to_x)
        yield
        first.wait_recv()
        second.wait_recv()
        add_blocks(held, low_1, (4, 2), lambda a, d: (a, y, d, low), lambda a, d: (a, d))
        add_blocks(held, high_1, (4, 2), lambda a, b: (a, b, x, high), lambda a, b: (a, b))
        first = copies.start(held.at[:, y, 1 - x, low], low_2, to_x)
        second = copies.start(held.at[:, 1 - y, x, high], high_2, to_y)
        yield
        first.wait_recv()
        second.wait_recv()
        add_blocks(held, low_2, (4,), lambda a: (a, y, x, low), lambda a: (a,))
        add_blocks(held, high_2, (4,), lambda a: (a, y, x, high), lambda a: (a,))
        along = [
            copies.start(held.at[(z + k) % 4, y, x], from_z.at[k - 1], to_z[k - 1])
            for k in (1, 2, 3)
        ]
        yield
        for copy in along:
            copy.wait_recv()
        total = held[z, y, x].astype(jnp.float32)
        for k in range(3):
            total = total + from_z[k].astype(jnp.float32)
        out[2][...] = total
        yield
        yield

    parts = [(which, index) for index in range(D // WIDE) for which in ORDER]
    chunks = [side_chunk()] + [product_chunk(slot, *p) for slot, p in enumerate(parts)]
    exchange_start(vector, vector_all, vec_send, vec_recv, n)
    for step in range(len(chunks) + 5):
        for index in range(min(step, len(chunks) - 1), -1, -1):
            if step - index < 6:
                next(chunks[index], None)
        if step == ROWS_AT:
            exchange_start(buckets, arrived, row_send, row_recv, n)
    exchange_wait(vector, vector_all, vec_send, vec_recv, n)
    exchange_wait(buckets, arrived, row_send, row_recv, n)
    copies.drain()
    for copy in own:
        copy.wait()


ROWS_AT = 0
ORDER = (0, 1, 2)


def scatter_grads(pairs, side, buckets, vector):
    blocked = []
    for i, pair in enumerate(pairs):
        height = FF // 32 if i == 0 else 256
        blocked.append(pair if i % 2 else pair.reshape(-1, 2, height, pair.shape[1]))
    groups = [
        Group(0, 4, FF // 32, [(0, 16, 0, 1, 0, 2)], 1),
        Group(2, 2, 256, [(0, 8, 2, 3, 0, 1)], 0),
        Group(0, 2, 256, [(0, 6, 4, 5, 0, 1), (6, 8, 6, 7, 6, 1)], 0),
    ]
    height = side.shape[4]
    half = height // 32 * 16 + 16
    hbm = pl.BlockSpec(memory_space=pl.ANY)
    vmem = pl.BlockSpec(memory_space=pltpu.VMEM)
    dma = pltpu.SemaphoreType.DMA
    scratch = [shape for group in groups for shape in group.scratch()]
    for lead in (
        (4, 2, 2, height),
        (4, 2, 2, height),
        (4, 2, half),
        (4, 2, height - half),
        (4, half),
        (4, height - half),
        (3, height),
    ):
        scratch.append(pltpu.VMEM(lead + (D,), LOW))
    chunks = len(groups) * D // WIDE
    total = 5 * chunks + 8
    shape = jax.ShapeDtypeStruct
    return pl.pallas_call(
        functools.partial(scatter_kernel, groups, len(pairs)),
        name="scatter_grads",
        out_shape=(
            shape((256, D), jnp.float32),
            shape((FF // 32, D), jnp.float32),
            shape((height, D), jnp.float32),
            shape(buckets.shape, buckets.dtype),
            shape(vector.shape, vector.dtype),
        ),
        in_specs=[vmem] * len(pairs) + [hbm] * 3,
        out_specs=(vmem, vmem, vmem, hbm, hbm),
        scratch_shapes=scratch
        + [
            dma((total,)),
            dma((total,)),
            dma((chunks, 4)),
            dma((chunks, 3)),
            dma((3,)),
        ]
        + [dma((32,))] * 4,
        compiler_params=pltpu.CompilerParams(
            collective_id=1, has_side_effects=True, vmem_limit_bytes=64000 * 1024
        ),
    )(*blocked, side, buckets, vector)


def sum_kernel(values, out, landed, total, send, recv, send_again, recv_again):
    n = 32
    me = my_rank()
    enter(n)
    exchange_start(values, landed, send, recv, n)
    landed[me] = values[me]
    exchange_wait(values, landed, send, recv, n)

    def add(index, carry):
        return carry + landed[index]

    total[...] = lax.fori_loop(0, n, add, jnp.zeros(total.shape, jnp.float32))
    out[me] = total[...]

    def copy(step):
        target = (me + step) % n
        return pltpu.make_async_remote_copy(
            src_ref=total,
            dst_ref=out.at[me],
            send_sem=send_again.at[step],
            recv_sem=recv_again.at[step],
            device_id=by_rank(target),
            device_id_type=MESH,
        )

    def begin(step, carry):
        copy(step).start()
        return carry

    def finish(step, carry):
        copy(step).wait()
        return carry

    lax.fori_loop(1, n, begin, 0)
    lax.fori_loop(1, n, finish, 0)


def sum_over_devices(flat):
    n = lax.axis_size(BOTH)
    if not special():
        return lax.psum(flat, BOTH)
    unit = n * 128
    lines = -(-flat.shape[0] // unit)
    values = jnp.pad(flat, (0, lines * unit - flat.shape[0])).reshape(n, lines, 128)
    vmem = pl.BlockSpec(memory_space=pltpu.VMEM)
    dma = pltpu.SemaphoreType.DMA
    result = pl.pallas_call(
        sum_kernel,
        name="sum_over_devices",
        out_shape=jax.ShapeDtypeStruct(values.shape, jnp.float32),
        in_specs=[vmem],
        out_specs=vmem,
        scratch_shapes=[
            pltpu.VMEM(values.shape, jnp.float32),
            pltpu.VMEM(values.shape[1:], jnp.float32),
            dma((n,)),
            dma((n,)),
            dma((n,)),
            dma((n,)),
        ],
        compiler_params=pltpu.CompilerParams(collective_id=2, has_side_effects=True),
    )(values)
    return result.reshape(-1)[: flat.shape[0]]


def special():
    return lax.axis_size("fsdp") == 16 and lax.axis_size("dp") == 2


def swap(blocks):
    shape = blocks.shape
    n_fsdp, n_dp = lax.axis_size("fsdp"), lax.axis_size("dp")
    split = blocks.reshape((n_fsdp, n_dp) + shape[1:])
    half = lax.all_to_all(split, "fsdp", split_axis=0, concat_axis=0, tiled=True)
    return lax.all_to_all(half, "dp", split_axis=1, concat_axis=1, tiled=True).reshape(shape)

def ask_rows(blocks, local_row, local_counts, block_rows, capacity):
    n = lax.axis_size(BOTH)
    onehot = (blocks[:, None] == jnp.arange(n)[None, :]).astype(jnp.int32)
    rank = jnp.sum(jnp.cumsum(onehot, axis=0) * onehot, axis=1) - 1
    slot = blocks * capacity + rank
    bucket_ids = jnp.full((n * capacity,), -1, jnp.int32).at[slot].set(local_row)
    message = jnp.concatenate(
        [
            bucket_ids.reshape(n, capacity),
            jnp.broadcast_to(local_counts[None, :], (n, MICRO)),
        ],
        axis=1,
    )
    answer = swap(message)
    asked = answer[:, :capacity].reshape(-1)
    to_slot = (jnp.arange(n * capacity)[:, None] == slot[None, :]).astype(LOW)
    from_slot = (asked[:, None] == jnp.arange(block_rows)[None, :]).astype(LOW)
    return to_slot, from_slot, jnp.sum(answer[:, capacity:], axis=0)


def gather_blocks(arrays, blocks, local_row, local_counts, table, capacity):
    n = lax.axis_size(BOTH)
    if special():
        row = local_row.astype(jnp.int32)
        values = jnp.stack([row // 256, row % 256, jnp.ones_like(row)], axis=1).astype(LOW)
        tally = jnp.pad(local_counts.astype(jnp.float32), (3, 125 - MICRO)).reshape(1, 128)
        *gathered, rows, to_slot, from_slot, answer = gather_weights(
            arrays, blocks.reshape(1, -1), jnp.pad(values, ((0, 0), (0, 125))), tally, table
        )
        full = [g.reshape((-1, a.shape[-1])) for g, a in zip(gathered, arrays)]
        counts = jnp.sum(answer[:, 0, 3 : 3 + MICRO], axis=0)
        return full, rows, to_slot, from_slot.reshape(n * capacity, -1), counts
    to_slot, from_slot, counts = ask_rows(
        blocks, local_row, local_counts, table.shape[0], capacity
    )
    found = multiply(from_slot, table).astype(LOW).reshape(n, capacity, D)
    full = [lax.all_gather(a, BOTH, axis=0, tiled=True) for a in arrays]
    return full, swap(found), to_slot, from_slot, counts.astype(jnp.float32)


def reduce_blocks(pairs, grad_pos, grad_head, buckets, vector):
    n = lax.axis_size(BOTH)
    if special():
        side = jnp.concatenate([grad_pos.astype(LOW), grad_head.astype(LOW)], axis=0)
        grad_in, grad_down, grad_side, arrived, pieces = scatter_grads(
            pairs, side.reshape(4, 2, 2, 2, -1, D), buckets, vector.reshape(n, -1, 128)
        )
        return grad_side, grad_in, grad_down, arrived, pieces
    down, up, joint, attended = [
        multiply(pairs[2 * i], pairs[2 * i + 1]) for i in range(4)
    ]

    def own(value):
        return lax.psum_scatter(value, BOTH, scatter_dimension=0, tiled=True)

    return (
        own(jnp.concatenate([grad_pos, grad_head], axis=0)),
        own(jnp.concatenate([joint, attended, up], axis=0)),
        own(down),
        swap(buckets),
        own(vector),
    )


def factor_stats(gradient, rows_new):
    square = gradient * gradient
    return jnp.sum(square + tiny_square, axis=0), jnp.sum(square / rows_new[:, None], axis=0)


def clip_of(weighted, cols_new, mean_rows, size):
    mean_square = jnp.sum(weighted / cols_new, axis=-1) * mean_rows / size
    return jnp.maximum(1.0, jnp.sqrt(mean_square))


DOWN, WORD, POS, HEAD, INNER, EXTRA = 0, 1, 2, 3, 4, 14
LOSS_LANE, TOTAL_LANE = 13, 16


def row_stats(gradient, rows_old):
    square = gradient * gradient
    floored = square + tiny_square
    rows_new = decay_rate * rows_old + (1.0 - decay_rate) * jnp.mean(
        floored, axis=1, keepdims=True
    )
    return rows_new, floored, square / rows_new


def down_rows_sum(value):
    return jnp.sum(value, axis=0, keepdims=True)


def lanes(width=D):
    return lax.broadcasted_iota(jnp.int32, (1, width), 1)


def upright(row, count, start=0):
    shape = (count, row.shape[1])
    at = start + lax.broadcasted_iota(jnp.int32, shape, 0)
    there = lax.broadcasted_iota(jnp.int32, shape, 1) == at
    return jnp.sum(jnp.where(there, row, 0.0), axis=1, keepdims=True)


def flat(column, width, start=0):
    shape = (column.shape[0], width)
    at = start + lax.broadcasted_iota(jnp.int32, shape, 0)
    there = lax.broadcasted_iota(jnp.int32, shape, 1) == at
    return jnp.sum(jnp.where(there, column, 0.0), axis=0, keepdims=True)


def inner_part(rank):
    return jnp.where(rank < 12, 0, jnp.where(rank < 16, 1, 2))


def own_segment(rank):
    start = rank * 512
    bounds = piece_bounds()[1:]
    inner = sum((jnp.where(start >= bound, 1, 0) for bound in bounds))
    tail = sum((jnp.where(start >= bounds[-1] + D * k, 1, 0) for k in (1, 2, 3)))
    return inner + tail


def position_rows(rank, count):
    rows = rank * count + lax.broadcasted_iota(jnp.int32, (count, 1), 0)
    return rows < SEQ_LEN


def stats_kernel(
    g_in,
    g_down,
    g_side,
    pieces,
    word,
    in_old,
    down_old,
    side_old,
    word_old,
    moment_old,
    loss,
    in_new,
    down_new,
    side_new,
    word_new,
    moment_new,
    update,
    payload,
    held,
):
    rank = my_rank()
    step = pl.program_id(0)

    @pl.when(step == 0)
    def _():
        lane = lanes()
        payload[...] = jnp.zeros_like(payload)
        held[...] = jnp.zeros_like(held)
        word_new[...] = jnp.zeros_like(word_new)
        rows, floored, weighted = row_stats(g_in[...], upright(in_old[...], g_in.shape[0]))
        in_new[...] = flat(rows, in_new.shape[1])
        total, total_weighted = down_rows_sum(floored), down_rows_sum(weighted)
        which = inner_part(rank)
        for k in range(3):
            mine = jnp.where(which == k, 1.0, 0.0)
            payload[8 + k : 9 + k] = total * mine
            payload[11 + k : 12 + k] = total_weighted * mine
        rows, floored, weighted = row_stats(g_down[...], upright(down_old[...], g_down.shape[0]))
        down_new[...] = flat(rows, down_new.shape[1])
        payload[0:1] = down_rows_sum(floored)
        payload[1:2] = down_rows_sum(weighted)
        extra = jnp.where(lane == TOTAL_LANE + DOWN, down_rows_sum(rows), 0.0)
        rows, floored, weighted = row_stats(g_side[...], upright(side_old[...], g_side.shape[0]))
        side_new[...] = flat(rows, side_new.shape[1])
        first = position_rows(rank, g_side.shape[0])
        for k, pick in ((0, first), (1, jnp.logical_not(first))):
            payload[4 + k : 5 + k] = down_rows_sum(jnp.where(pick, floored, 0.0))
            payload[6 + k : 7 + k] = down_rows_sum(jnp.where(pick, weighted, 0.0))
            part = down_rows_sum(jnp.where(pick, rows, 0.0))
            extra = jnp.where(lane == TOTAL_LANE + POS + k, part, extra)
        gradient = pieces[0]
        for k in range(1, pieces.shape[0]):
            gradient = gradient + pieces[k]
        moment = decay_rate * moment_old[...] + (1.0 - decay_rate) * (
            gradient * gradient + tiny_square
        )
        change = gradient * lax.rsqrt(moment)
        moment_new[...] = moment
        update[...] = change
        squares = jnp.sum(down_rows_sum(change * change), axis=1, keepdims=True)
        extra = jnp.where(lane == own_segment(rank), squares, extra)
        payload[EXTRA : EXTRA + 1] = jnp.where(lane == LOSS_LANE, loss[...], extra)

    start = step * word.shape[0]
    rows, floored, weighted = row_stats(
        word[...], upright(word_old[...], word.shape[0], start)
    )
    word_new[...] += flat(rows, word_new.shape[1], start)
    held[0:1] += down_rows_sum(floored)
    held[1:2] += down_rows_sum(weighted)
    held[2:3] += jnp.broadcast_to(down_rows_sum(rows), (1, D))

    @pl.when(step == pl.num_programs(0) - 1)
    def _():
        payload[2:3] = held[0:1]
        payload[3:4] = held[1:2]
        extra = payload[EXTRA : EXTRA + 1]
        payload[EXTRA : EXTRA + 1] = jnp.where(
            lanes() == TOTAL_LANE + WORD, held[2:3], extra
        )


def lane_of(row, lane):
    return jnp.sum(jnp.where(lanes() == lane, row, 0.0), axis=1, keepdims=True)


def clip_scale(weighted, cols_new, mean_rows, size):
    mean_square = jnp.sum(weighted / cols_new, axis=1, keepdims=True) * mean_rows / size
    return learn_rate / jnp.maximum(1.0, jnp.sqrt(mean_square))


def step_of(gradient, rows_new, cols_new, mean_rows, rate):
    return rate * gradient * lax.rsqrt(rows_new * cols_new / mean_rows)


def update_kernel(
    summed,
    w_in,
    w_down,
    w_side,
    w_vec,
    w_word,
    g_in,
    g_down,
    g_side,
    change,
    g_word,
    in_rows,
    down_cols,
    word_cols,
    side_cols,
    in_cols_new,
    down_rows_new,
    side_rows_new,
    word_rows_new,
    new_in,
    in_copy,
    new_down,
    down_copy,
    new_side,
    side_copy,
    new_vec,
    vec_copy,
    new_word,
    word_copy,
    in_rows_new,
    down_cols_new,
    word_cols_new,
    side_cols_new,
    loss,
):
    rank = my_rank()
    half = 1.0 - decay_rate
    extra = summed[EXTRA : EXTRA + 1]

    def total(lane):
        return lane_of(extra, TOTAL_LANE + lane)

    word_factor = decay_rate * word_cols[...] + half * summed[2:3] / VOCAB
    word_mean = total(WORD) / VOCAB
    word_rate = clip_scale(summed[3:4], word_factor, word_mean, VOCAB * D)

    @pl.when(pl.program_id(0) == 0)
    def _():
        word_cols_new[...] = word_factor
        loss[...] = lane_of(extra, LOSS_LANE)
        which = inner_part(rank)
        factor = jnp.zeros((1, D), jnp.float32)
        mean = jnp.zeros((1, 1), jnp.float32)
        rate = jnp.zeros((1, 1), jnp.float32)
        for k, width in enumerate((3 * D, D, FF)):
            mine = which == k
            rows = decay_rate * in_rows[k : k + 1] + half * summed[8 + k : 9 + k] / width
            in_rows_new[k : k + 1] = rows
            center = jnp.mean(rows, axis=1, keepdims=True)
            speed = clip_scale(summed[11 + k : 12 + k], rows, center, D * width)
            factor = jnp.where(mine, rows, factor)
            mean = jnp.where(mine, center, mean)
            rate = jnp.where(mine, speed, rate)
        change_in = step_of(g_in[...], upright(in_cols_new[...], g_in.shape[0]), factor, mean, rate)
        fresh = w_in[...] - change_in.T
        new_in[...] = fresh
        in_copy[...] = fresh.astype(LOW)
        factor = decay_rate * down_cols[...] + half * summed[0:1] / FF
        down_cols_new[...] = factor
        mean = total(DOWN) / FF
        rate = clip_scale(summed[1:2], factor, mean, FF * D)
        rows = upright(down_rows_new[...], g_down.shape[0])
        fresh = w_down[...] - step_of(g_down[...], rows, factor, mean, rate)
        new_down[...] = fresh
        down_copy[...] = fresh.astype(LOW)
        steps = []
        rows = upright(side_rows_new[...], g_side.shape[0])
        for k, count in ((0, SEQ_LEN), (1, D)):
            factor = decay_rate * side_cols[k : k + 1] + half * summed[4 + k : 5 + k] / count
            side_cols_new[k : k + 1] = factor
            mean = total(POS + k) / count
            rate = clip_scale(summed[6 + k : 7 + k], factor, mean, count * D)
            steps.append(step_of(g_side[...], rows, factor, mean, rate))
        first = position_rows(rank, g_side.shape[0])
        fresh = w_side[...] - jnp.where(first, steps[0], steps[1])
        new_side[...] = fresh
        side_copy[...] = fresh.astype(LOW)
        segment = own_segment(rank)
        size = jnp.where(segment == 5, float(FF), float(D))
        clip = jnp.maximum(1.0, jnp.sqrt(lane_of(extra, segment) / size))
        fresh = w_vec[...] - learn_rate * change[...] / clip
        new_vec[...] = fresh
        vec_copy[...] = fresh.astype(LOW)

    count = g_word.shape[0]
    rows = upright(word_rows_new[...], count, pl.program_id(0) * count)
    fresh = w_word[...] - step_of(g_word[...], rows, word_factor, word_mean, word_rate)
    new_word[...] = fresh
    word_copy[...] = fresh.astype(LOW)


def adapt_fused(given, grads, local_loss):
    (
        layer_in,
        layer_down,
        word_table,
        side_mat,
        vectors,
        in_rows,
        in_cols,
        down_rows,
        down_cols,
        word_rows,
        word_cols,
        side_rows,
        side_cols,
        vec_moment,
    ) = given
    g_in, g_down, g_word, g_side, pieces = grads
    shape = jax.ShapeDtypeStruct
    single = jnp.float32
    words = word_table.shape[0]
    tile = words // 4

    def whole(*dims):
        return pl.BlockSpec(dims, lambda i: (0,) * len(dims))

    def tiled(width):
        return pl.BlockSpec((tile, width), lambda i: (i, 0))

    h_in, h_down, h_side = g_in.shape[0], g_down.shape[0], g_side.shape[0]
    vec_shape = pieces.shape[1:]
    in_new, down_new, side_new, word_new, moment_new, change, payload = pl.pallas_call(
        stats_kernel,
        name="stats",
        grid=(4,),
        in_specs=[
            whole(h_in, D),
            whole(h_down, D),
            whole(h_side, D),
            whole(*pieces.shape),
            tiled(D),
            whole(1, h_in),
            whole(1, h_down),
            whole(1, h_side),
            whole(1, words),
            whole(*vec_shape),
            whole(1, 1),
        ],
        out_specs=(
            whole(1, h_in),
            whole(1, h_down),
            whole(1, h_side),
            whole(1, words),
            whole(*vec_shape),
            whole(*vec_shape),
            whole(16, D),
        ),
        out_shape=(
            shape((1, h_in), single),
            shape((1, h_down), single),
            shape((1, h_side), single),
            shape((1, words), single),
            shape(vec_shape, single),
            shape(vec_shape, single),
            shape((16, D), single),
        ),
        scratch_shapes=[pltpu.VMEM((3, D), single)],
    )(
        g_in,
        g_down,
        g_side,
        pieces,
        g_word,
        in_cols.reshape(1, -1),
        down_rows.reshape(1, -1),
        side_rows.reshape(1, -1),
        word_rows.reshape(1, -1),
        vec_moment.reshape(vec_shape),
        local_loss.reshape(1, 1),
    )
    summed = sum_over_devices(payload.reshape(-1)).reshape(16, D)
    outs = [
        (whole(D, h_in), shape((D, h_in), single)),
        (whole(D, h_in), shape((D, h_in), LOW)),
        (whole(h_down, D), shape((h_down, D), single)),
        (whole(h_down, D), shape((h_down, D), LOW)),
        (whole(h_side, D), shape((h_side, D), single)),
        (whole(h_side, D), shape((h_side, D), LOW)),
        (whole(*vec_shape), shape(vec_shape, single)),
        (whole(*vec_shape), shape(vec_shape, LOW)),
        (tiled(D), shape((words, D), single)),
        (tiled(D), shape((words, D), LOW)),
        (whole(3, D), shape((3, D), single)),
        (whole(1, D), shape((1, D), single)),
        (whole(1, D), shape((1, D), single)),
        (whole(2, D), shape((2, D), single)),
        (whole(1, 1), shape((1, 1), single)),
    ]
    (
        new_in,
        in_copy,
        new_down,
        down_copy,
        new_side,
        side_copy,
        new_vec,
        vec_copy,
        new_word,
        word_copy,
        in_rows_new,
        down_cols_new,
        word_cols_new,
        side_cols_new,
        loss,
    ) = pl.pallas_call(
        update_kernel,
        name="update",
        grid=(4,),
        in_specs=[
            whole(16, D),
            whole(D, h_in),
            whole(h_down, D),
            whole(h_side, D),
            whole(*vec_shape),
            tiled(D),
            whole(h_in, D),
            whole(h_down, D),
            whole(h_side, D),
            whole(*vec_shape),
            tiled(D),
            whole(3, D),
            whole(1, D),
            whole(1, D),
            whole(2, D),
            whole(1, h_in),
            whole(1, h_down),
            whole(1, h_side),
            whole(1, words),
        ],
        out_specs=tuple(spec for spec, _ in outs),
        out_shape=tuple(kind for _, kind in outs),
    )(
        summed,
        layer_in[0],
        layer_down[0],
        side_mat,
        vectors.reshape(vec_shape),
        word_table,
        g_in,
        g_down,
        g_side,
        change,
        g_word,
        in_rows[0],
        down_cols,
        word_cols.reshape(1, D),
        side_cols,
        in_new,
        down_new,
        side_new,
        word_new,
    )
    return (
        loss[0, 0],
        new_in[None],
        in_rows_new[None],
        in_new.reshape(1, -1),
        in_copy[None],
        new_down[None],
        down_new.reshape(1, -1),
        down_cols_new,
        down_copy[None],
        new_word,
        word_new.reshape(-1),
        word_cols_new.reshape(-1),
        word_copy,
        new_side,
        side_new.reshape(-1),
        side_cols_new,
        side_copy,
        new_vec.reshape(-1),
        moment_new.reshape(-1),
        vec_copy.reshape(-1),
    )


def adapt(given, grads, local_loss):
    (
        layer_in,
        layer_down,
        word_table,
        side_mat,
        vectors,
        in_rows,
        in_cols,
        down_rows,
        down_cols,
        word_rows,
        word_cols,
        side_rows,
        side_cols,
        vec_moment,
    ) = given
    grad_in_t, grad_down, grad_word, grad_side, grad_vec = grads
    my_index = lax.axis_index(BOTH)
    side_rows_local = side_mat.shape[0]
    vec_local = vectors.shape[0]
    grad_in = grad_in_t.T

    col_local = layer_in.shape[2]
    col_global = my_index * col_local + jnp.arange(col_local)
    sub_cols = jnp.stack(
        [col_global < 3 * D, (col_global >= 3 * D) & (col_global < 4 * D), col_global >= 4 * D]
    ).astype(jnp.float32)
    sub_width = jnp.array([3 * D, D, FF], jnp.float32)
    square_in = grad_in * grad_in
    in_cols_new = decay_rate * in_cols[0] + (1.0 - decay_rate) * jnp.mean(
        square_in + tiny_square, axis=0
    )
    row_part_in = jnp.stack(
        [jnp.sum((square_in + tiny_square) * pick[None, :], axis=1) for pick in sub_cols]
    )
    row_weighted_in = jnp.stack(
        [jnp.sum(square_in * (pick / in_cols_new)[None, :], axis=1) for pick in sub_cols]
    )

    def rows_of(gradient, rows_old):
        return decay_rate * rows_old + (1.0 - decay_rate) * jnp.mean(
            gradient * gradient + tiny_square, axis=1
        )

    rows_new_down = rows_of(grad_down, down_rows[0])
    col_down, weighted_down = factor_stats(grad_down, rows_new_down)
    rows_new_word = rows_of(grad_word, word_rows)
    col_word, weighted_word = factor_stats(grad_word, rows_new_word)
    row_global = my_index * side_rows_local + jnp.arange(side_rows_local)
    is_pos = row_global < SEQ_LEN
    which = jnp.stack([is_pos, jnp.logical_not(is_pos)]).astype(jnp.float32)
    side_counts = jnp.array([SEQ_LEN, D], jnp.float32)
    rows_new_side = rows_of(grad_side, side_rows)
    square_side = grad_side * grad_side
    col_side = jnp.stack(
        [jnp.sum((square_side + tiny_square) * pick[:, None], axis=0) for pick in which]
    )
    weighted_side = jnp.stack(
        [jnp.sum(square_side * (pick / rows_new_side)[:, None], axis=0) for pick in which]
    )
    total_side = jnp.sum(which * rows_new_side[None, :], axis=1)
    seg_onehot = (
        segment_index(my_index * vec_local + jnp.arange(vec_local))[:, None]
        == jnp.arange(9 * LAYERS + 4)[None, :]
    )
    new_moment = decay_rate * vec_moment + (1.0 - decay_rate) * (grad_vec * grad_vec + tiny_square)
    vec_update = grad_vec * lax.rsqrt(new_moment)
    seg_part = jnp.sum(jnp.where(seg_onehot, (vec_update * vec_update)[:, None], 0.0), axis=0)
    parts = [
        row_part_in,
        row_weighted_in,
        col_down,
        weighted_down,
        col_word,
        weighted_word,
        col_side,
        weighted_side,
        total_side,
        jnp.sum(rows_new_down)[None],
        jnp.sum(rows_new_word)[None],
        seg_part,
        local_loss[None],
    ]
    summed = sum_over_devices(jnp.concatenate([p.reshape(-1) for p in parts]))
    sums, offset = [], 0
    for p in parts:
        sums.append(summed[offset : offset + p.size].reshape(p.shape))
        offset += p.size
    (
        row_sum_in,
        row_weighted_in,
        col_down,
        weighted_down,
        col_word,
        weighted_word,
        col_side,
        weighted_side,
        total_side,
        total_down,
        total_word,
        seg_squares,
        loss_total,
    ) = sums
    half = 1.0 - decay_rate
    rows_new_in = decay_rate * in_rows[0] + half * row_sum_in / sub_width[:, None]
    mean_in = jnp.mean(rows_new_in, axis=1)
    scale_in = clip_of(row_weighted_in, rows_new_in, mean_in, D * sub_width)

    def choose(options):
        return jnp.sum(sub_cols[:, None, :] * options[:, :, None], axis=0)

    row_sel_in = choose(rows_new_in)
    factor_in = jnp.sum(sub_cols * (learn_rate / scale_in)[:, None], axis=0)
    mean_sel_in = jnp.sum(sub_cols * mean_in[:, None], axis=0)
    new_in = layer_in[0] - factor_in[None, :] * grad_in * lax.rsqrt(
        row_sel_in * in_cols_new[None, :] / mean_sel_in[None, :]
    )
    cols_new_down = decay_rate * down_cols[0] + half * col_down / FF
    mean_down = total_down[0] / FF
    scale_down = clip_of(weighted_down, cols_new_down, mean_down, FF * D)
    new_down = layer_down[0] - (learn_rate / scale_down) * grad_down * lax.rsqrt(
        rows_new_down[:, None] * cols_new_down[None, :] / mean_down
    )
    cols_new_word = decay_rate * word_cols + half * col_word / VOCAB
    mean_word = total_word[0] / VOCAB
    scale_word = clip_of(weighted_word, cols_new_word, mean_word, VOCAB * D)
    new_word = word_table - (learn_rate / scale_word) * grad_word * lax.rsqrt(
        rows_new_word[:, None] * cols_new_word[None, :] / mean_word
    )
    cols_new_side = decay_rate * side_cols + half * col_side / side_counts[:, None]
    mean_side = total_side / side_counts
    scale_side = clip_of(weighted_side, cols_new_side, mean_side, side_counts * D)
    col_sel_side = jnp.where(is_pos[:, None], cols_new_side[0][None, :], cols_new_side[1][None, :])
    mean_sel_side = jnp.where(is_pos, mean_side[0], mean_side[1])
    factor_side = learn_rate / jnp.where(is_pos, scale_side[0], scale_side[1])
    new_side = side_mat - factor_side[:, None] * grad_side * lax.rsqrt(
        rows_new_side[:, None] * col_sel_side / mean_sel_side[:, None]
    )
    seg_scale = jnp.maximum(1.0, jnp.sqrt(seg_squares / segment_sizes()))
    vec_scale = jnp.sum(jnp.where(seg_onehot, seg_scale[None, :], 0.0), axis=1)
    new_vectors = vectors - learn_rate * vec_update / vec_scale
    return (
        loss_total[0],
        new_in[None],
        rows_new_in[None],
        in_cols_new[None],
        new_in.astype(LOW)[None],
        new_down[None],
        rows_new_down[None],
        cols_new_down[None],
        new_down.astype(LOW)[None],
        new_word,
        rows_new_word,
        cols_new_word,
        new_word.astype(LOW),
        new_side,
        rows_new_side,
        cols_new_side,
        new_side.astype(LOW),
        new_vectors,
        new_moment,
        new_vectors.astype(LOW),
    )


def local(
    token_ids,
    labels,
    loss_mask,
    batch_of,
    layer_in,
    layer_down,
    word_table,
    side_mat,
    vectors,
    in_rows,
    in_cols,
    down_rows,
    down_cols,
    word_rows,
    word_cols,
    side_rows,
    side_cols,
    vec_moment,
):
    seq_dev, length = token_ids.shape
    tokens = seq_dev * length
    n_blocks = lax.axis_size(BOTH)
    my_index = lax.axis_index(BOTH)
    mask_float = loss_mask.astype(jnp.float32)
    member = batch_of[:, None] == jnp.arange(MICRO)[None, :]
    local_counts = jnp.sum(member * jnp.sum(loss_mask, axis=1)[:, None], axis=0)
    block_rows = word_table.shape[0]
    capacity = max(2, 2 * tokens // n_blocks)
    flat_ids = token_ids.reshape(tokens)
    blocks = flat_ids // block_rows
    label_float = labels.astype(jnp.float32).reshape(tokens)

    side_rows_local = side_mat.shape[0]
    vec_local = vectors.shape[0]
    vector_row = jnp.pad(vectors.astype(LOW).reshape(1, -1), ((0, 15), (0, D - vec_local)))
    (side_all, weight_in, weight_down), returned, to_slot, from_slot, counts = gather_blocks(
        [
            jnp.concatenate([side_mat.astype(LOW), vector_row], axis=0),
            layer_in[0].astype(LOW).T,
            layer_down[0].astype(LOW),
        ],
        blocks,
        flat_ids - blocks * block_rows,
        local_counts.astype(jnp.int32),
        word_table.astype(LOW),
        capacity,
    )
    seq_count = jnp.sum(member * counts[None, :], axis=1)
    token_weight = (mask_float / (seq_count * MICRO)[:, None]).reshape(tokens)
    side_all = side_all.reshape(n_blocks, side_rows_local + 16, D)
    side_full = side_all[:, :side_rows_local].reshape(-1, D)
    vector_full = side_all[:, side_rows_local, :vec_local].reshape(-1)
    all_vectors = vector_full.astype(jnp.float32)
    pos_rows = side_full[:SEQ_LEN].astype(jnp.float32)
    head_mat = side_full[SEQ_LEN:]
    global_offset = LAYERS * (8 * D + FF)
    gain_emb = all_vectors[global_offset : global_offset + D]
    shift_emb = all_vectors[global_offset + D : global_offset + 2 * D]
    head_bias = all_vectors[global_offset + 2 * D : global_offset + 3 * D]
    predictor = all_vectors[global_offset + 3 * D : global_offset + 4 * D]
    predictor_low = vector_full[global_offset + 3 * D : global_offset + 4 * D]
    own_rows = multiply_left(to_slot, returned.reshape(n_blocks * capacity, D))
    embedded = (own_rows.reshape(seq_dev, length, D) + pos_rows[None, :, :]).reshape(tokens, D)
    hidden = layer_norm(embedded, gain_emb, shift_emb)
    pieces = layer_slices(all_vectors, 0)
    hidden, kept = layer_forward(hidden, weight_in, weight_down, pieces, seq_dev)
    final_low = hidden.astype(LOW)
    head_pre = multiply(final_low, head_mat) + head_bias
    head_act_low = exact_gelu(head_pre).astype(LOW)
    logits = multiply(head_act_low, predictor_low)
    local_loss = jnp.sum(token_weight * (jax.nn.softplus(logits) - label_float * logits))
    d_logits = token_weight * (jax.nn.sigmoid(logits) - label_float)
    d_predictor = jnp.sum(d_logits[:, None] * head_act_low.astype(jnp.float32), axis=0)
    d_head_low = gelu_back(head_pre, d_logits[:, None] * predictor[None, :]).astype(LOW)
    grad_head = multiply_left(final_low, d_head_low)
    d_head_bias = jnp.sum(d_head_low.astype(jnp.float32), axis=0)
    d_hidden = multiply_right(d_head_low, head_mat)
    d_hidden, pairs, grad_pieces = layer_backward(
        d_hidden, weight_in, weight_down, pieces, kept, seq_dev
    )
    d_embedded, d_gain_emb, d_shift_emb = norm_back(embedded, gain_emb, shift_emb, d_hidden)
    grad_pos = jnp.sum(d_embedded.reshape(seq_dev, length, D), axis=0)
    grad_vector = jnp.concatenate([grad_pieces, d_gain_emb, d_shift_emb, d_head_bias, d_predictor])
    buckets = (
        multiply(to_slot, d_embedded.astype(LOW))
        .astype(LOW)
        .reshape(n_blocks, capacity, D)
    )
    grad_side, grad_in_t, grad_down, arrived, grad_vec = reduce_blocks(
        pairs, grad_pos, grad_head, buckets, grad_vector
    )
    grad_word = multiply_left(from_slot, arrived.reshape(n_blocks * capacity, D))
    given = (
        layer_in,
        layer_down,
        word_table,
        side_mat,
        vectors,
        in_rows,
        in_cols,
        down_rows,
        down_cols,
        word_rows,
        word_cols,
        side_rows,
        side_cols,
        vec_moment,
    )
    grads = (grad_in_t, grad_down, grad_word, grad_side, grad_vec)
    if special():
        return adapt_fused(given, grads, local_loss)
    return adapt(given, grads, local_loss)


def solution(mesh):
    return jax.shard_map(
        local,
        mesh=mesh,
        in_specs=(
            P(("fsdp", "dp"), None),
            P(("fsdp", "dp"), None),
            P(("fsdp", "dp"), None),
            P(("fsdp", "dp")),
            P(None, None, ("fsdp", "dp")),
            P(None, ("fsdp", "dp"), None),
            P(("fsdp", "dp"), None),
            P(("fsdp", "dp"), None),
            P(("fsdp", "dp")),
            P(),
            P(None, ("fsdp", "dp")),
            P(None, ("fsdp", "dp")),
            P(),
            P(("fsdp", "dp")),
            P(),
            P(("fsdp", "dp")),
            P(),
            P(("fsdp", "dp")),
        ),
        out_specs=(
            P(),
            P(None, None, ("fsdp", "dp")),
            P(),
            P(None, ("fsdp", "dp")),
            P(None, None, ("fsdp", "dp")),
            P(None, ("fsdp", "dp"), None),
            P(None, ("fsdp", "dp")),
            P(),
            P(None, ("fsdp", "dp"), None),
            P(("fsdp", "dp"), None),
            P(("fsdp", "dp")),
            P(),
            P(("fsdp", "dp"), None),
            P(("fsdp", "dp"), None),
            P(("fsdp", "dp")),
            P(),
            P(("fsdp", "dp"), None),
            P(("fsdp", "dp")),
            P(("fsdp", "dp")),
            P(("fsdp", "dp")),
        ),
        check_vma=False,
    )
```
